32 devices in a mesh: fsdp: 4 (over z), heads: 2 (over core), tensor: 4 (over y, x).
Axes of the slice: x: 2, y: 2, z: 4, core: 2. Of those that a mesh axis runs over, the one named last changes fastest.
Arguments:
- block_input: bfloat16 [1536, 1536], P(('fsdp', 'heads')), may hold values from -6 to 6
- segments: int32 [1536], replicated, may hold values from 0 to 2, as said below
- routes: int32 [1536, 8], P(('fsdp', 'heads')), may hold values from 0 to 15, all different within a row
- attn_gain: bfloat16 [1536], P(('fsdp', 'heads')), may hold values from 0.5 to 1.5
- ffn_gain: bfloat16 [1536], P(('fsdp', 'heads')), may hold values from 0.5 to 1.5
- query_weight: bfloat16 [1536, 1536], P(('fsdp', 'heads')), may hold values from -0.4375 to 0.4375
- key_matrix: bfloat16 [1536, 512], P(('fsdp', 'heads')), may hold values from -0.4375 to 0.4375
- value_matrix: bfloat16 [1536, 512], P(('fsdp', 'heads')), may hold values from -0.15625 to 0.15625
- out_weight: bfloat16 [1536, 1536], P(('fsdp', 'heads')), may hold values from -12 to 12
- router_weight: bfloat16 [1536, 16], P(('fsdp', 'heads')), may hold values from -0.3125 to 0.3125
- gate_weight: bfloat16 [16, 1536, 512], P(None, ('fsdp', 'heads'), 'tensor'), may hold values from -0.15625 to 0.15625
- up_weight: bfloat16 [16, 1536, 512], P(None, ('fsdp', 'heads'), 'tensor'), may hold values from -0.15625 to 0.15625
- down_weight: bfloat16 [16, 512, 1536], P(None, 'tensor', ('fsdp', 'heads')), may hold values from -1 to 1
- grad_output: float32 [1536, 1536], P(('fsdp', 'heads')), may hold values from -6 to 6
Outputs:
- block_output: float32 [1536, 1536], P(('fsdp', 'heads'), 'tensor')
- grad_input: float32 [1536, 1536], P(('fsdp', 'heads'))
- grad_attn_gain: float32 [1536], P(('fsdp', 'heads'))
- grad_ffn_gain: float32 [1536], P(('fsdp', 'heads'))
- grad_query: float32 [1536, 1536], P(('fsdp', 'heads'))
- grad_key: float32 [1536, 512], P(('fsdp', 'heads'))
- grad_value: float32 [1536, 512], P(('fsdp', 'heads'))
- grad_out_proj: float32 [1536, 1536], P(('fsdp', 'heads'))
- grad_router: float32 [1536, 16], P(('fsdp', 'heads'))
- grad_gate: float32 [16, 1536, 512], P(None, ('fsdp', 'heads'), 'tensor')
- grad_up: float32 [16, 1536, 512], P(None, ('fsdp', 'heads'), 'tensor')
- grad_down: float32 [16, 512, 1536], P(None, 'tensor', ('fsdp', 'heads'))
The draws below stay inside these ranges and needn't reach their ends.
Inputs may be any that keep to these rules, and one draw needn't show every extreme that they name: `segments`: segment numbers start at 0 and rise by one at each document's start; there are 3 documents, each of 96 to 960 tokens, and the first has exactly 960. `routes`: each token names 8 different experts; every expert is named by some token.
All inputs are finite; a program needn't handle non-finite values.
Results may differ from the reference program's by a relative error of at most 0.017.
Values may be sent and summed in bfloat16 or wider, within the bound.
A program may use at most 256 MiB of HBM per device.

```python
import jax
import jax.numpy as jnp
from jax import lax

MODEL_DIM = 1536
QUERY_HEADS = 24
KEY_VALUE_HEADS = 8
HEAD_DIM = 64
FF = 512
TOPK = 8
E = 16
TOKENS = 1536
DOC_MOST = 960
DOC_LEAST = 96
DOCS = 3


def draw_segments(key, part):
    other_docs = DOCS - 1
    rest_tokens = TOKENS - DOC_MOST
    spare_tokens = rest_tokens - other_docs * DOC_LEAST
    shares = jax.random.randint(key, (other_docs,), 1, 5, dtype=jnp.int32)
    extra = spare_tokens * shares // jnp.sum(shares)
    leftover = spare_tokens - jnp.sum(extra)
    extra = extra + (jnp.arange(other_docs, dtype=jnp.int32) < leftover).astype(jnp.int32)
    lengths = jnp.concatenate([jnp.full((1,), DOC_MOST, jnp.int32), (DOC_LEAST + extra).astype(jnp.int32)])
    cuts = jnp.cumsum(lengths).astype(jnp.int32)[:-1]
    token_positions = jnp.arange(TOKENS, dtype=jnp.int32)
    crossed = token_positions[:, None] >= cuts[None, :]
    return jnp.sum(crossed.astype(jnp.int32), axis=1).astype(jnp.int32)


def block_scale(rng, shape, pieces, least, high):
    level, own = 1.0, jax.random.fold_in(rng, 6)
    for dim, shards_of in pieces:
        heights = jnp.exp(jax.random.uniform(jax.random.fold_in(own, dim), (shards_of,), jnp.float32, least / len(pieces), high / len(pieces)))
        level = level * jnp.repeat(heights, shape[dim] // shards_of).reshape([-1 if axis == dim else 1 for axis in range(len(shape))])
    return level


def choose_distinct(key, rows, count, top, lift):
    ranking = jax.random.permutation(jax.random.fold_in(key, 1), count)
    favour = ranking
    for power in range(3):
        favour = favour * favour // count
    favour = favour * lift // count
    lots = jax.random.randint(jax.random.fold_in(key, 2), (rows, count), 0, 4096) + favour
    fixed_rows = jax.random.permutation(jax.random.fold_in(key, 3), rows)[jnp.arange(count) % rows]
    lots = jnp.where(jnp.arange(rows)[:, None] == fixed_rows[None, :], 1 << 14, lots)
    priority = lots * count + jnp.arange(count)
    return lax.top_k(priority.astype(jnp.int32), top)[1].astype(jnp.int32)


def normal_values(stream_key, extent, scale, most, cuts=(), kind=jnp.bfloat16):
    factor_of = block_scale(stream_key, extent, cuts, -0.22, 0.18) if cuts else 1.0
    values = jax.random.normal(stream_key, extent, jnp.float32) * scale * factor_of
    return jnp.minimum(jnp.maximum(values, -most), most).astype(kind)


def setup_inputs(seed: int = 0) -> dict:
    keys = jax.random.split(jax.random.key(seed), 15)
    block_input = normal_values(keys[0], (TOKENS, MODEL_DIM), 1.0, 6.0, ((0, 8),))
    segments = draw_segments(jax.random.fold_in(keys[14], 71), 0)
    routes = choose_distinct(keys[2], TOKENS, E, TOPK, 4096)
    attn_gain = jnp.clip(1.0 + 0.1 * jax.random.normal(keys[3], (MODEL_DIM,), jnp.float32), 0.5, 1.5).astype(jnp.bfloat16)
    ffn_gain = jnp.clip(1.0 + 0.1 * jax.random.normal(keys[4], (MODEL_DIM,), jnp.float32), 0.5, 1.5).astype(jnp.bfloat16)
    query_weight = normal_values(keys[5], (MODEL_DIM, QUERY_HEADS * HEAD_DIM), (MODEL_DIM // 8) ** -0.5, 0.4375, ((0, 8),))
    key_matrix = normal_values(keys[6], (MODEL_DIM, KEY_VALUE_HEADS * HEAD_DIM), (MODEL_DIM // 8) ** -0.5, 0.4375, ((0, 8),))
    value_matrix = normal_values(keys[7], (MODEL_DIM, KEY_VALUE_HEADS * HEAD_DIM), MODEL_DIM ** -0.5, 0.15625, ((0, 8),))
    out_weight = normal_values(keys[8], (QUERY_HEADS * HEAD_DIM, MODEL_DIM), 2.0, 12.0, ((0, 8),))
    router_weight = normal_values(keys[9], (MODEL_DIM, E), (MODEL_DIM // 4) ** -0.5, 0.3125, ((0, 8),))
    gate_weight = normal_values(keys[10], (E, MODEL_DIM, FF), MODEL_DIM ** -0.5, 0.15625, ((1, 8), (2, 4)))
    up_weight = normal_values(keys[11], (E, MODEL_DIM, FF), MODEL_DIM ** -0.5, 0.15625, ((1, 8), (2, 4)))
    down_weight = normal_values(keys[12], (E, FF, MODEL_DIM), (FF // 16) ** -0.5, 1.0, ((1, 4), (2, 8)))
    grad_output = normal_values(keys[13], (TOKENS, MODEL_DIM), 1.0, 6.0, ((0, 8),), jnp.float32)
    return {"block_input": block_input, "segments": segments, "routes": routes, "attn_gain": attn_gain, "ffn_gain": ffn_gain, "query_weight": query_weight, "key_matrix": key_matrix, "value_matrix": value_matrix, "out_weight": out_weight, "router_weight": router_weight, "gate_weight": gate_weight, "up_weight": up_weight, "down_weight": down_weight, "grad_output": grad_output}


@jax.custom_vjp
def lower_precision(v):
    return lax.optimization_barrier(v.astype(jnp.bfloat16)).astype(jnp.float32)

@jax.custom_vjp
def lower_backward(v):
    return v

def low_keep(v):
    return (lower_precision(v), None)

def low_pass(kept, grad):
    return (grad,)

def back_keep(v):
    return (v, None)

def back_low(kept, grad):
    return (lower_precision(grad),)
lower_precision.defvjp(low_keep, low_pass)
lower_backward.defvjp(back_keep, back_low)
norm_eps = 1e-06
score_scale = 0.015625
residual_scale = 0.22
rope_base = 10000.0

def rms_gain(vectors, gain):
    factor = lax.rsqrt(lax.optimization_barrier(jnp.mean(vectors * vectors, axis=-1, keepdims=True)) + norm_eps)
    return vectors * factor * gain

def apply_rotary(vectors, token_positions):
    half_size = vectors.shape[-1] // 2
    inverse = rope_base ** (-(jnp.arange(half_size, dtype=jnp.float32) * 2.0 / vectors.shape[-1]))
    angles = token_positions[:, None].astype(jnp.float32) * inverse[None, :]
    cosine_lookup = jnp.cos(angles)[:, None, :]
    sine_lookup = jnp.sin(angles)[:, None, :]
    first_half = vectors[..., :half_size]
    second_half = vectors[..., half_size:]
    return jnp.concatenate([first_half * cosine_lookup - second_half * sine_lookup, second_half * cosine_lookup + first_half * sine_lookup], axis=-1)

def reference(block_input, segments, routes, attn_gain, ffn_gain, query_weight, key_matrix, value_matrix, out_weight, router_weight, gate_weight, up_weight, down_weight, grad_output):
    highest_precision = lax.Precision.HIGHEST
    floats = tuple((array.astype(jnp.float32) for array in (block_input, attn_gain, ffn_gain, query_weight, key_matrix, value_matrix, out_weight, router_weight, gate_weight, up_weight, down_weight)))

    def forward(inputs, gain_attn, gain_ffn, weight_query, weight_key, value_weight_full, weight_out, weight_router, weight_gate, weight_up, weight_down):
        sequence_length = inputs.shape[0]
        token_positions = jnp.arange(sequence_length, dtype=jnp.int32)
        normalized_input = lower_precision(rms_gain(inputs, gain_attn))
        query_lin = lower_backward(jnp.dot(normalized_input, weight_query, precision=highest_precision))
        key_linear = lower_backward(jnp.dot(normalized_input, weight_key, precision=highest_precision))
        query_vectors = lower_backward(lower_precision(apply_rotary(query_lin.reshape(sequence_length, QUERY_HEADS, HEAD_DIM), token_positions)))
        keys_gathered = lower_backward(lower_precision(apply_rotary(key_linear.reshape(sequence_length, KEY_VALUE_HEADS, HEAD_DIM), token_positions)))
        values_gathered = lower_backward(lower_precision(jnp.dot(normalized_input, value_weight_full, precision=highest_precision))).reshape(sequence_length, KEY_VALUE_HEADS, HEAD_DIM)
        heads_per_group = QUERY_HEADS // KEY_VALUE_HEADS
        grouped_heads = query_vectors.reshape(sequence_length, KEY_VALUE_HEADS, heads_per_group, HEAD_DIM)
        block_size = min(512, sequence_length)
        starts = jnp.arange(sequence_length // block_size, dtype=jnp.int32) * block_size

        def attend_block(block_start):
            block_rows = lax.dynamic_slice_in_dim(grouped_heads, block_start, block_size, 0)
            raw_scores = jnp.einsum('qkgd,jkd->kgqj', block_rows, keys_gathered, precision=highest_precision) * score_scale
            scores = lower_backward(raw_scores)
            query_pos = block_start + jnp.arange(block_size, dtype=jnp.int32)
            query_seg = lax.dynamic_slice_in_dim(segments, block_start, block_size, 0)
            allowed = (query_pos[:, None] >= token_positions[None, :]) & (query_seg[:, None] == segments[None, :])
            weights = jnp.where(allowed[None, None], jnp.exp(scores), 0.0)
            denominator = lax.optimization_barrier(jnp.sum(weights, axis=-1))
            numerator = lower_backward(jnp.einsum('kgqj,jkd->kgqd', lower_precision(weights), values_gathered, precision=highest_precision))
            result_block = lower_backward(lower_precision(numerator / denominator[..., None]))
            return result_block.transpose(2, 0, 1, 3)
        attended = lax.map(jax.checkpoint(attend_block), starts).reshape(sequence_length, QUERY_HEADS * HEAD_DIM)
        projected = lower_backward(jnp.dot(attended, weight_out, precision=highest_precision))
        hidden = inputs + residual_scale * projected
        normed_two = lower_precision(rms_gain(hidden, gain_ffn))
        logits = lower_backward(jnp.dot(normed_two, weight_router, precision=highest_precision))
        onehot = (routes[:, :, None] == jnp.arange(E, dtype=jnp.int32)[None, None, :]).astype(jnp.float32)
        picked = jnp.einsum('tke,te->tk', onehot, logits, precision=highest_precision)
        route_probs = jax.nn.softmax(picked, axis=-1)
        combine = jnp.einsum('tke,tk->te', onehot, route_probs, precision=highest_precision)

        def expert_step(running, packed):
            expert_gate, expert_up, expert_down, weight_col = packed
            gate_pre = lower_backward(jnp.dot(normed_two, expert_gate, precision=highest_precision))
            up_pre = lower_backward(jnp.dot(normed_two, expert_up, precision=highest_precision))
            active = lower_precision(jax.nn.silu(gate_pre) * up_pre)
            expert_out = lower_backward(jnp.dot(active, expert_down, precision=highest_precision))
            return (running + weight_col[:, None] * expert_out, None)
        mixed_sum, _ = lax.scan(jax.checkpoint(expert_step), jnp.zeros_like(hidden), (weight_gate, weight_up, weight_down, combine.T))
        return hidden + residual_scale * mixed_sum
    result, pullback = jax.vjp(forward, *floats)
    grads = pullback(grad_output.astype(jnp.float32))
    return (result, grads[0], grads[1], grads[2], grads[3], grads[4], grads[5], grads[6], grads[7], grads[8], grads[9], grads[10])
```

```python
import math

import jax
import jax.numpy as jnp
from jax import lax
from jax.sharding import PartitionSpec as P

QUERY_HEADS = 24
KEY_VALUE_HEADS = 8
HEAD_DIM = 64
E = 16


norm_eps = 1e-06
score_scale = 0.015625
residual_scale = 0.22
rope_base = 10000.0


def rotary_table(token_positions, head_size):
    half_size = head_size // 2
    inverse = rope_base ** (-(jnp.arange(half_size, dtype=jnp.float32) * 2.0 / head_size))
    angles = token_positions[:, None].astype(jnp.float32) * inverse[None, :]
    return (jnp.cos(angles)[:, None, :], jnp.sin(angles)[:, None, :])


def apply_rotary(vectors, cosine_lookup, sine_lookup):
    half_size = vectors.shape[-1] // 2
    first_half = vectors[..., :half_size]
    second_half = vectors[..., half_size:]
    return jnp.concatenate(
        [
            first_half * cosine_lookup - second_half * sine_lookup,
            second_half * cosine_lookup + first_half * sine_lookup,
        ],
        axis=-1,
    )


def reverse_rotary(gradient, cosine_lookup, sine_lookup):
    half_size = gradient.shape[-1] // 2
    first_half = gradient[..., :half_size]
    second_half = gradient[..., half_size:]
    return jnp.concatenate(
        [
            first_half * cosine_lookup + second_half * sine_lookup,
            second_half * cosine_lookup - first_half * sine_lookup,
        ],
        axis=-1,
    )


def body(
    block_input,
    segments,
    routes,
    attn_gain,
    ffn_gain,
    query_weight,
    key_matrix,
    value_matrix,
    out_weight,
    router_weight,
    gate_weight,
    up_weight,
    down_weight,
    grad_output,
):
    head_count = lax.axis_size("heads")
    n_tensor = lax.axis_size("tensor")
    n_fsdp = lax.axis_size("fsdp")
    fsdp_index = lax.axis_index("fsdp")
    heads_index = lax.axis_index("heads")
    tensor_index = lax.axis_index("tensor")
    token_rows = block_input.shape[0]
    model_width = block_input.shape[1]
    query_rows = token_rows * head_count
    seq_rows = query_rows * n_fsdp
    key_value_local = KEY_VALUE_HEADS // head_count
    heads_per_group = QUERY_HEADS // KEY_VALUE_HEADS
    slice_width = model_width // n_tensor
    gathered = (
        lax.all_gather(attn_gain, ("fsdp", "heads"), axis=0, tiled=True),
        lax.all_gather(ffn_gain, ("fsdp", "heads"), axis=0, tiled=True),
        lax.all_gather(query_weight, ("fsdp", "heads"), axis=0, tiled=True),
        lax.all_gather(key_matrix, ("fsdp", "heads"), axis=0, tiled=True),
        lax.all_gather(value_matrix, ("fsdp", "heads"), axis=0, tiled=True),
        lax.all_gather(out_weight, ("fsdp", "heads"), axis=0, tiled=True),
        lax.all_gather(router_weight, ("fsdp", "heads"), axis=0, tiled=True),
        lax.all_gather(gate_weight, ("fsdp", "heads"), axis=1, tiled=True),
        lax.all_gather(up_weight, ("fsdp", "heads"), axis=1, tiled=True),
        lax.all_gather(down_weight, ("fsdp", "heads"), axis=2, tiled=True),
    )
    gain_attn = gathered[0].astype(jnp.float32)
    gain_ffn = gathered[1].astype(jnp.float32)
    full_query, full_key, full_value, full_out, full_router, full_gate, full_up, full_down = (
        gathered[2:]
    )
    inputs = block_input.astype(jnp.float32)
    scale_one = lax.rsqrt(jnp.mean(inputs * inputs, axis=-1, keepdims=True) + norm_eps)
    unit_one = inputs * scale_one
    normalized_input = (unit_one * gain_attn).astype(jnp.bfloat16)
    query_lin = jnp.dot(normalized_input, full_query, preferred_element_type=jnp.float32)
    key_linear = jnp.dot(normalized_input, full_key, preferred_element_type=jnp.float32)
    value_lin = jnp.dot(normalized_input, full_value, preferred_element_type=jnp.float32)
    own_start = (fsdp_index * head_count + heads_index) * token_rows
    token_positions = own_start + jnp.arange(token_rows, dtype=jnp.int32)
    cosine_lookup, sine_lookup = rotary_table(token_positions, HEAD_DIM)
    query_send = (
        apply_rotary(
            query_lin.reshape(token_rows, QUERY_HEADS, HEAD_DIM), cosine_lookup, sine_lookup
        )
        .reshape(token_rows, QUERY_HEADS * HEAD_DIM)
        .astype(jnp.bfloat16)
    )
    key_send = (
        apply_rotary(
            key_linear.reshape(token_rows, KEY_VALUE_HEADS, HEAD_DIM), cosine_lookup, sine_lookup
        )
        .reshape(token_rows, KEY_VALUE_HEADS * HEAD_DIM)
        .astype(jnp.bfloat16)
    )
    value_send = value_lin.astype(jnp.bfloat16)
    query_heads, key_local, value_local = (
        lax.all_to_all(query_send, "heads", split_axis=1, concat_axis=0, tiled=True),
        lax.all_to_all(key_send, "heads", split_axis=1, concat_axis=0, tiled=True),
        lax.all_to_all(value_send, "heads", split_axis=1, concat_axis=0, tiled=True),
    )
    query_vectors = query_heads.reshape(query_rows, key_value_local, heads_per_group, HEAD_DIM)
    query_start = fsdp_index * query_rows
    query_pos = query_start + jnp.arange(query_rows, dtype=jnp.int32)
    query_seg = lax.dynamic_slice_in_dim(segments, query_start, query_rows, 0)

    def masked_exp(key_block, key_start):
        block_rows = key_block.shape[0]
        raw_scores = (
            jnp.einsum(
                "qkgd,jkd->kgqj", query_vectors, key_block, preferred_element_type=jnp.float32
            )
            * score_scale
        )
        key_pos = key_start + jnp.arange(block_rows, dtype=jnp.int32)
        key_seg = lax.dynamic_slice_in_dim(segments, key_start, block_rows, 0)
        allowed = (query_pos[:, None] >= key_pos[None, :]) & (
            query_seg[:, None] == key_seg[None, :]
        )
        return jnp.where(allowed[None, None], jnp.exp(raw_scores), 0.0)

    def split_blocks(key_piece):
        keys_piece, values_piece = key_piece
        piece_rows = keys_piece.shape[0]
        block_rows = math.gcd(piece_rows, query_rows)
        block_count = piece_rows // block_rows
        starts = jnp.arange(block_count, dtype=jnp.int32) * block_rows
        return (
            keys_piece.reshape(block_count, block_rows, key_value_local, HEAD_DIM),
            values_piece.reshape(block_count, block_rows, key_value_local, HEAD_DIM),
            starts,
        )

    start_state = (
        jnp.zeros((key_value_local, heads_per_group, query_rows), jnp.float32),
        jnp.zeros((key_value_local, heads_per_group, query_rows, HEAD_DIM), jnp.float32),
    )
    fold_state = start_state

    def block_step(running, block_item):
        denominator, numerator = running
        key_block, value_block, key_start = block_item
        weights = masked_exp(key_block, key_start)
        denominator = denominator + jnp.sum(weights, axis=-1)
        numerator = numerator + jnp.einsum(
            "kgqj,jkd->kgqd",
            weights.astype(jnp.bfloat16),
            value_block,
            preferred_element_type=jnp.float32,
        )
        return ((denominator, numerator), None)

    fold_state, _ = lax.scan(
        block_step,
        fold_state,
        split_blocks(
            (
                lax.all_gather(key_local, "fsdp", axis=0, tiled=True),
                lax.all_gather(value_local, "fsdp", axis=0, tiled=True),
            )
        ),
    )
    denominator, numerator = fold_state
    attn_full = numerator / denominator[..., None]
    attn_send = (
        attn_full.transpose(2, 0, 1, 3)
        .reshape(query_rows, key_value_local * heads_per_group * HEAD_DIM)
        .astype(jnp.bfloat16)
    )
    attn_back = lax.all_to_all(attn_send, "heads", split_axis=0, concat_axis=1, tiled=True)
    attn_proj = jnp.dot(attn_back, full_out, preferred_element_type=jnp.float32)
    hidden = inputs + residual_scale * attn_proj
    scale_two = lax.rsqrt(jnp.mean(hidden * hidden, axis=-1, keepdims=True) + norm_eps)
    unit_two = hidden * scale_two
    normed_two = (unit_two * gain_ffn).astype(jnp.bfloat16)
    logits = jnp.dot(normed_two, full_router, preferred_element_type=jnp.float32)
    onehot = (routes[:, :, None] == jnp.arange(E, dtype=jnp.int32)[None, None, :]).astype(
        jnp.float32
    )
    picked = jnp.sum(onehot * logits[:, None, :], axis=-1)
    route_probs = jax.nn.softmax(picked, axis=-1)
    combine = jnp.sum(onehot * route_probs[:, :, None], axis=1)
    gate_pre = jnp.einsum("td,edf->etf", normed_two, full_gate, preferred_element_type=jnp.float32)
    up_pre = jnp.einsum("td,edf->etf", normed_two, full_up, preferred_element_type=jnp.float32)
    sigmoid_gate = jax.nn.sigmoid(gate_pre)
    silu_gate = gate_pre * sigmoid_gate
    active = (silu_gate * up_pre).astype(jnp.bfloat16)
    expert_out = jnp.einsum("etf,efd->etd", active, full_down, preferred_element_type=jnp.float32)
    mixed_part = jnp.sum(combine.T[:, :, None] * expert_out, axis=0)
    mixed_sum = lax.psum_scatter(
        mixed_part.astype(jnp.bfloat16), "tensor", scatter_dimension=1, tiled=True
    ).astype(jnp.float32)
    hidden_mine = lax.dynamic_slice_in_dim(hidden, tensor_index * slice_width, slice_width, 1)
    block_output = hidden_mine + residual_scale * mixed_sum
    mixed_grad = residual_scale * grad_output
    expert_grad = (combine.T[:, :, None] * mixed_grad[None]).astype(jnp.bfloat16)
    combine_part = jnp.sum(expert_out * mixed_grad[None], axis=-1).T
    active_grad = jnp.einsum(
        "etd,efd->etf", expert_grad, full_down, preferred_element_type=jnp.float32
    )
    gate_grad = (
        active_grad * up_pre * sigmoid_gate * (1.0 + gate_pre * (1.0 - sigmoid_gate))
    ).astype(jnp.bfloat16)
    up_grad = (active_grad * silu_gate).astype(jnp.bfloat16)
    normed_part = jnp.einsum(
        "etf,edf->td", gate_grad, full_gate, preferred_element_type=jnp.float32
    ) + jnp.einsum("etf,edf->td", up_grad, full_up, preferred_element_type=jnp.float32)
    gate_full = jnp.einsum("td,etf->edf", normed_two, gate_grad, preferred_element_type=jnp.float32)
    up_full = jnp.einsum("td,etf->edf", normed_two, up_grad, preferred_element_type=jnp.float32)
    down_full = jnp.einsum("etf,etd->efd", active, expert_grad, preferred_element_type=jnp.float32)
    grad_gate, grad_up, grad_down = (
        lax.psum_scatter(gate_full.astype(jnp.bfloat16), ("fsdp", "heads"), scatter_dimension=1, tiled=True),
        lax.psum_scatter(up_full.astype(jnp.bfloat16), ("fsdp", "heads"), scatter_dimension=1, tiled=True),
        lax.psum_scatter(down_full.astype(jnp.bfloat16), ("fsdp", "heads"), scatter_dimension=2, tiled=True),
    )
    normed_grad, combine_grad = lax.psum((normed_part, combine_part), "tensor")
    pick_grad = jnp.sum(onehot * combine_grad[:, None, :], axis=-1)
    picked_grad = route_probs * (
        pick_grad - jnp.sum(route_probs * pick_grad, axis=-1, keepdims=True)
    )
    logit_grad = jnp.sum(onehot * picked_grad[:, :, None], axis=1).astype(jnp.bfloat16)
    router_full = jnp.dot(normed_two.T, logit_grad, preferred_element_type=jnp.float32)
    normed_grad = normed_grad + jnp.dot(
        logit_grad, full_router.T, preferred_element_type=jnp.float32
    )
    gain_ffn_full = jnp.sum(normed_grad * unit_two, axis=0)
    unit_grad = normed_grad * gain_ffn
    hidden_grad = grad_output + scale_two * (
        unit_grad - unit_two * jnp.mean(unit_grad * unit_two, axis=-1, keepdims=True)
    )
    proj_grad = (residual_scale * hidden_grad).astype(jnp.bfloat16)
    out_full = jnp.dot(attn_back.T, proj_grad, preferred_element_type=jnp.float32)
    attn_grad = jnp.dot(proj_grad, full_out.T, preferred_element_type=jnp.float32).astype(
        jnp.bfloat16
    )
    grad_heads = lax.all_to_all(attn_grad, "heads", split_axis=1, concat_axis=0, tiled=True)
    grad_float = (
        grad_heads.reshape(query_rows, key_value_local, heads_per_group, HEAD_DIM)
        .transpose(1, 2, 0, 3)
        .astype(jnp.float32)
    )
    scaled_grad = (grad_float / denominator[..., None]).astype(jnp.bfloat16)
    shift_term = jnp.sum(grad_float * attn_full, axis=-1) / denominator
    start_back = (
        jnp.zeros((key_value_local, heads_per_group, query_rows, HEAD_DIM), jnp.float32),
        jnp.zeros((seq_rows, key_value_local * HEAD_DIM), jnp.float32),
        jnp.zeros((seq_rows, key_value_local * HEAD_DIM), jnp.float32),
    )
    fold_state = start_back

    def block_step(running, block_item):
        query_acc, key_acc, value_acc = running
        key_block, value_block, key_start = block_item
        block_rows = key_block.shape[0]
        weights = masked_exp(key_block, key_start)
        dot_grad = jnp.einsum(
            "kgqd,jkd->kgqj", scaled_grad, value_block, preferred_element_type=jnp.float32
        )
        score_grad = (weights * (dot_grad - shift_term[..., None])).astype(jnp.bfloat16)
        query_acc = (
            query_acc
            + jnp.einsum(
                "kgqj,jkd->kgqd", score_grad, key_block, preferred_element_type=jnp.float32
            )
            * score_scale
        )
        key_part = (
            jnp.einsum(
                "kgqj,qkgd->jkd", score_grad, query_vectors, preferred_element_type=jnp.float32
            )
            * score_scale
        )
        value_part = jnp.einsum(
            "kgqj,kgqd->jkd",
            weights.astype(jnp.bfloat16),
            scaled_grad,
            preferred_element_type=jnp.float32,
        )
        key_old = lax.dynamic_slice_in_dim(key_acc, key_start, block_rows, 0)
        value_old = lax.dynamic_slice_in_dim(value_acc, key_start, block_rows, 0)
        key_acc = lax.dynamic_update_slice_in_dim(
            key_acc,
            key_old + key_part.reshape(block_rows, key_value_local * HEAD_DIM),
            key_start,
            0,
        )
        value_acc = lax.dynamic_update_slice_in_dim(
            value_acc,
            value_old + value_part.reshape(block_rows, key_value_local * HEAD_DIM),
            key_start,
            0,
        )
        return ((query_acc, key_acc, value_acc), None)

    fold_state, _ = lax.scan(
        block_step,
        fold_state,
        split_blocks(
            (
                lax.all_gather(key_local, "fsdp", axis=0, tiled=True),
                lax.all_gather(value_local, "fsdp", axis=0, tiled=True),
            )
        ),
    )
    query_acc, key_acc, value_acc = fold_state
    key_mine, value_mine = (
        lax.psum_scatter(key_acc, "fsdp", scatter_dimension=0, tiled=True),
        lax.psum_scatter(value_acc, "fsdp", scatter_dimension=0, tiled=True),
    )
    query_send_back = (
        query_acc.transpose(2, 0, 1, 3)
        .reshape(query_rows, key_value_local * heads_per_group * HEAD_DIM)
        .astype(jnp.bfloat16)
    )
    query_ret, key_returned, value_ret = (
        lax.all_to_all(query_send_back, "heads", split_axis=0, concat_axis=1, tiled=True),
        lax.all_to_all(
            key_mine.astype(jnp.bfloat16), "heads", split_axis=0, concat_axis=1, tiled=True
        ),
        lax.all_to_all(
            value_mine.astype(jnp.bfloat16), "heads", split_axis=0, concat_axis=1, tiled=True
        ),
    )
    query_lin_grad = (
        reverse_rotary(
            query_ret.astype(jnp.float32).reshape(token_rows, QUERY_HEADS, HEAD_DIM),
            cosine_lookup,
            sine_lookup,
        )
        .reshape(token_rows, QUERY_HEADS * HEAD_DIM)
        .astype(jnp.bfloat16)
    )
    key_lin_grad = (
        reverse_rotary(
            key_returned.astype(jnp.float32).reshape(token_rows, KEY_VALUE_HEADS, HEAD_DIM),
            cosine_lookup,
            sine_lookup,
        )
        .reshape(token_rows, KEY_VALUE_HEADS * HEAD_DIM)
        .astype(jnp.bfloat16)
    )
    query_full = jnp.dot(normalized_input.T, query_lin_grad, preferred_element_type=jnp.float32)
    key_full = jnp.dot(normalized_input.T, key_lin_grad, preferred_element_type=jnp.float32)
    value_full = jnp.dot(normalized_input.T, value_ret, preferred_element_type=jnp.float32)
    normed_one_grad = jnp.dot(query_lin_grad, full_query.T, preferred_element_type=jnp.float32)
    normed_one_grad = normed_one_grad + jnp.dot(
        key_lin_grad, full_key.T, preferred_element_type=jnp.float32
    )
    normed_one_grad = normed_one_grad + jnp.dot(
        value_ret, full_value.T, preferred_element_type=jnp.float32
    )
    gain_attn_full = jnp.sum(normed_one_grad * unit_one, axis=0)
    unit_one_grad = normed_one_grad * gain_attn
    grad_input = hidden_grad + scale_one * (
        unit_one_grad - unit_one * jnp.mean(unit_one_grad * unit_one, axis=-1, keepdims=True)
    )
    grad_attn_gain, grad_ffn_gain, grad_query, grad_key, grad_value, grad_out_proj, grad_router = (
        lax.psum_scatter(gain_attn_full, ("fsdp", "heads"), scatter_dimension=0, tiled=True),
        lax.psum_scatter(gain_ffn_full, ("fsdp", "heads"), scatter_dimension=0, tiled=True),
        lax.psum_scatter(query_full.astype(jnp.bfloat16), ("fsdp", "heads"), scatter_dimension=0, tiled=True),
        lax.psum_scatter(key_full.astype(jnp.bfloat16), ("fsdp", "heads"), scatter_dimension=0, tiled=True),
        lax.psum_scatter(value_full.astype(jnp.bfloat16), ("fsdp", "heads"), scatter_dimension=0, tiled=True),
        lax.psum_scatter(out_full.astype(jnp.bfloat16), ("fsdp", "heads"), scatter_dimension=0, tiled=True),
        lax.psum_scatter(router_full, ("fsdp", "heads"), scatter_dimension=0, tiled=True),
    )
    grad_query, grad_key, grad_value, grad_out_proj, grad_gate, grad_up, grad_down = (
        g.astype(jnp.float32)
        for g in (grad_query, grad_key, grad_value, grad_out_proj, grad_gate, grad_up, grad_down)
    )
    return (
        block_output,
        grad_input,
        grad_attn_gain,
        grad_ffn_gain,
        grad_query,
        grad_key,
        grad_value,
        grad_out_proj,
        grad_router,
        grad_gate,
        grad_up,
        grad_down,
    )


def solution(mesh):
    in_specs = (
        P(("fsdp", "heads"), None),
        P(),
        P(("fsdp", "heads"), None),
        P(("fsdp", "heads")),
        P(("fsdp", "heads")),
        P(("fsdp", "heads"), None),
        P(("fsdp", "heads"), None),
        P(("fsdp", "heads"), None),
        P(("fsdp", "heads"), None),
        P(("fsdp", "heads"), None),
        P(None, ("fsdp", "heads"), "tensor"),
        P(None, ("fsdp", "heads"), "tensor"),
        P(None, "tensor", ("fsdp", "heads")),
        P(("fsdp", "heads"), None),
    )
    out_specs = (
        P(("fsdp", "heads"), "tensor"),
        P(("fsdp", "heads"), None),
        P(("fsdp", "heads")),
        P(("fsdp", "heads")),
        P(("fsdp", "heads"), None),
        P(("fsdp", "heads"), None),
        P(("fsdp", "heads"), None),
        P(("fsdp", "heads"), None),
        P(("fsdp", "heads"), None),
        P(None, ("fsdp", "heads"), "tensor"),
        P(None, ("fsdp", "heads"), "tensor"),
        P(None, "tensor", ("fsdp", "heads")),
    )
    return jax.shard_map(body, mesh=mesh, in_specs=in_specs, out_specs=out_specs, check_vma=False)
```

```python
import math

import jax
import jax.numpy as jnp
from jax import lax
from jax.experimental import pallas as pl
from jax.experimental.pallas import tpu as pltpu
from jax.sharding import PartitionSpec as P

QUERY_HEADS = 24
KEY_VALUE_HEADS = 8
HEAD_DIM = 64
E = 16


norm_eps = 1e-06
score_scale = 0.015625
residual_scale = 0.22
rope_base = 10000.0


def rotary_table(token_positions, head_size):
    half_size = head_size // 2
    inverse = rope_base ** (-(jnp.arange(half_size, dtype=jnp.float32) * 2.0 / head_size))
    angles = token_positions[:, None].astype(jnp.float32) * inverse[None, :]
    return (jnp.cos(angles)[:, None, :], jnp.sin(angles)[:, None, :])


def apply_rotary(vectors, cosine_lookup, sine_lookup):
    half_size = vectors.shape[-1] // 2
    first_half = vectors[..., :half_size]
    second_half = vectors[..., half_size:]
    return jnp.concatenate(
        [
            first_half * cosine_lookup - second_half * sine_lookup,
            second_half * cosine_lookup + first_half * sine_lookup,
        ],
        axis=-1,
    )


def reverse_rotary(gradient, cosine_lookup, sine_lookup):
    half_size = gradient.shape[-1] // 2
    first_half = gradient[..., :half_size]
    second_half = gradient[..., half_size:]
    return jnp.concatenate(
        [
            first_half * cosine_lookup + second_half * sine_lookup,
            second_half * cosine_lookup - first_half * sine_lookup,
        ],
        axis=-1,
    )


def body(
    block_input,
    segments,
    routes,
    attn_gain,
    ffn_gain,
    query_weight,
    key_matrix,
    value_matrix,
    out_weight,
    router_weight,
    gate_weight,
    up_weight,
    down_weight,
    grad_output,
):
    head_count = lax.axis_size("heads")
    n_tensor = lax.axis_size("tensor")
    n_fsdp = lax.axis_size("fsdp")
    fsdp_index = lax.axis_index("fsdp")
    heads_index = lax.axis_index("heads")
    tensor_index = lax.axis_index("tensor")
    token_rows = block_input.shape[0]
    model_width = block_input.shape[1]
    query_rows = token_rows * head_count
    seq_rows = query_rows * n_fsdp
    key_value_local = KEY_VALUE_HEADS // head_count
    heads_per_group = QUERY_HEADS // KEY_VALUE_HEADS
    slice_width = model_width // n_tensor
    gathered = (
        lax.all_gather(attn_gain, ("fsdp", "heads"), axis=0, tiled=True),
        lax.all_gather(ffn_gain, ("fsdp", "heads"), axis=0, tiled=True),
        lax.all_gather(query_weight, ("fsdp", "heads"), axis=0, tiled=True),
        lax.all_gather(key_matrix, ("fsdp", "heads"), axis=0, tiled=True),
        lax.all_gather(value_matrix, ("fsdp", "heads"), axis=0, tiled=True),
        lax.all_gather(out_weight, ("fsdp", "heads"), axis=0, tiled=True),
        lax.all_gather(router_weight, ("fsdp", "heads"), axis=0, tiled=True),
        lax.all_gather(gate_weight, ("fsdp", "heads"), axis=1, tiled=True),
        lax.all_gather(up_weight, ("fsdp", "heads"), axis=1, tiled=True),
        lax.all_gather(down_weight, ("fsdp", "heads"), axis=2, tiled=True),
    )
    gain_attn = gathered[0].astype(jnp.float32)
    gain_ffn = gathered[1].astype(jnp.float32)
    full_query, full_key, full_value, full_out, full_router, full_gate, full_up, full_down = (
        gathered[2:]
    )
    inputs = block_input.astype(jnp.float32)
    scale_one = lax.rsqrt(jnp.mean(inputs * inputs, axis=-1, keepdims=True) + norm_eps)
    unit_one = inputs * scale_one
    normalized_input = (unit_one * gain_attn).astype(jnp.bfloat16)
    query_lin = jnp.dot(normalized_input, full_query, preferred_element_type=jnp.float32)
    key_linear = jnp.dot(normalized_input, full_key, preferred_element_type=jnp.float32)
    value_lin = jnp.dot(normalized_input, full_value, preferred_element_type=jnp.float32)
    own_start = (fsdp_index * head_count + heads_index) * token_rows
    token_positions = own_start + jnp.arange(token_rows, dtype=jnp.int32)
    cosine_lookup, sine_lookup = rotary_table(token_positions, HEAD_DIM)
    query_send = (
        apply_rotary(
            query_lin.reshape(token_rows, QUERY_HEADS, HEAD_DIM), cosine_lookup, sine_lookup
        )
        .reshape(token_rows, QUERY_HEADS * HEAD_DIM)
        .astype(jnp.bfloat16)
    )
    key_send = (
        apply_rotary(
            key_linear.reshape(token_rows, KEY_VALUE_HEADS, HEAD_DIM), cosine_lookup, sine_lookup
        )
        .reshape(token_rows, KEY_VALUE_HEADS * HEAD_DIM)
        .astype(jnp.bfloat16)
    )
    value_send = value_lin.astype(jnp.bfloat16)
    query_heads, key_local, value_local = (
        lax.all_to_all(query_send, "heads", split_axis=1, concat_axis=0, tiled=True),
        lax.all_to_all(key_send, "heads", split_axis=1, concat_axis=0, tiled=True),
        lax.all_to_all(value_send, "heads", split_axis=1, concat_axis=0, tiled=True),
    )
    query_vectors = query_heads.reshape(query_rows, key_value_local, heads_per_group, HEAD_DIM)
    query_start = fsdp_index * query_rows
    query_pos = query_start + jnp.arange(query_rows, dtype=jnp.int32)
    query_seg = lax.dynamic_slice_in_dim(segments, query_start, query_rows, 0)

    def masked_exp(key_block, key_start):
        block_rows = key_block.shape[0]
        raw_scores = (
            jnp.einsum(
                "qkgd,jkd->kgqj", query_vectors, key_block, preferred_element_type=jnp.float32
            )
            * score_scale
        )
        key_pos = key_start + jnp.arange(block_rows, dtype=jnp.int32)
        key_seg = lax.dynamic_slice_in_dim(segments, key_start, block_rows, 0)
        allowed = (query_pos[:, None] >= key_pos[None, :]) & (
            query_seg[:, None] == key_seg[None, :]
        )
        return jnp.where(allowed[None, None], jnp.exp(raw_scores), 0.0)

    def split_blocks(key_piece):
        keys_piece, values_piece = key_piece
        piece_rows = keys_piece.shape[0]
        block_rows = math.gcd(piece_rows, query_rows)
        block_count = piece_rows // block_rows
        starts = jnp.arange(block_count, dtype=jnp.int32) * block_rows
        return (
            keys_piece.reshape(block_count, block_rows, key_value_local, HEAD_DIM),
            values_piece.reshape(block_count, block_rows, key_value_local, HEAD_DIM),
            starts,
        )

    start_state = (
        jnp.zeros((key_value_local, heads_per_group, query_rows), jnp.float32),
        jnp.zeros((key_value_local, heads_per_group, query_rows, HEAD_DIM), jnp.float32),
    )
    fold_state = start_state

    def block_step(running, block_item):
        denominator, numerator = running
        key_block, value_block, key_start = block_item
        weights = masked_exp(key_block, key_start)
        denominator = denominator + jnp.sum(weights, axis=-1)
        numerator = numerator + jnp.einsum(
            "kgqj,jkd->kgqd",
            weights.astype(jnp.bfloat16),
            value_block,
            preferred_element_type=jnp.float32,
        )
        return ((denominator, numerator), None)

    fold_state, _ = lax.scan(
        block_step,
        fold_state,
        split_blocks(
            (
                lax.all_gather(key_local, "fsdp", axis=0, tiled=True),
                lax.all_gather(value_local, "fsdp", axis=0, tiled=True),
            )
        ),
    )
    denominator, numerator = fold_state
    attn_full = numerator / denominator[..., None]
    attn_send = (
        attn_full.transpose(2, 0, 1, 3)
        .reshape(query_rows, key_value_local * heads_per_group * HEAD_DIM)
        .astype(jnp.bfloat16)
    )
    attn_back = lax.all_to_all(attn_send, "heads", split_axis=0, concat_axis=1, tiled=True)
    attn_proj = jnp.dot(attn_back, full_out, preferred_element_type=jnp.float32)
    hidden = inputs + residual_scale * attn_proj
    scale_two = lax.rsqrt(jnp.mean(hidden * hidden, axis=-1, keepdims=True) + norm_eps)
    unit_two = hidden * scale_two
    normed_two = (unit_two * gain_ffn).astype(jnp.bfloat16)
    logits = jnp.dot(normed_two, full_router, preferred_element_type=jnp.float32)
    onehot = (routes[:, :, None] == jnp.arange(E, dtype=jnp.int32)[None, None, :]).astype(
        jnp.float32
    )
    picked = jnp.sum(onehot * logits[:, None, :], axis=-1)
    route_probs = jax.nn.softmax(picked, axis=-1)
    combine = jnp.sum(onehot * route_probs[:, :, None], axis=1)
    gate_pre = jnp.einsum("td,edf->etf", normed_two, full_gate, preferred_element_type=jnp.float32)
    up_pre = jnp.einsum("td,edf->etf", normed_two, full_up, preferred_element_type=jnp.float32)
    sigmoid_gate = jax.nn.sigmoid(gate_pre)
    silu_gate = gate_pre * sigmoid_gate
    active = (silu_gate * up_pre).astype(jnp.bfloat16)
    expert_out = jnp.einsum("etf,efd->etd", active, full_down, preferred_element_type=jnp.float32)
    mixed_part = jnp.sum(combine.T[:, :, None] * expert_out, axis=0)
    mixed_sum = lax.psum_scatter(
        mixed_part.astype(jnp.bfloat16), "tensor", scatter_dimension=1, tiled=True
    ).astype(jnp.float32)
    hidden_mine = lax.dynamic_slice_in_dim(hidden, tensor_index * slice_width, slice_width, 1)
    block_output = hidden_mine + residual_scale * mixed_sum
    mixed_grad = residual_scale * grad_output
    expert_grad = (combine.T[:, :, None] * mixed_grad[None]).astype(jnp.bfloat16)
    combine_part = jnp.sum(expert_out * mixed_grad[None], axis=-1).T
    active_grad = jnp.einsum(
        "etd,efd->etf", expert_grad, full_down, preferred_element_type=jnp.float32
    )
    gate_grad = (
        active_grad * up_pre * sigmoid_gate * (1.0 + gate_pre * (1.0 - sigmoid_gate))
    ).astype(jnp.bfloat16)
    up_grad = (active_grad * silu_gate).astype(jnp.bfloat16)
    normed_part = jnp.einsum(
        "etf,edf->td", gate_grad, full_gate, preferred_element_type=jnp.float32
    ) + jnp.einsum("etf,edf->td", up_grad, full_up, preferred_element_type=jnp.float32)
    gate_full = jnp.einsum("td,etf->edf", normed_two, gate_grad, preferred_element_type=jnp.float32)
    up_full = jnp.einsum("td,etf->edf", normed_two, up_grad, preferred_element_type=jnp.float32)
    down_full = jnp.einsum("etf,etd->efd", active, expert_grad, preferred_element_type=jnp.float32)
    grad_gate, grad_up, grad_down = (
        lax.psum_scatter(gate_full.astype(jnp.bfloat16), ("fsdp", "heads"), scatter_dimension=1, tiled=True),
        lax.psum_scatter(up_full.astype(jnp.bfloat16), ("fsdp", "heads"), scatter_dimension=1, tiled=True),
        lax.psum_scatter(down_full.astype(jnp.bfloat16), ("fsdp", "heads"), scatter_dimension=2, tiled=True),
    )
    normed_grad, combine_grad = lax.psum((normed_part, combine_part), "tensor")
    pick_grad = jnp.sum(onehot * combine_grad[:, None, :], axis=-1)
    picked_grad = route_probs * (
        pick_grad - jnp.sum(route_probs * pick_grad, axis=-1, keepdims=True)
    )
    logit_grad = jnp.sum(onehot * picked_grad[:, :, None], axis=1).astype(jnp.bfloat16)
    router_full = jnp.dot(normed_two.T, logit_grad, preferred_element_type=jnp.float32)
    normed_grad = normed_grad + jnp.dot(
        logit_grad, full_router.T, preferred_element_type=jnp.float32
    )
    gain_ffn_full = jnp.sum(normed_grad * unit_two, axis=0)
    unit_grad = normed_grad * gain_ffn
    hidden_grad = grad_output + scale_two * (
        unit_grad - unit_two * jnp.mean(unit_grad * unit_two, axis=-1, keepdims=True)
    )
    proj_grad = (residual_scale * hidden_grad).astype(jnp.bfloat16)
    out_full = jnp.dot(attn_back.T, proj_grad, preferred_element_type=jnp.float32)
    attn_grad = jnp.dot(proj_grad, full_out.T, preferred_element_type=jnp.float32).astype(
        jnp.bfloat16
    )
    grad_heads = lax.all_to_all(attn_grad, "heads", split_axis=1, concat_axis=0, tiled=True)
    grad_float = (
        grad_heads.reshape(query_rows, key_value_local, heads_per_group, HEAD_DIM)
        .transpose(1, 2, 0, 3)
        .astype(jnp.float32)
    )
    scaled_grad = (grad_float / denominator[..., None]).astype(jnp.bfloat16)
    shift_term = jnp.sum(grad_float * attn_full, axis=-1) / denominator
    start_back = (
        jnp.zeros((key_value_local, heads_per_group, query_rows, HEAD_DIM), jnp.float32),
        jnp.zeros((seq_rows, key_value_local * HEAD_DIM), jnp.float32),
        jnp.zeros((seq_rows, key_value_local * HEAD_DIM), jnp.float32),
    )
    fold_state = start_back

    def block_step(running, block_item):
        query_acc, key_acc, value_acc = running
        key_block, value_block, key_start = block_item
        block_rows = key_block.shape[0]
        weights = masked_exp(key_block, key_start)
        dot_grad = jnp.einsum(
            "kgqd,jkd->kgqj", scaled_grad, value_block, preferred_element_type=jnp.float32
        )
        score_grad = (weights * (dot_grad - shift_term[..., None])).astype(jnp.bfloat16)
        query_acc = (
            query_acc
            + jnp.einsum(
                "kgqj,jkd->kgqd", score_grad, key_block, preferred_element_type=jnp.float32
            )
            * score_scale
        )
        key_part = (
            jnp.einsum(
                "kgqj,qkgd->jkd", score_grad, query_vectors, preferred_element_type=jnp.float32
            )
            * score_scale
        )
        value_part = jnp.einsum(
            "kgqj,kgqd->jkd",
            weights.astype(jnp.bfloat16),
            scaled_grad,
            preferred_element_type=jnp.float32,
        )
        key_old = lax.dynamic_slice_in_dim(key_acc, key_start, block_rows, 0)
        value_old = lax.dynamic_slice_in_dim(value_acc, key_start, block_rows, 0)
        key_acc = lax.dynamic_update_slice_in_dim(
            key_acc,
            key_old + key_part.reshape(block_rows, key_value_local * HEAD_DIM),
            key_start,
            0,
        )
        value_acc = lax.dynamic_update_slice_in_dim(
            value_acc,
            value_old + value_part.reshape(block_rows, key_value_local * HEAD_DIM),
            key_start,
            0,
        )
        return ((query_acc, key_acc, value_acc), None)

    fold_state, _ = lax.scan(
        block_step,
        fold_state,
        split_blocks(
            (
                lax.all_gather(key_local, "fsdp", axis=0, tiled=True),
                lax.all_gather(value_local, "fsdp", axis=0, tiled=True),
            )
        ),
    )
    query_acc, key_acc, value_acc = fold_state
    key_mine, value_mine = (
        lax.psum_scatter(key_acc, "fsdp", scatter_dimension=0, tiled=True),
        lax.psum_scatter(value_acc, "fsdp", scatter_dimension=0, tiled=True),
    )
    query_send_back = (
        query_acc.transpose(2, 0, 1, 3)
        .reshape(query_rows, key_value_local * heads_per_group * HEAD_DIM)
        .astype(jnp.bfloat16)
    )
    query_ret, key_returned, value_ret = (
        lax.all_to_all(query_send_back, "heads", split_axis=0, concat_axis=1, tiled=True),
        lax.all_to_all(
            key_mine.astype(jnp.bfloat16), "heads", split_axis=0, concat_axis=1, tiled=True
        ),
        lax.all_to_all(
            value_mine.astype(jnp.bfloat16), "heads", split_axis=0, concat_axis=1, tiled=True
        ),
    )
    query_lin_grad = (
        reverse_rotary(
            query_ret.astype(jnp.float32).reshape(token_rows, QUERY_HEADS, HEAD_DIM),
            cosine_lookup,
            sine_lookup,
        )
        .reshape(token_rows, QUERY_HEADS * HEAD_DIM)
        .astype(jnp.bfloat16)
    )
    key_lin_grad = (
        reverse_rotary(
            key_returned.astype(jnp.float32).reshape(token_rows, KEY_VALUE_HEADS, HEAD_DIM),
            cosine_lookup,
            sine_lookup,
        )
        .reshape(token_rows, KEY_VALUE_HEADS * HEAD_DIM)
        .astype(jnp.bfloat16)
    )
    query_full = jnp.dot(normalized_input.T, query_lin_grad, preferred_element_type=jnp.float32)
    key_full = jnp.dot(normalized_input.T, key_lin_grad, preferred_element_type=jnp.float32)
    value_full = jnp.dot(normalized_input.T, value_ret, preferred_element_type=jnp.float32)
    normed_one_grad = jnp.dot(query_lin_grad, full_query.T, preferred_element_type=jnp.float32)
    normed_one_grad = normed_one_grad + jnp.dot(
        key_lin_grad, full_key.T, preferred_element_type=jnp.float32
    )
    normed_one_grad = normed_one_grad + jnp.dot(
        value_ret, full_value.T, preferred_element_type=jnp.float32
    )
    gain_attn_full = jnp.sum(normed_one_grad * unit_one, axis=0)
    unit_one_grad = normed_one_grad * gain_attn
    grad_input = hidden_grad + scale_one * (
        unit_one_grad - unit_one * jnp.mean(unit_one_grad * unit_one, axis=-1, keepdims=True)
    )
    grad_attn_gain, grad_ffn_gain, grad_query, grad_key, grad_value, grad_out_proj, grad_router = (
        lax.psum_scatter(gain_attn_full, ("fsdp", "heads"), scatter_dimension=0, tiled=True),
        lax.psum_scatter(gain_ffn_full, ("fsdp", "heads"), scatter_dimension=0, tiled=True),
        lax.psum_scatter(query_full.astype(jnp.bfloat16), ("fsdp", "heads"), scatter_dimension=0, tiled=True),
        lax.psum_scatter(key_full.astype(jnp.bfloat16), ("fsdp", "heads"), scatter_dimension=0, tiled=True),
        lax.psum_scatter(value_full.astype(jnp.bfloat16), ("fsdp", "heads"), scatter_dimension=0, tiled=True),
        lax.psum_scatter(out_full.astype(jnp.bfloat16), ("fsdp", "heads"), scatter_dimension=0, tiled=True),
        lax.psum_scatter(router_full, ("fsdp", "heads"), scatter_dimension=0, tiled=True),
    )
    grad_query, grad_key, grad_value, grad_out_proj, grad_gate, grad_up, grad_down = (
        g.astype(jnp.float32)
        for g in (grad_query, grad_key, grad_value, grad_out_proj, grad_gate, grad_up, grad_down)
    )
    return (
        block_output,
        grad_input,
        grad_attn_gain,
        grad_ffn_gain,
        grad_query,
        grad_key,
        grad_value,
        grad_out_proj,
        grad_router,
        grad_gate,
        grad_up,
        grad_down,
    )


MESH_ID = pl.DeviceIdType.MESH
F32 = jnp.float32
BF16 = jnp.bfloat16

TB = 192
DM = 1536
TC = 384
NBLK = 8
NQ = 6
FIRST_DOC_BLOCKS = 5


def contract(left, right, left_dim, right_dim, precision=None):
    return lax.dot_general(
        left,
        right,
        (((left_dim,), (right_dim,)), ((), ())),
        preferred_element_type=F32,
        precision=precision,
    )


def rows(index):
    return pl.ds(pl.multiple_of(index * TB, TB), TB)


def cols(index):
    return pl.ds(pl.multiple_of(index * TC, 128), TC)


class Place:
    def __init__(self):
        self.z = lax.axis_index("fsdp")
        self.c = lax.axis_index("heads")
        self.t = lax.axis_index("tensor")
        self.b = 2 * self.z + self.c

    def partner(self):
        return (self.z, 1 - self.c, self.t)

    def at_z(self, z):
        return (z, self.c, self.t)

    def at_block(self, block):
        return (block // 2, block % 2, self.t)

    def peer_t(self, k):
        if k == 1:
            return self.t + 1 - 2 * (self.t % 2)
        if k == 2:
            return (self.t + 2) % 4
        return 3 - self.t

    def plane(self, k):
        return (self.z, self.c, self.peer_t(k))

    def other(self, k):
        return (self.b + k) % NBLK

    def arrival(self, i):
        if i == 0:
            return self.z + 1 - 2 * (self.z % 2)
        if i == 1:
            return 2 - self.z // 2
        return 3 - 3 * (self.z // 2)

    def forward_to(self, i):
        return 3 - self.z if i == 0 else 3 * (self.z - 1)

    def middle(self):
        return self.z * (3 - self.z) > 0


def remote(src, dst, send_sem, recv_sem, device):
    return pltpu.make_async_remote_copy(
        src_ref=src,
        dst_ref=dst,
        send_sem=send_sem,
        recv_sem=recv_sem,
        device_id=device,
        device_id_type=MESH_ID,
    )


class Pending:
    def __init__(self):
        self.items = []

    def start(self, copy, when=None):
        if when is None:
            copy.start()
        else:

            @pl.when(when)
            def _():
                copy.start()

        self.items.append((copy, when))

    def drain(self):
        for copy, when in self.items:
            if when is None:
                copy.wait_send()
            else:

                @pl.when(when)
                def _(copy=copy):
                    copy.wait_send()

        self.items = []


class LineGather:
    def __init__(self, me, pend, view, line_view, sems):
        self.me, self.pend, self.view, self.line_view = me, pend, view, line_view
        self.send, self.recv, self.psend, self.precv = sems

    def start(self):
        me = self.me
        own = self.line_view(me.b)
        self.pend.start(
            remote(own, own, self.send.at[0], self.recv.at[me.z], me.at_z(me.z + 1)), me.z < 3
        )
        self.pend.start(
            remote(own, own, self.send.at[1], self.recv.at[me.z], me.at_z(me.z - 1)), me.z > 0
        )
        whole = self.view(me.b)
        self.pend.start(
            remote(whole, whole, self.psend.at[3], self.precv.at[me.z], me.partner())
        )

    def arrive(self, i):
        me = self.me
        source = me.arrival(i)
        block = self.line_view(2 * source + me.c)
        remote(block, block, self.send.at[0], self.recv.at[source], me.partner()).wait_recv()
        self.pend.start(
            remote(
                block, block, self.send.at[2 + i], self.recv.at[source], me.at_z(me.forward_to(i))
            ),
            me.middle(),
        )
        return source, block

    def share(self, i):
        me = self.me
        source = me.arrival(i)
        whole = self.view(2 * source + me.c)
        self.pend.start(
            remote(whole, whole, self.psend.at[i], self.precv.at[source], me.partner())
        )

    def finish(self):
        me = self.me
        for source in range(4):
            whole = self.view(2 * source + (1 - me.c))
            remote(
                whole, whole, self.psend.at[0], self.precv.at[source], me.partner()
            ).wait_recv()


class FullGather(LineGather):
    def __init__(self, me, pend, buffer, sems):
        super().__init__(
            me,
            pend,
            lambda block: buffer.at[rows(block), :],
            lambda block: buffer.at[rows(block), cols(me.t)],
            sems[:4],
        )
        self.buffer = buffer
        self.xsend, self.xrecv = sems[4:]

    def arrive(self, i):
        source, block = super().arrive(i)
        for k in (3, 1, 2):
            self.pend.start(
                remote(
                    block,
                    block,
                    self.xsend.at[i, k - 1],
                    self.xrecv.at[k - 1, source],
                    self.me.plane(k),
                )
            )

    def cross(self, i):
        me = self.me
        source = me.arrival(i)
        for k in (1, 2, 3):
            piece = self.buffer.at[rows(2 * source + me.c), cols(me.peer_t(k))]
            remote(
                piece, piece, self.xsend.at[i, k - 1], self.xrecv.at[k - 1, source], me.plane(k)
            ).wait_recv()
        self.share(i)


def swap_halves(u):
    lane = lax.broadcasted_iota(jnp.int32, u.shape, 1)
    return jnp.where(lane % 64 < 32, pltpu.roll(u, 96, 1), pltpu.roll(u, 32, 1))


def half_mask(half):
    lane = lax.broadcasted_iota(jnp.int32, (TB, 128), 1)
    return (lane // 64) == half


def head_from_chunk(chunk, h):
    if h % 2 != h // 3:
        chunk = pltpu.roll(chunk, 64, 1)
    return jnp.where(half_mask(h // 3), chunk, 0.0)


def chunk_from_heads(first, second, pair):
    if (2 * pair) // 3 != 0:
        first = pltpu.roll(first, 64, 1)
    if (2 * pair + 1) // 3 != 1:
        second = pltpu.roll(second, 64, 1)
    return jnp.where(half_mask(0), first, second)


def row_chunks(body, size=64):
    def step(i, carry):
        body(pl.ds(pl.multiple_of(i * size, size), size))
        return carry

    lax.fori_loop(0, TB // size, step, 0)


class Bag(dict):
    __getattr__ = dict.__getitem__


def bags(tree):
    return Bag({k: bags(v) for k, v in tree.items()}) if isinstance(tree, dict) else tree


def scratch_tree():
    def f32(*shape):
        return pltpu.VMEM(shape, F32)

    def b16(*shape):
        return pltpu.VMEM(shape, BF16)

    dma = pltpu.SemaphoreType.DMA

    def pair(*shape):
        return (dma(shape), dma(shape))

    def line():
        return (dma((5,)), dma((4,)), dma((4,)), dma((4,)))

    def full():
        return (*line(), dma((3, 3)), dma((3, 4)))

    def scatter():
        return dict(
            part=b16(DM, DM),
            core=b16(4, TB, DM),
            plane=b16(4, 3, TB, TC),
            line=b16(4, TB, TC),
            sems=(*pair(4), *pair(4, 3), *pair(4)),
        )

    def reduce(width):
        return dict(core=b16(4, TB, width), line=b16(4, TB, width), sems=(*pair(4), *pair(4)))

    return dict(
        w_qkv=b16(DM, 640),
        small=b16(NBLK, 32, 256),
        w_out=b16(DM, DM),
        d_moe=b16(DM, DM),
        hn=b16(DM, DM),
        kv=b16(DM, 256),
        w_moe=b16(DM, 768),
        comb=f32(NBLK, 16, 256),
        xn=b16(TB, DM),
        r_one=f32(TB, 1),
        r_two=f32(TB, 1),
        hidden=f32(TB, DM),
        qz=b16(NQ, TB, 128),
        oz=f32(NQ, TB, 128),
        den=f32(NQ, TB, 128),
        o_full=b16(TB, DM),
        gains=f32(8, DM),
        router_t=b16(16, DM),
        dgu=b16(DM, 512),
        cz=b16(DM, 256),
        h=scatter(),
        y=scatter(),
        dhn=b16(TB, DM),
        dc_own=f32(NBLK, 8, 256),
        dc_in=f32(NBLK, 8, 256),
        dc_plane=f32(3, NBLK, 8, 256),
        dc_t=f32(16, 256),
        g_moe=b16(DM, 768),
        dh=f32(TB, DM),
        dproj=b16(TB, DM),
        flat=f32(24, DM),
        sm=dict(own=f32(NBLK, 24, 256), inn=f32(NBLK, 24, 256)),
        sn=dict(own=f32(NBLK, 8, 256), inn=f32(NBLK, 8, 256)),
        g_out_sum=b16(TB, TC),
        dnz=b16(NQ, TB, 128),
        shift=f32(NQ, TB, 128),
        dq=f32(NQ, TB, 128),
        dkv=b16(DM, 256),
        dqkv=b16(TB, 640),
        g_qkv_sum=b16(TB, 640),
        dx=b16(TB, DM),
        dx_in=b16(3, TB, TC),
        dxn=b16(TB, DM),
        local_sem=dma((10,)),
        lg=dict(s=line(), w=line(), kv=line(), c=line()),
        fg=dict(wo=full(), dm=full(), hn=full()),
        aa=dict(wm=pair(8), gm=pair(8), dc=pair(8), sm=pair(8), sn=pair(8)),
        pl=dict(o=pair(3), dc=pair(3), dh=pair(3), go=pair(3), gq=pair(3), xs=pair(3), xg=pair(3)),
        rd=dict(go=reduce(TC), dkv=reduce(256), gq=reduce(640)),
    )


def kernel(r):
    g_out_part = r.dgu.at[:, 0:TC]
    g_qkv_part = r.w_moe.at[:, 0:640]
    me = Place()
    pend = Pending()
    z, c, t, b = me.z, me.c, me.t, me.b

    loc = r.local_sem
    local = [
        pltpu.make_async_copy(r.wq.at[:, cols(t)], r.w_qkv.at[rows(b), 0:384], loc.at[0]),
        pltpu.make_async_copy(
            r.wk.at[:, pl.ds(pl.multiple_of(128 * t, 128), 128)],
            r.w_qkv.at[rows(b), 384:512], loc.at[1],
        ),
        pltpu.make_async_copy(
            r.wv.at[:, pl.ds(pl.multiple_of(128 * t, 128), 128)],
            r.w_qkv.at[rows(b), 512:640], loc.at[2],
        ),
        pltpu.make_async_copy(r.wo, r.w_out.at[rows(b), :], loc.at[3]),
    ]
    moe_sources = []
    for which, shard in enumerate((r.gate, r.up, r.down_t)):
        for e in range(2):
            moe_sources.append((shard, e, pl.ds(256 * which + 128 * e, 128)))
    own_moe = [
        pltpu.make_async_copy(shard.at[2 * b + e], r.w_moe.at[rows(b), lanes], loc.at[4 + i])
        for i, (shard, e, lanes) in enumerate(moe_sources)
    ]
    for copy in local:
        copy.start()
    for copy in own_moe:
        copy.start()
    barrier = pltpu.get_barrier_semaphore()
    for k in range(1, NBLK):
        pl.semaphore_signal(
            barrier, inc=1, device_id=me.at_block(me.other(k)), device_id_type=MESH_ID
        )
    for k in (1, 2, 3):
        pl.semaphore_signal(barrier, inc=1, device_id=me.plane(k), device_id_type=MESH_ID)
    r.small[b] = r.small_own[...]
    r.d_moe[rows(b), :] = (residual_scale * r.gout[...]).astype(BF16)
    pl.semaphore_wait(barrier, NBLK - 1 + 3)

    def line(view, sems):
        return LineGather(me, pend, view, view, sems)

    g_small = line(lambda k: r.small.at[k], r.lg.s)
    g_qkv = line(lambda k: r.w_qkv.at[rows(k), :], r.lg.w)
    g_kv = line(lambda k: r.kv.at[rows(k), :], r.lg.kv)
    g_comb = line(lambda k: r.comb.at[k], r.lg.c)
    g_wout = FullGather(me, pend, r.w_out, r.fg.wo)
    g_dmoe = FullGather(me, pend, r.d_moe, r.fg.dm)
    g_hn = FullGather(me, pend, r.hn, r.fg.hn)

    g_small.start()
    for copy in local[:3]:
        copy.wait()
    g_qkv.start()
    local[3].wait()
    g_wout.start()
    g_dmoe.start()

    def rms_one(chunk):
        v = r.x[chunk, :].astype(F32)
        r.r_one[chunk, :] = lax.rsqrt(jnp.mean(v * v, axis=1, keepdims=True) + norm_eps)

    row_chunks(rms_one)
    for i in range(3):
        g_small.arrive(i)
        g_small.share(i)
        g_qkv.arrive(i)
        g_qkv.share(i)
        g_wout.arrive(i)
    g_small.finish()
    for k in range(NBLK):
        piece = r.small[k].astype(F32)
        r.router_t[:, TB * k : TB * (k + 1)] = piece[0:16, 0:TB].astype(BF16)
        r.gains[0:8, TB * k : TB * (k + 1)] = piece[16:24, 0:TB]

    def normalize_one(chunk):
        v = r.x[chunk, :].astype(F32)
        r.xn[chunk, :] = (v * r.r_one[chunk, :] * r.gains[0:1, :]).astype(BF16)

    row_chunks(normalize_one)
    g_qkv.finish()
    qkv = jnp.dot(r.xn[...], r.w_qkv[...], preferred_element_type=F32)
    cosine, sine = r.rope_c[...], r.rope_s[...]
    key = qkv[:, 384:512]
    r.kv[rows(b), 0:128] = (key * cosine + swap_halves(key) * sine).astype(BF16)
    r.kv[rows(b), 128:256] = qkv[:, 512:640].astype(BF16)
    g_kv.start()
    for pair in range(3):
        u = qkv[:, 128 * pair : 128 * (pair + 1)]
        u = (u * cosine + swap_halves(u) * sine).astype(BF16).astype(F32)
        r.qz[2 * pair] = head_from_chunk(u, 2 * pair).astype(BF16)
        r.qz[2 * pair + 1] = head_from_chunk(u, 2 * pair + 1).astype(BF16)
    for h in range(NQ):
        r.oz[h] = jnp.zeros((TB, 128), F32)
        r.den[h] = jnp.zeros((TB, 128), F32)
    for i in range(3):
        g_kv.arrive(i)
        g_kv.share(i)
        g_dmoe.arrive(i)

    moe_send, moe_recv = r.aa.wm
    for k in range(1, NBLK):
        peer = me.other(k)
        for shard, e, lanes in moe_sources:
            remote(
                shard.at[2 * peer + e],
                r.w_moe.at[rows(b), lanes],
                moe_send.at[k],
                moe_recv.at[b],
                me.at_block(peer),
            ).start()
    g_kv.finish()

    first_block = FIRST_DOC_BLOCKS * (b // FIRST_DOC_BLOCKS)

    def allowed(kb):
        q_pos = b * TB + lax.broadcasted_iota(jnp.int32, (TB, TB), 0)
        k_pos = kb * TB + lax.broadcasted_iota(jnp.int32, (TB, TB), 1)
        same = r.seg_q[...] == r.seg_k[pl.ds(kb, 1), 0:TB]
        return (q_pos >= k_pos) & same

    def attend(kb, carry):
        keys = r.kv[rows(kb), 0:128]
        values = r.kv[rows(kb), 128:256]
        mask = allowed(kb)
        for h in range(NQ):
            scores = contract(r.qz[h], keys, 1, 1) * score_scale
            e = jnp.where(mask, jnp.exp(scores), 0.0)
            r.den[h] += jnp.broadcast_to(jnp.sum(e, axis=1, keepdims=True), (TB, 128))
            r.oz[h] += jnp.dot(e.astype(BF16), values, preferred_element_type=F32)
        return carry

    lax.fori_loop(first_block, b + 1, attend, 0)
    for i in range(3):
        g_wout.cross(i)
    for pair in range(3):
        heads = []
        for h in (2 * pair, 2 * pair + 1):
            o = jnp.where(half_mask(h // 3), r.oz[h] / r.den[h], 0.0)
            r.oz[h] = o
            heads.append(o)
        chunk = chunk_from_heads(heads[0], heads[1], pair).astype(BF16)
        r.o_full[:, pl.ds(pl.multiple_of(TC * t + 128 * pair, 128), 128)] = chunk

    def plane_gather(sems, own_view, peer_view):
        send, recv = sems
        for k in (3, 1, 2):
            pend.start(
                remote(own_view, own_view, send.at[k - 1], recv.at[k - 1], me.plane(k))
            )

        def wait():
            for k in (1, 2, 3):
                piece = peer_view(k)
                remote(piece, piece, send.at[k - 1], recv.at[k - 1], me.plane(k)).wait_recv()

        return wait

    wait_o = plane_gather(
        r.pl.o, r.o_full.at[:, cols(t)], lambda k: r.o_full.at[:, cols(me.peer_t(k))]
    )
    g_wout.finish()
    wait_o()

    def project(n, carry):
        lanes = pl.ds(pl.multiple_of(n * 256, 256), 256)
        r.hidden[:, lanes] = r.x[:, lanes].astype(F32) + residual_scale * jnp.dot(
            r.o_full[...], r.w_out[:, lanes], preferred_element_type=F32
        )
        return carry

    lax.fori_loop(0, DM // 256, project, 0)

    def normalize_two(chunk):
        v = r.hidden[chunk, :]
        factor = lax.rsqrt(jnp.mean(v * v, axis=1, keepdims=True) + norm_eps)
        r.r_two[chunk, :] = factor
        r.dproj[chunk, :] = (v * factor * r.gains[1:2, :]).astype(BF16)

    row_chunks(normalize_two)
    r.hn[rows(b), :] = r.dproj[...]
    g_hn.start()
    logits = contract(r.router_t[...], r.dproj[...], 1, 1)
    chosen = r.mask_t[...] > 0.5
    top = jnp.max(jnp.where(chosen, logits, -1e30), axis=0, keepdims=True)
    weight = jnp.where(chosen, jnp.exp(jnp.where(chosen, logits - top, 0.0)), 0.0)
    combine = weight / jnp.sum(weight, axis=0, keepdims=True)
    r.comb[b, :, 0:TB] = combine
    g_comb.start()
    for i in range(3):
        g_dmoe.cross(i)
    for i in range(3):
        g_comb.arrive(i)
        g_comb.share(i)
        g_hn.arrive(i)
    g_dmoe.finish()
    g_comb.finish()
    for i in range(3):
        g_hn.cross(i)
    g_hn.finish()
    for copy in own_moe:
        copy.wait()
    for k in range(1, NBLK):
        peer = me.other(k)
        whole = r.w_moe.at[rows(peer), :]
        remote(whole, whole, moe_send.at[k], moe_recv.at[peer], me.partner()).wait_recv()

    lane = lax.broadcasted_iota(jnp.int32, (16, 256), 1)
    expert = lax.broadcasted_iota(jnp.int32, (16, 256), 0)
    spread = (expert == 2 * b + lane // 128).astype(F32)
    sel_row = lax.broadcasted_iota(jnp.int32, (8, 256), 0)
    sel_lane = lax.broadcasted_iota(jnp.int32, (8, 256), 1)
    select = (sel_row == sel_lane // 128).astype(F32)

    def core_copy(own, i):
        part = own.part.at[rows(2 * i + (1 - c)), :]
        return remote(part, own.core.at[i], own.sems[0].at[i], own.sems[1].at[i], me.partner())

    def plane_copy(own, i, k):
        piece = own.part.at[rows(2 * i + c), cols(me.peer_t(k))]
        return remote(
            piece,
            own.plane.at[i, k - 1],
            own.sems[2].at[i, k - 1],
            own.sems[3].at[i, k - 1],
            me.plane(k),
        )

    def line_copy(own, i):
        return remote(
            own.part.at[rows(2 * i + c), cols(t)],
            own.line.at[z],
            own.sems[4].at[i],
            own.sems[5].at[z],
            me.at_z(i),
        )

    def core_sum(own, i):
        core_copy(own, i).wait_recv()

        def add(chunk):
            where = pl.ds(pl.multiple_of((2 * i + c) * TB + chunk.start, 64), 64)
            own.part[where, :] = (
                own.part[where, :].astype(F32) + own.core[i, chunk, :].astype(F32)
            ).astype(BF16)

        row_chunks(add)
        for k in (3, 1, 2):
            plane_copy(own, i, k).start()

    def expert_block(step, carry):
        i = step % 4
        late = step // 4
        block = 2 * i + (1 - c) + late * (2 * c - 1)
        where = rows(block)
        gate_up = jnp.dot(r.hn[where, :], r.w_moe[:, 0:512], preferred_element_type=F32)
        v = jnp.dot(r.d_moe[where, :], r.w_moe[:, 512:768], preferred_element_type=F32)
        g, u = gate_up[:, 0:256], gate_up[:, 256:512]
        scale = contract(r.comb[block, :, 0:TB], spread, 0, 0, lax.Precision.HIGHEST)
        sig = 1.0 / (1.0 + jnp.exp(-g))
        silu = g * sig
        active = (silu * u).astype(BF16).astype(F32)
        r.cz[where, :] = (scale * active).astype(BF16)
        dc = contract(select, active * v, 1, 1, lax.Precision.HIGHEST)
        r.dc_own[block, :, 0:TB] = dc
        dz = scale * v
        r.dgu[where, 0:256] = (dz * u * sig * (1.0 + g * (1.0 - sig))).astype(BF16)
        r.dgu[where, 256:512] = (dz * silu).astype(BF16)
        dgu = r.dgu[where, :]
        for n in range(3):
            lanes = slice(512 * n, 512 * (n + 1))
            r.h.part[where, lanes] = contract(dgu, r.w_moe[lanes, 0:512], 1, 1).astype(BF16)

        @pl.when(late == 0)
        def _():
            core_copy(r.h, i).start()

        @pl.when(late == 1)
        def _():
            core_sum(r.h, i)

        return carry

    lax.fori_loop(0, NBLK, expert_block, 0)

    dc_send, dc_recv = r.aa.dc
    for k in range(1, NBLK):
        peer = me.other(k)
        pend.start(
            remote(
                r.dc_own.at[peer], r.dc_in.at[b], dc_send.at[k], dc_recv.at[b],
                me.at_block(peer),
            )
        )
    r.dc_in[b] = r.dc_own[b]

    def output_block(step, carry):
        i = step % 4
        late = step // 4
        block = 2 * i + (1 - c) + late * (2 * c - 1)
        where = rows(block)
        cz = r.cz[where, :]
        for n in range(3):
            lanes = slice(512 * n, 512 * (n + 1))
            r.y.part[where, lanes] = contract(cz, r.w_moe[lanes, 512:768], 1, 1).astype(BF16)

        @pl.when(late == 0)
        def _():
            core_copy(r.y, i).start()

        @pl.when(late == 1)
        def _():
            core_sum(r.y, i)

        return carry

    lax.fori_loop(0, NBLK, output_block, 0)

    def weight_grads(n, carry):
        lanes = pl.ds(pl.multiple_of(n * 256, 256), 256)
        r.g_moe[lanes, 0:512] = contract(r.hn[:, lanes], r.dgu[...], 0, 0).astype(BF16)
        r.g_moe[lanes, 512:768] = contract(r.d_moe[:, lanes], r.cz[...], 0, 0).astype(BF16)
        return carry

    lax.fori_loop(0, DM // 256, weight_grads, 0)

    def plane_sum(own):
        def step(i, carry):
            for k in (1, 2, 3):
                plane_copy(own, i, k).wait_recv()
            total = own.part[rows(2 * i + c), cols(t)].astype(F32)
            for k in range(3):
                total = total + own.plane[i, k].astype(F32)
            total = total.astype(BF16)

            @pl.when(i == z)
            def _():
                own.line[z] = total

            @pl.when(i != z)
            def _():
                own.part[rows(2 * i + c), cols(t)] = total
                line_copy(own, i).start()

            return carry

        lax.fori_loop(0, 4, step, 0)

    def line_wait(own):
        def step(i, carry):
            @pl.when(i != z)
            def _():
                there = own.line.at[i]
                remote(there, there, own.sems[4].at[i], own.sems[5].at[i], me.partner()).wait_recv()

            return carry

        lax.fori_loop(0, 4, step, 0)
        total = own.line[0].astype(F32)
        for i in range(1, 4):
            total = total + own.line[i].astype(F32)
        return total

    def scatter_drain(own):
        def step(i, carry):
            core_copy(own, i).wait_send()
            for k in (1, 2, 3):
                plane_copy(own, i, k).wait_send()

            @pl.when(i != z)
            def _():
                line_copy(own, i).wait_send()

            return carry

        lax.fori_loop(0, 4, step, 0)

    plane_sum(r.h)

    gm_send, gm_recv = r.aa.gm
    moe_targets = []
    for which, target in enumerate((r.gate_out, r.up_out, r.down_out)):
        for e in range(2):
            moe_targets.append((target, e, pl.ds(256 * which + 128 * e, 128)))
    for k in range(1, NBLK):
        peer = me.other(k)
        for target, e, lanes in moe_targets:
            remote(
                r.g_moe.at[rows(peer), lanes],
                target.at[2 * b + e],
                gm_send.at[k],
                gm_recv.at[b],
                me.at_block(peer),
            ).start()
    own_grads = [
        pltpu.make_async_copy(r.g_moe.at[rows(b), lanes], target.at[2 * b + e], loc.at[4 + i])
        for i, (target, e, lanes) in enumerate(moe_targets)
    ]
    for copy in own_grads:
        copy.start()

    for k in range(1, NBLK):
        peer = me.other(k)
        there = r.dc_in.at[peer]
        remote(there, there, dc_send.at[k], dc_recv.at[peer], me.partner()).wait_recv()
    dcp_send, dcp_recv = r.pl.dc
    dc_copies = [
        remote(
            r.dc_in, r.dc_plane.at[k - 1], dcp_send.at[k - 1], dcp_recv.at[k - 1], me.plane(k)
        )
        for k in (1, 2, 3)
    ]
    for copy in dc_copies:
        pend.start(copy)
    for copy in dc_copies:
        copy.wait_recv()
    for k in range(NBLK):
        total = r.dc_in[k] + r.dc_plane[0, k] + r.dc_plane[1, k] + r.dc_plane[2, k]
        r.dc_t[2 * k : 2 * k + 2, :] = total[0:2, :]
    dc = r.dc_t[:, 0:TB]
    combine = r.comb[b, :, 0:TB]
    d_logits = combine * (dc - jnp.sum(combine * dc, axis=0, keepdims=True))
    d_logits = d_logits.astype(BF16)
    r.flat[0:16, :] = jnp.dot(d_logits, r.hn[rows(b), :], preferred_element_type=F32)

    r.dhn[:, cols(t)] = line_wait(r.h).astype(BF16)
    plane_gather(r.pl.dh, r.dhn.at[:, cols(t)], lambda k: r.dhn.at[:, cols(me.peer_t(k))])()

    r.dh[...] = r.dhn[...].astype(F32) + contract(d_logits, r.router_t[...], 0, 0)
    r.flat[16:24, :] = jnp.zeros((8, DM), F32)

    def norm_two_back(chunk):
        dhn = r.dh[chunk, :]
        unit = r.hidden[chunk, :] * r.r_two[chunk, :]
        r.flat[16:17, :] += jnp.sum(dhn * unit, axis=0, keepdims=True)
        du = dhn * r.gains[1:2, :]
        mean = jnp.mean(du * unit, axis=1, keepdims=True)
        dh = r.gout[chunk, :] + r.r_two[chunk, :] * (du - unit * mean)
        r.dh[chunk, :] = dh
        r.dproj[chunk, :] = (residual_scale * dh).astype(BF16)

    row_chunks(norm_two_back)

    def to_owners(store, sems, width):
        send, recv = sems
        for k in range(NBLK):
            store.own[k, :, 0:TB] = r.flat[0:width, TB * k : TB * (k + 1)]
        store.inn[b] = store.own[b]
        for k in range(1, NBLK):
            peer = me.other(k)
            pend.start(
                remote(
                    store.own.at[peer], store.inn.at[b], send.at[k], recv.at[b],
                    me.at_block(peer),
                )
            )

        def wait():
            for k in range(1, NBLK):
                peer = me.other(k)
                there = store.inn.at[peer]
                remote(there, there, send.at[k], recv.at[peer], me.partner()).wait_recv()
            total = store.inn[0]
            for k in range(1, NBLK):
                total = total + store.inn[k]
            return total

        return wait

    wait_sm = to_owners(r.sm, r.aa.sm, 24)

    d_o = contract(r.dproj[...], r.w_out[cols(t), :], 1, 1).astype(BF16).astype(F32)
    for h in range(NQ):
        pair = h // 2
        dh_z = head_from_chunk(d_o[:, 128 * pair : 128 * (pair + 1)], h)
        den = r.den[h]
        r.dnz[h] = (dh_z / den).astype(BF16)
        r.shift[h] = (
            jnp.broadcast_to(jnp.sum(dh_z * r.oz[h], axis=1, keepdims=True), (TB, 128)) / den
        )
        r.dq[h] = jnp.zeros((TB, 128), F32)

    def out_grads(n, carry):
        lanes = pl.ds(pl.multiple_of(n * 256, 256), 256)
        g_out_part[lanes, :] = contract(
            r.o_full[:, lanes], r.dproj[:, cols(t)], 0, 0
        ).astype(BF16)
        return carry

    lax.fori_loop(0, DM // 256, out_grads, 0)

    class Reduce:
        def __init__(self, part, own):
            self.part, self.core, self.line, self.sems = part, own.core, own.line, own.sems

        def core_copy(self, i):
            return remote(
                self.part.at[rows(2 * i + (1 - c)), :],
                self.core.at[i],
                self.sems[0].at[i],
                self.sems[1].at[i],
                me.partner(),
            )

        def line_copy(self, i):
            return remote(
                self.part.at[rows(2 * i + c), :],
                self.line.at[z],
                self.sems[2].at[i],
                self.sems[3].at[z],
                me.at_z(i),
            )

        def start(self):
            def step(i, carry):
                self.core_copy(i).start()
                return carry

            lax.fori_loop(0, 4, step, 0)

        def middle(self):
            def step(i, carry):
                self.core_copy(i).wait_recv()
                where = rows(2 * i + c)
                total = self.part[where, :].astype(F32) + self.core[i].astype(F32)
                total = total.astype(BF16)
                self.part[where, :] = total

                @pl.when(i == z)
                def _():
                    self.line[z] = total

                @pl.when(i != z)
                def _():
                    self.line_copy(i).start()

                return carry

            lax.fori_loop(0, 4, step, 0)

        def total(self):
            def step(i, carry):
                @pl.when(i != z)
                def _():
                    there = self.line.at[i]
                    remote(
                        there, there, self.sems[2].at[i], self.sems[3].at[i], me.partner()
                    ).wait_recv()

                return carry

            lax.fori_loop(0, 4, step, 0)
            total = self.line[0].astype(F32)
            for i in range(1, 4):
                total = total + self.line[i].astype(F32)
            return total

        def drain(self):
            def step(i, carry):
                self.core_copy(i).wait_send()

                @pl.when(i != z)
                def _():
                    self.line_copy(i).wait_send()

                return carry

            lax.fori_loop(0, 4, step, 0)

    red_out = Reduce(g_out_part, r.rd.go)
    red_out.start()

    plane_sum(r.y)

    def clear(i, carry):
        r.dkv[rows(i), :] = jnp.zeros((TB, 256), BF16)
        return carry

    lax.fori_loop(0, NBLK, clear, 0)

    def attend_back(kb, carry):
        keys = r.kv[rows(kb), 0:128]
        values = r.kv[rows(kb), 128:256]
        mask = allowed(kb)
        dk = jnp.zeros((TB, 128), F32)
        dv = jnp.zeros((TB, 128), F32)
        for h in range(NQ):
            q = r.qz[h]
            dn = r.dnz[h]
            scores = contract(q, keys, 1, 1) * score_scale
            e = jnp.where(mask, jnp.exp(scores), 0.0)
            dp = contract(dn, values, 1, 1)
            ds = (e * (dp - r.shift[h][:, 0:1])).astype(BF16)
            r.dq[h] += jnp.dot(ds, keys, preferred_element_type=F32)
            dk = dk + contract(ds, q, 0, 0)
            dv = dv + contract(e.astype(BF16), dn, 0, 0)
        r.dkv[rows(kb), 0:128] = (dk * score_scale).astype(BF16)
        r.dkv[rows(kb), 128:256] = dv.astype(BF16)
        return carry

    lax.fori_loop(first_block, b + 1, attend_back, 0)
    red_kv = Reduce(r.dkv, r.rd.dkv)
    red_kv.start()
    red_out.middle()
    for pair in range(3):
        heads = [
            jnp.where(half_mask(h // 3), r.dq[h] * score_scale, 0.0)
            for h in (2 * pair, 2 * pair + 1)
        ]
        u = chunk_from_heads(heads[0], heads[1], pair).astype(BF16).astype(F32)
        r.dqkv[:, 128 * pair : 128 * (pair + 1)] = (
            u * cosine - swap_halves(u) * sine
        ).astype(BF16)
    red_kv.middle()
    r.g_out_sum[...] = red_out.total().astype(BF16)
    go_send, go_recv = r.pl.go
    own_go = pltpu.make_async_copy(r.g_out_sum, r.g_out_out.at[:, cols(t)], loc.at[0])
    own_go.start()
    for k in (3, 1, 2):
        pend.start(
            remote(
                r.g_out_sum, r.g_out_out.at[:, cols(t)], go_send.at[k - 1], go_recv.at[k - 1],
                me.plane(k),
            )
        )
    d_kv = red_kv.total().astype(BF16)
    u = d_kv[:, 0:128].astype(F32)
    r.dqkv[:, 384:512] = (u * cosine - swap_halves(u) * sine).astype(BF16)
    r.dqkv[:, 512:640] = d_kv[:, 128:256]

    for n in range(3):
        lanes = slice(512 * n, 512 * (n + 1))
        r.dx[:, lanes] = contract(r.dqkv[...], r.w_qkv[lanes, :], 1, 1).astype(BF16)
    xs_send, xs_recv = r.pl.xs
    dx_copies = [
        remote(
            r.dx.at[:, cols(me.peer_t(k))], r.dx_in.at[k - 1], xs_send.at[k - 1],
            xs_recv.at[k - 1], me.plane(k),
        )
        for k in (3, 1, 2)
    ]
    for copy in dx_copies:
        pend.start(copy)

    def qkv_grads(n, carry):
        lanes = pl.ds(pl.multiple_of(n * 256, 256), 256)
        g_qkv_part[lanes, :] = contract(r.xn[:, lanes], r.dqkv[...], 0, 0).astype(BF16)
        return carry

    lax.fori_loop(0, DM // 256, qkv_grads, 0)
    red_qkv = Reduce(g_qkv_part, r.rd.gq)
    red_qkv.start()
    for copy in dx_copies:
        copy.wait_recv()
    total = r.dx[:, cols(t)].astype(F32)
    for k in range(3):
        total = total + r.dx_in[k].astype(F32)
    r.dxn[:, cols(t)] = total.astype(BF16)
    wait_dx = plane_gather(
        r.pl.xg, r.dxn.at[:, cols(t)], lambda k: r.dxn.at[:, cols(me.peer_t(k))]
    )
    red_qkv.middle()
    r.block_out[...] = r.hidden[:, cols(t)] + residual_scale * line_wait(r.y)
    wait_dx()
    r.flat[0:8, :] = jnp.zeros((8, DM), F32)

    def norm_one_back(chunk):
        dxn = r.dxn[chunk, :].astype(F32)
        factor = r.r_one[chunk, :]
        unit = r.x[chunk, :].astype(F32) * factor
        r.flat[0:1, :] += jnp.sum(dxn * unit, axis=0, keepdims=True)
        du = dxn * r.gains[0:1, :]
        mean = jnp.mean(du * unit, axis=1, keepdims=True)
        r.grad_in[chunk, :] = r.dh[chunk, :] + factor * (du - unit * mean)

    row_chunks(norm_one_back)
    wait_sn = to_owners(r.sn, r.aa.sn, 8)
    r.g_qkv_sum[...] = red_qkv.total().astype(BF16)
    gq_send, gq_recv = r.pl.gq
    own_gq = pltpu.make_async_copy(r.g_qkv_sum, r.g_qkv_out.at[t], loc.at[1])
    own_gq.start()
    for k in (3, 1, 2):
        pend.start(
            remote(
                r.g_qkv_sum, r.g_qkv_out.at[t], gq_send.at[k - 1], gq_recv.at[k - 1],
                me.plane(k),
            )
        )
    r.sm_out[...] = wait_sm()
    r.sn_out[...] = wait_sn()

    for k in (1, 2, 3):
        there = r.g_out_out.at[:, cols(me.peer_t(k))]
        remote(there, there, go_send.at[k - 1], go_recv.at[k - 1], me.plane(k)).wait_recv()
        there = r.g_qkv_out.at[me.peer_t(k)]
        remote(there, there, gq_send.at[k - 1], gq_recv.at[k - 1], me.plane(k)).wait_recv()
    own_go.wait()
    own_gq.wait()
    for copy in own_grads:
        copy.wait()
    for k in range(1, NBLK):
        peer = me.other(k)
        whole = r.g_moe.at[rows(peer), :]
        remote(whole, whole, gm_send.at[k], gm_recv.at[peer], me.partner()).wait_recv()
        remote(whole, whole, gm_send.at[k], gm_recv.at[peer], me.partner()).wait_send()
        remote(whole, whole, moe_send.at[k], moe_recv.at[peer], me.partner()).wait_send()
    scatter_drain(r.h)
    scatter_drain(r.y)
    red_out.drain()
    red_kv.drain()
    red_qkv.drain()
    pend.drain()


def fast_body(
    block_input,
    segments,
    routes,
    attn_gain,
    ffn_gain,
    query_weight,
    key_matrix,
    value_matrix,
    out_weight,
    router_weight,
    gate_weight,
    up_weight,
    down_weight,
    grad_output,
):
    block = 2 * lax.axis_index("fsdp") + lax.axis_index("heads")
    start = block * TB
    positions = start + jnp.arange(TB, dtype=jnp.int32)
    half = HEAD_DIM // 2
    inverse = rope_base ** (-(jnp.arange(half, dtype=F32) * 2.0 / HEAD_DIM))
    angles = positions[:, None].astype(F32) * inverse[None, :]
    cosine, sine = jnp.cos(angles), jnp.sin(angles)
    rope_c = jnp.concatenate([cosine] * 4, axis=1)
    rope_s = jnp.concatenate([-sine, sine, -sine, sine], axis=1)
    seg_rows = segments.reshape(NBLK, TB)
    seg_k = jnp.pad(seg_rows, ((0, 0), (0, 256 - TB)))
    seg_q = lax.dynamic_slice_in_dim(segments, start, TB, 0)[:, None]
    mask_t = jnp.sum(
        (routes.T[:, None, :] == jnp.arange(E, dtype=jnp.int32)[None, :, None]).astype(F32), axis=0
    )
    small = jnp.concatenate(
        [router_weight.T, attn_gain[None], ffn_gain[None], jnp.zeros((14, TB), BF16)], axis=0
    )
    small = jnp.pad(small, ((0, 0), (0, 256 - TB)))
    down_t = down_weight.transpose(0, 2, 1)

    vmem, hbm = pl.BlockSpec(memory_space=pltpu.VMEM), pl.BlockSpec(memory_space=pl.ANY)
    ins = dict(
        x=(block_input, vmem), gout=(grad_output, vmem), rope_c=(rope_c, vmem),
        rope_s=(rope_s, vmem), seg_q=(seg_q, vmem), seg_k=(seg_k, vmem), mask_t=(mask_t, vmem),
        small_own=(small, vmem), wq=(query_weight, hbm), wk=(key_matrix, hbm),
        wv=(value_matrix, hbm), wo=(out_weight, hbm), gate=(gate_weight, hbm),
        up=(up_weight, hbm), down_t=(down_t, hbm),
    )
    outs = dict(
        block_out=((TB, TC), F32, vmem),
        grad_in=((TB, DM), F32, vmem),
        sm_out=((24, 256), F32, vmem),
        sn_out=((8, 256), F32, vmem),
        g_qkv_out=((4, TB, 640), BF16, hbm),
        g_out_out=((TB, DM), BF16, hbm),
        gate_out=((E, TB, 128), BF16, hbm),
        up_out=((E, TB, 128), BF16, hbm),
        down_out=((E, TB, 128), BF16, hbm),
    )
    leaves, tree = jax.tree.flatten(scratch_tree())

    def entry(*refs):
        table = bags(jax.tree.unflatten(tree, refs[len(ins) + len(outs) :]))
        table.update(zip((*ins, *outs), refs))
        kernel(table)

    results = pl.pallas_call(
        entry,
        name="layer",
        out_shape=[jax.ShapeDtypeStruct(shape, kind) for shape, kind, _ in outs.values()],
        in_specs=[spec for _, spec in ins.values()],
        out_specs=[spec for _, _, spec in outs.values()],
        scratch_shapes=leaves,
        compiler_params=pltpu.CompilerParams(
            collective_id=0, has_side_effects=True, vmem_limit_bytes=VMEM_BYTES
        ),
    )(*[value for value, _ in ins.values()])
    res = Bag(zip(outs, results))
    g_qkv = res.g_qkv_out.astype(F32).transpose(1, 0, 2)
    return (
        res.block_out,
        res.grad_in,
        res.sn_out[0, :TB],
        res.sm_out[16, :TB],
        g_qkv[:, :, 0:384].reshape(TB, DM),
        g_qkv[:, :, 384:512].reshape(TB, 512),
        g_qkv[:, :, 512:640].reshape(TB, 512),
        res.g_out_out.astype(F32),
        res.sm_out[0:16, :TB].T,
        res.gate_out.astype(F32),
        res.up_out.astype(F32),
        res.down_out.astype(F32).transpose(0, 2, 1),
    )


VMEM_BYTES = 67043328


def fits(mesh):
    return (mesh.shape["fsdp"], mesh.shape["heads"], mesh.shape["tensor"]) == (4, 2, 4)


def solution(mesh):
    in_specs = (
        P(("fsdp", "heads"), None),
        P(),
        P(("fsdp", "heads"), None),
        P(("fsdp", "heads")),
        P(("fsdp", "heads")),
        P(("fsdp", "heads"), None),
        P(("fsdp", "heads"), None),
        P(("fsdp", "heads"), None),
        P(("fsdp", "heads"), None),
        P(("fsdp", "heads"), None),
        P(None, ("fsdp", "heads"), "tensor"),
        P(None, ("fsdp", "heads"), "tensor"),
        P(None, "tensor", ("fsdp", "heads")),
        P(("fsdp", "heads"), None),
    )
    out_specs = (
        P(("fsdp", "heads"), "tensor"),
        P(("fsdp", "heads"), None),
        P(("fsdp", "heads")),
        P(("fsdp", "heads")),
        P(("fsdp", "heads"), None),
        P(("fsdp", "heads"), None),
        P(("fsdp", "heads"), None),
        P(("fsdp", "heads"), None),
        P(("fsdp", "heads"), None),
        P(None, ("fsdp", "heads"), "tensor"),
        P(None, ("fsdp", "heads"), "tensor"),
        P(None, "tensor", ("fsdp", "heads")),
    )
    chosen = fast_body if fits(mesh) else body
    return jax.shard_map(chosen, mesh=mesh, in_specs=in_specs, out_specs=out_specs, check_vma=False)
```

```python
import math

import jax
import jax.numpy as jnp
from jax import lax
from jax.experimental import pallas as pl
from jax.experimental.pallas import tpu as pltpu
from jax.sharding import PartitionSpec as P

QUERY_HEADS = 24
KEY_VALUE_HEADS = 8
HEAD_DIM = 64
E = 16


norm_eps = 1e-06
score_scale = 0.015625
residual_scale = 0.22
rope_base = 10000.0


def rotary_table(token_positions, head_size):
    half_size = head_size // 2
    inverse = rope_base ** (-(jnp.arange(half_size, dtype=jnp.float32) * 2.0 / head_size))
    angles = token_positions[:, None].astype(jnp.float32) * inverse[None, :]
    return (jnp.cos(angles)[:, None, :], jnp.sin(angles)[:, None, :])


def apply_rotary(vectors, cosine_lookup, sine_lookup):
    half_size = vectors.shape[-1] // 2
    first_half = vectors[..., :half_size]
    second_half = vectors[..., half_size:]
    return jnp.concatenate(
        [
            first_half * cosine_lookup - second_half * sine_lookup,
            second_half * cosine_lookup + first_half * sine_lookup,
        ],
        axis=-1,
    )


def reverse_rotary(gradient, cosine_lookup, sine_lookup):
    half_size = gradient.shape[-1] // 2
    first_half = gradient[..., :half_size]
    second_half = gradient[..., half_size:]
    return jnp.concatenate(
        [
            first_half * cosine_lookup + second_half * sine_lookup,
            second_half * cosine_lookup - first_half * sine_lookup,
        ],
        axis=-1,
    )


def body(
    block_input,
    segments,
    routes,
    attn_gain,
    ffn_gain,
    query_weight,
    key_matrix,
    value_matrix,
    out_weight,
    router_weight,
    gate_weight,
    up_weight,
    down_weight,
    grad_output,
):
    head_count = lax.axis_size("heads")
    n_tensor = lax.axis_size("tensor")
    n_fsdp = lax.axis_size("fsdp")
    fsdp_index = lax.axis_index("fsdp")
    heads_index = lax.axis_index("heads")
    tensor_index = lax.axis_index("tensor")
    token_rows = block_input.shape[0]
    model_width = block_input.shape[1]
    query_rows = token_rows * head_count
    seq_rows = query_rows * n_fsdp
    key_value_local = KEY_VALUE_HEADS // head_count
    heads_per_group = QUERY_HEADS // KEY_VALUE_HEADS
    slice_width = model_width // n_tensor
    gathered = (
        lax.all_gather(attn_gain, ("fsdp", "heads"), axis=0, tiled=True),
        lax.all_gather(ffn_gain, ("fsdp", "heads"), axis=0, tiled=True),
        lax.all_gather(query_weight, ("fsdp", "heads"), axis=0, tiled=True),
        lax.all_gather(key_matrix, ("fsdp", "heads"), axis=0, tiled=True),
        lax.all_gather(value_matrix, ("fsdp", "heads"), axis=0, tiled=True),
        lax.all_gather(out_weight, ("fsdp", "heads"), axis=0, tiled=True),
        lax.all_gather(router_weight, ("fsdp", "heads"), axis=0, tiled=True),
        lax.all_gather(gate_weight, ("fsdp", "heads"), axis=1, tiled=True),
        lax.all_gather(up_weight, ("fsdp", "heads"), axis=1, tiled=True),
        lax.all_gather(down_weight, ("fsdp", "heads"), axis=2, tiled=True),
    )
    gain_attn = gathered[0].astype(jnp.float32)
    gain_ffn = gathered[1].astype(jnp.float32)
    full_query, full_key, full_value, full_out, full_router, full_gate, full_up, full_down = (
        gathered[2:]
    )
    inputs = block_input.astype(jnp.float32)
    scale_one = lax.rsqrt(jnp.mean(inputs * inputs, axis=-1, keepdims=True) + norm_eps)
    unit_one = inputs * scale_one
    normalized_input = (unit_one * gain_attn).astype(jnp.bfloat16)
    query_lin = jnp.dot(normalized_input, full_query, preferred_element_type=jnp.float32)
    key_linear = jnp.dot(normalized_input, full_key, preferred_element_type=jnp.float32)
    value_lin = jnp.dot(normalized_input, full_value, preferred_element_type=jnp.float32)
    own_start = (fsdp_index * head_count + heads_index) * token_rows
    token_positions = own_start + jnp.arange(token_rows, dtype=jnp.int32)
    cosine_lookup, sine_lookup = rotary_table(token_positions, HEAD_DIM)
    query_send = (
        apply_rotary(
            query_lin.reshape(token_rows, QUERY_HEADS, HEAD_DIM), cosine_lookup, sine_lookup
        )
        .reshape(token_rows, QUERY_HEADS * HEAD_DIM)
        .astype(jnp.bfloat16)
    )
    key_send = (
        apply_rotary(
            key_linear.reshape(token_rows, KEY_VALUE_HEADS, HEAD_DIM), cosine_lookup, sine_lookup
        )
        .reshape(token_rows, KEY_VALUE_HEADS * HEAD_DIM)
        .astype(jnp.bfloat16)
    )
    value_send = value_lin.astype(jnp.bfloat16)
    query_heads, key_local, value_local = (
        lax.all_to_all(query_send, "heads", split_axis=1, concat_axis=0, tiled=True),
        lax.all_to_all(key_send, "heads", split_axis=1, concat_axis=0, tiled=True),
        lax.all_to_all(value_send, "heads", split_axis=1, concat_axis=0, tiled=True),
    )
    query_vectors = query_heads.reshape(query_rows, key_value_local, heads_per_group, HEAD_DIM)
    query_start = fsdp_index * query_rows
    query_pos = query_start + jnp.arange(query_rows, dtype=jnp.int32)
    query_seg = lax.dynamic_slice_in_dim(segments, query_start, query_rows, 0)

    def masked_exp(key_block, key_start):
        block_rows = key_block.shape[0]
        raw_scores = (
            jnp.einsum(
                "qkgd,jkd->kgqj", query_vectors, key_block, preferred_element_type=jnp.float32
            )
            * score_scale
        )
        key_pos = key_start + jnp.arange(block_rows, dtype=jnp.int32)
        key_seg = lax.dynamic_slice_in_dim(segments, key_start, block_rows, 0)
        allowed = (query_pos[:, None] >= key_pos[None, :]) & (
            query_seg[:, None] == key_seg[None, :]
        )
        return jnp.where(allowed[None, None], jnp.exp(raw_scores), 0.0)

    def split_blocks(key_piece):
        keys_piece, values_piece = key_piece
        piece_rows = keys_piece.shape[0]
        block_rows = math.gcd(piece_rows, query_rows)
        block_count = piece_rows // block_rows
        starts = jnp.arange(block_count, dtype=jnp.int32) * block_rows
        return (
            keys_piece.reshape(block_count, block_rows, key_value_local, HEAD_DIM),
            values_piece.reshape(block_count, block_rows, key_value_local, HEAD_DIM),
            starts,
        )

    start_state = (
        jnp.zeros((key_value_local, heads_per_group, query_rows), jnp.float32),
        jnp.zeros((key_value_local, heads_per_group, query_rows, HEAD_DIM), jnp.float32),
    )
    fold_state = start_state

    def block_step(running, block_item):
        denominator, numerator = running
        key_block, value_block, key_start = block_item
        weights = masked_exp(key_block, key_start)
        denominator = denominator + jnp.sum(weights, axis=-1)
        numerator = numerator + jnp.einsum(
            "kgqj,jkd->kgqd",
            weights.astype(jnp.bfloat16),
            value_block,
            preferred_element_type=jnp.float32,
        )
        return ((denominator, numerator), None)

    fold_state, _ = lax.scan(
        block_step,
        fold_state,
        split_blocks(
            (
                lax.all_gather(key_local, "fsdp", axis=0, tiled=True),
                lax.all_gather(value_local, "fsdp", axis=0, tiled=True),
            )
        ),
    )
    denominator, numerator = fold_state
    attn_full = numerator / denominator[..., None]
    attn_send = (
        attn_full.transpose(2, 0, 1, 3)
        .reshape(query_rows, key_value_local * heads_per_group * HEAD_DIM)
        .astype(jnp.bfloat16)
    )
    attn_back = lax.all_to_all(attn_send, "heads", split_axis=0, concat_axis=1, tiled=True)
    attn_proj = jnp.dot(attn_back, full_out, preferred_element_type=jnp.float32)
    hidden = inputs + residual_scale * attn_proj
    scale_two = lax.rsqrt(jnp.mean(hidden * hidden, axis=-1, keepdims=True) + norm_eps)
    unit_two = hidden * scale_two
    normed_two = (unit_two * gain_ffn).astype(jnp.bfloat16)
    logits = jnp.dot(normed_two, full_router, preferred_element_type=jnp.float32)
    onehot = (routes[:, :, None] == jnp.arange(E, dtype=jnp.int32)[None, None, :]).astype(
        jnp.float32
    )
    picked = jnp.sum(onehot * logits[:, None, :], axis=-1)
    route_probs = jax.nn.softmax(picked, axis=-1)
    combine = jnp.sum(onehot * route_probs[:, :, None], axis=1)
    gate_pre = jnp.einsum("td,edf->etf", normed_two, full_gate, preferred_element_type=jnp.float32)
    up_pre = jnp.einsum("td,edf->etf", normed_two, full_up, preferred_element_type=jnp.float32)
    sigmoid_gate = jax.nn.sigmoid(gate_pre)
    silu_gate = gate_pre * sigmoid_gate
    active = (silu_gate * up_pre).astype(jnp.bfloat16)
    expert_out = jnp.einsum("etf,efd->etd", active, full_down, preferred_element_type=jnp.float32)
    mixed_part = jnp.sum(combine.T[:, :, None] * expert_out, axis=0)
    mixed_sum = lax.psum_scatter(
        mixed_part.astype(jnp.bfloat16), "tensor", scatter_dimension=1, tiled=True
    ).astype(jnp.float32)
    hidden_mine = lax.dynamic_slice_in_dim(hidden, tensor_index * slice_width, slice_width, 1)
    block_output = hidden_mine + residual_scale * mixed_sum
    mixed_grad = residual_scale * grad_output
    expert_grad = (combine.T[:, :, None] * mixed_grad[None]).astype(jnp.bfloat16)
    combine_part = jnp.sum(expert_out * mixed_grad[None], axis=-1).T
    active_grad = jnp.einsum(
        "etd,efd->etf", expert_grad, full_down, preferred_element_type=jnp.float32
    )
    gate_grad = (
        active_grad * up_pre * sigmoid_gate * (1.0 + gate_pre * (1.0 - sigmoid_gate))
    ).astype(jnp.bfloat16)
    up_grad = (active_grad * silu_gate).astype(jnp.bfloat16)
    normed_part = jnp.einsum(
        "etf,edf->td", gate_grad, full_gate, preferred_element_type=jnp.float32
    ) + jnp.einsum("etf,edf->td", up_grad, full_up, preferred_element_type=jnp.float32)
    gate_full = jnp.einsum("td,etf->edf", normed_two, gate_grad, preferred_element_type=jnp.float32)
    up_full = jnp.einsum("td,etf->edf", normed_two, up_grad, preferred_element_type=jnp.float32)
    down_full = jnp.einsum("etf,etd->efd", active, expert_grad, preferred_element_type=jnp.float32)
    grad_gate, grad_up, grad_down = (
        lax.psum_scatter(gate_full.astype(jnp.bfloat16), ("fsdp", "heads"), scatter_dimension=1, tiled=True),
        lax.psum_scatter(up_full.astype(jnp.bfloat16), ("fsdp", "heads"), scatter_dimension=1, tiled=True),
        lax.psum_scatter(down_full.astype(jnp.bfloat16), ("fsdp", "heads"), scatter_dimension=2, tiled=True),
    )
    normed_grad, combine_grad = lax.psum((normed_part, combine_part), "tensor")
    pick_grad = jnp.sum(onehot * combine_grad[:, None, :], axis=-1)
    picked_grad = route_probs * (
        pick_grad - jnp.sum(route_probs * pick_grad, axis=-1, keepdims=True)
    )
    logit_grad = jnp.sum(onehot * picked_grad[:, :, None], axis=1).astype(jnp.bfloat16)
    router_full = jnp.dot(normed_two.T, logit_grad, preferred_element_type=jnp.float32)
    normed_grad = normed_grad + jnp.dot(
        logit_grad, full_router.T, preferred_element_type=jnp.float32
    )
    gain_ffn_full = jnp.sum(normed_grad * unit_two, axis=0)
    unit_grad = normed_grad * gain_ffn
    hidden_grad = grad_output + scale_two * (
        unit_grad - unit_two * jnp.mean(unit_grad * unit_two, axis=-1, keepdims=True)
    )
    proj_grad = (residual_scale * hidden_grad).astype(jnp.bfloat16)
    out_full = jnp.dot(attn_back.T, proj_grad, preferred_element_type=jnp.float32)
    attn_grad = jnp.dot(proj_grad, full_out.T, preferred_element_type=jnp.float32).astype(
        jnp.bfloat16
    )
    grad_heads = lax.all_to_all(attn_grad, "heads", split_axis=1, concat_axis=0, tiled=True)
    grad_float = (
        grad_heads.reshape(query_rows, key_value_local, heads_per_group, HEAD_DIM)
        .transpose(1, 2, 0, 3)
        .astype(jnp.float32)
    )
    scaled_grad = (grad_float / denominator[..., None]).astype(jnp.bfloat16)
    shift_term = jnp.sum(grad_float * attn_full, axis=-1) / denominator
    start_back = (
        jnp.zeros((key_value_local, heads_per_group, query_rows, HEAD_DIM), jnp.float32),
        jnp.zeros((seq_rows, key_value_local * HEAD_DIM), jnp.float32),
        jnp.zeros((seq_rows, key_value_local * HEAD_DIM), jnp.float32),
    )
    fold_state = start_back

    def block_step(running, block_item):
        query_acc, key_acc, value_acc = running
        key_block, value_block, key_start = block_item
        block_rows = key_block.shape[0]
        weights = masked_exp(key_block, key_start)
        dot_grad = jnp.einsum(
            "kgqd,jkd->kgqj", scaled_grad, value_block, preferred_element_type=jnp.float32
        )
        score_grad = (weights * (dot_grad - shift_term[..., None])).astype(jnp.bfloat16)
        query_acc = (
            query_acc
            + jnp.einsum(
                "kgqj,jkd->kgqd", score_grad, key_block, preferred_element_type=jnp.float32
            )
            * score_scale
        )
        key_part = (
            jnp.einsum(
                "kgqj,qkgd->jkd", score_grad, query_vectors, preferred_element_type=jnp.float32
            )
            * score_scale
        )
        value_part = jnp.einsum(
            "kgqj,kgqd->jkd",
            weights.astype(jnp.bfloat16),
            scaled_grad,
            preferred_element_type=jnp.float32,
        )
        key_old = lax.dynamic_slice_in_dim(key_acc, key_start, block_rows, 0)
        value_old = lax.dynamic_slice_in_dim(value_acc, key_start, block_rows, 0)
        key_acc = lax.dynamic_update_slice_in_dim(
            key_acc,
            key_old + key_part.reshape(block_rows, key_value_local * HEAD_DIM),
            key_start,
            0,
        )
        value_acc = lax.dynamic_update_slice_in_dim(
            value_acc,
            value_old + value_part.reshape(block_rows, key_value_local * HEAD_DIM),
            key_start,
            0,
        )
        return ((query_acc, key_acc, value_acc), None)

    fold_state, _ = lax.scan(
        block_step,
        fold_state,
        split_blocks(
            (
                lax.all_gather(key_local, "fsdp", axis=0, tiled=True),
                lax.all_gather(value_local, "fsdp", axis=0, tiled=True),
            )
        ),
    )
    query_acc, key_acc, value_acc = fold_state
    key_mine, value_mine = (
        lax.psum_scatter(key_acc, "fsdp", scatter_dimension=0, tiled=True),
        lax.psum_scatter(value_acc, "fsdp", scatter_dimension=0, tiled=True),
    )
    query_send_back = (
        query_acc.transpose(2, 0, 1, 3)
        .reshape(query_rows, key_value_local * heads_per_group * HEAD_DIM)
        .astype(jnp.bfloat16)
    )
    query_ret, key_returned, value_ret = (
        lax.all_to_all(query_send_back, "heads", split_axis=0, concat_axis=1, tiled=True),
        lax.all_to_all(
            key_mine.astype(jnp.bfloat16), "heads", split_axis=0, concat_axis=1, tiled=True
        ),
        lax.all_to_all(
            value_mine.astype(jnp.bfloat16), "heads", split_axis=0, concat_axis=1, tiled=True
        ),
    )
    query_lin_grad = (
        reverse_rotary(
            query_ret.astype(jnp.float32).reshape(token_rows, QUERY_HEADS, HEAD_DIM),
            cosine_lookup,
            sine_lookup,
        )
        .reshape(token_rows, QUERY_HEADS * HEAD_DIM)
        .astype(jnp.bfloat16)
    )
    key_lin_grad = (
        reverse_rotary(
            key_returned.astype(jnp.float32).reshape(token_rows, KEY_VALUE_HEADS, HEAD_DIM),
            cosine_lookup,
            sine_lookup,
        )
        .reshape(token_rows, KEY_VALUE_HEADS * HEAD_DIM)
        .astype(jnp.bfloat16)
    )
    query_full = jnp.dot(normalized_input.T, query_lin_grad, preferred_element_type=jnp.float32)
    key_full = jnp.dot(normalized_input.T, key_lin_grad, preferred_element_type=jnp.float32)
    value_full = jnp.dot(normalized_input.T, value_ret, preferred_element_type=jnp.float32)
    normed_one_grad = jnp.dot(query_lin_grad, full_query.T, preferred_element_type=jnp.float32)
    normed_one_grad = normed_one_grad + jnp.dot(
        key_lin_grad, full_key.T, preferred_element_type=jnp.float32
    )
    normed_one_grad = normed_one_grad + jnp.dot(
        value_ret, full_value.T, preferred_element_type=jnp.float32
    )
    gain_attn_full = jnp.sum(normed_one_grad * unit_one, axis=0)
    unit_one_grad = normed_one_grad * gain_attn
    grad_input = hidden_grad + scale_one * (
        unit_one_grad - unit_one * jnp.mean(unit_one_grad * unit_one, axis=-1, keepdims=True)
    )
    grad_attn_gain, grad_ffn_gain, grad_query, grad_key, grad_value, grad_out_proj, grad_router = (
        lax.psum_scatter(gain_attn_full, ("fsdp", "heads"), scatter_dimension=0, tiled=True),
        lax.psum_scatter(gain_ffn_full, ("fsdp", "heads"), scatter_dimension=0, tiled=True),
        lax.psum_scatter(query_full.astype(jnp.bfloat16), ("fsdp", "heads"), scatter_dimension=0, tiled=True),
        lax.psum_scatter(key_full.astype(jnp.bfloat16), ("fsdp", "heads"), scatter_dimension=0, tiled=True),
        lax.psum_scatter(value_full.astype(jnp.bfloat16), ("fsdp", "heads"), scatter_dimension=0, tiled=True),
        lax.psum_scatter(out_full.astype(jnp.bfloat16), ("fsdp", "heads"), scatter_dimension=0, tiled=True),
        lax.psum_scatter(router_full, ("fsdp", "heads"), scatter_dimension=0, tiled=True),
    )
    grad_query, grad_key, grad_value, grad_out_proj, grad_gate, grad_up, grad_down = (
        g.astype(jnp.float32)
        for g in (grad_query, grad_key, grad_value, grad_out_proj, grad_gate, grad_up, grad_down)
    )
    return (
        block_output,
        grad_input,
        grad_attn_gain,
        grad_ffn_gain,
        grad_query,
        grad_key,
        grad_value,
        grad_out_proj,
        grad_router,
        grad_gate,
        grad_up,
        grad_down,
    )


MESH_ID = pl.DeviceIdType.MESH
F32 = jnp.float32
BF16 = jnp.bfloat16

TB = 192
DM = 1536
TC = 384
NBLK = 8
NQ = 6
FIRST_DOC_BLOCKS = 5


def contract(left, right, left_dim, right_dim, precision=None):
    return lax.dot_general(
        left,
        right,
        (((left_dim,), (right_dim,)), ((), ())),
        preferred_element_type=F32,
        precision=precision,
    )


def rows(index):
    return pl.ds(pl.multiple_of(index * TB, TB), TB)


def cols(index):
    return pl.ds(pl.multiple_of(index * TC, 128), TC)


class Place:
    def __init__(self):
        self.z = lax.axis_index("fsdp")
        self.c = lax.axis_index("heads")
        self.t = lax.axis_index("tensor")
        self.b = 2 * self.z + self.c

    def partner(self):
        return (self.z, 1 - self.c, self.t)

    def at_z(self, z):
        return (z, self.c, self.t)

    def at_block(self, block):
        return (block // 2, block % 2, self.t)

    def peer_t(self, k):
        if k == 1:
            return self.t + 1 - 2 * (self.t % 2)
        if k == 2:
            return (self.t + 2) % 4
        return 3 - self.t

    def plane(self, k):
        return (self.z, self.c, self.peer_t(k))

    def other(self, k):
        return (self.b + k) % NBLK

    def arrival(self, i):
        if i == 0:
            return self.z + 1 - 2 * (self.z % 2)
        if i == 1:
            return 2 - self.z // 2
        return 3 - 3 * (self.z // 2)

    def forward_to(self, i):
        return 3 - self.z if i == 0 else 3 * (self.z - 1)

    def middle(self):
        return self.z * (3 - self.z) > 0

    def dest(self, j):
        inner = (self.z * (3 - self.z)) // 2
        turned = j + inner * (j // 2) * (1 - 2 * (j % 2))
        upper = self.z // 2
        return 3 * (1 - upper) + (2 * upper - 1) * turned


def remote(src, dst, send_sem, recv_sem, device):
    return pltpu.make_async_remote_copy(
        src_ref=src,
        dst_ref=dst,
        send_sem=send_sem,
        recv_sem=recv_sem,
        device_id=device,
        device_id_type=MESH_ID,
    )


class Pending:
    def __init__(self):
        self.items = []

    def start(self, copy, when=None):
        if when is None:
            copy.start()
        else:

            @pl.when(when)
            def _():
                copy.start()

        self.items.append((copy, when))

    def drain(self):
        for copy, when in self.items:
            if when is None:
                copy.wait_send()
            else:

                @pl.when(when)
                def _(copy=copy):
                    copy.wait_send()

        self.items = []


class LineGather:
    def __init__(self, me, pend, view, line_view, sems):
        self.me, self.pend, self.view, self.line_view = me, pend, view, line_view
        self.send, self.recv, self.psend, self.precv = sems

    def start(self):
        me = self.me
        own = self.line_view(me.b)
        self.pend.start(
            remote(own, own, self.send.at[0], self.recv.at[me.z], me.at_z(me.z + 1)), me.z < 3
        )
        self.pend.start(
            remote(own, own, self.send.at[1], self.recv.at[me.z], me.at_z(me.z - 1)), me.z > 0
        )
        whole = self.view(me.b)
        self.pend.start(
            remote(whole, whole, self.psend.at[3], self.precv.at[me.z], me.partner())
        )

    def arrive(self, i):
        me = self.me
        source = me.arrival(i)
        block = self.line_view(2 * source + me.c)
        remote(block, block, self.send.at[0], self.recv.at[source], me.partner()).wait_recv()
        self.pend.start(
            remote(
                block, block, self.send.at[2 + i], self.recv.at[source], me.at_z(me.forward_to(i))
            ),
            me.middle(),
        )
        return source, block

    def share(self, i):
        me = self.me
        source = me.arrival(i)
        whole = self.view(2 * source + me.c)
        self.pend.start(
            remote(whole, whole, self.psend.at[i], self.precv.at[source], me.partner())
        )

    def finish(self):
        me = self.me
        for source in range(4):
            whole = self.view(2 * source + (1 - me.c))
            remote(
                whole, whole, self.psend.at[0], self.precv.at[source], me.partner()
            ).wait_recv()


class UpGather(LineGather):
    def start(self):
        me = self.me
        own = self.view(me.b)
        self.pend.start(
            remote(own, own, self.send.at[0], self.recv.at[me.z], me.at_z(me.z + 1)),
            me.z < 2 + me.c,
        )
        self.pend.start(remote(own, own, self.psend.at[3], self.precv.at[me.z], me.partner()))

    def near(self, core):
        return self.me.z * (3 + core - self.me.z) > 0

    def take(self, source):
        block = self.view(2 * source + self.me.c)
        remote(
            block, block, self.send.at[0], self.recv.at[source], self.me.partner()
        ).wait_recv()
        return block

    def relay(self):
        me = self.me

        @pl.when(self.near(me.c))
        def _():
            self.take(me.z - 1)

        block = self.view(2 * (me.z - 1) + me.c)
        self.pend.start(
            remote(block, block, self.send.at[1], self.recv.at[me.z - 1], me.at_z(me.z + 1)),
            me.z == 1,
        )
        self.pend.start(
            remote(block, block, self.psend.at[0], self.precv.at[me.z - 1], me.partner()),
            self.near(me.c),
        )

        @pl.when(me.z == 2)
        def _():
            self.take(0)

        block = self.view(me.c)
        self.pend.start(
            remote(block, block, self.psend.at[1], self.precv.at[0], me.partner()), me.z == 2
        )

    def finish(self):
        me = self.me

        def take(source):
            block = self.view(2 * source + (1 - me.c))
            remote(
                block, block, self.psend.at[0], self.precv.at[source], me.partner()
            ).wait_recv()

        take(me.z)

        @pl.when(self.near(1 - me.c))
        def _():
            take(me.z - 1)

        @pl.when(me.z == 2)
        def _():
            take(0)


class FullGather(LineGather):
    def __init__(self, me, pend, buffer, sems):
        super().__init__(
            me,
            pend,
            lambda block: buffer.at[rows(block), :],
            lambda block: buffer.at[rows(block), cols(me.t)],
            sems[:4],
        )
        self.buffer = buffer
        self.xsend, self.xrecv = sems[4:]

    def spread(self, i):
        source = self.me.arrival(i)
        block = self.line_view(2 * source + self.me.c)
        for k in (3, 1, 2):
            self.pend.start(
                remote(
                    block,
                    block,
                    self.xsend.at[i, k - 1],
                    self.xrecv.at[k - 1, source],
                    self.me.plane(k),
                )
            )

    def cross(self, i):
        me = self.me
        source = me.arrival(i)
        for k in (1, 2, 3):
            piece = self.buffer.at[rows(2 * source + me.c), cols(me.peer_t(k))]
            remote(
                piece, piece, self.xsend.at[i, k - 1], self.xrecv.at[k - 1, source], me.plane(k)
            ).wait_recv()
        self.share(i)


def swap_halves(u):
    lane = lax.broadcasted_iota(jnp.int32, u.shape, 1)
    return jnp.where(lane % 64 < 32, pltpu.roll(u, 96, 1), pltpu.roll(u, 32, 1))


def half_mask(half):
    lane = lax.broadcasted_iota(jnp.int32, (TB, 128), 1)
    return (lane // 64) == half


def head_from_chunk(chunk, h):
    if h % 2 != h // 3:
        chunk = pltpu.roll(chunk, 64, 1)
    return jnp.where(half_mask(h // 3), chunk, 0.0)


def chunk_from_heads(first, second, pair):
    if (2 * pair) // 3 != 0:
        first = pltpu.roll(first, 64, 1)
    if (2 * pair + 1) // 3 != 1:
        second = pltpu.roll(second, 64, 1)
    return jnp.where(half_mask(0), first, second)


def row_chunks(body, size=64):
    def step(i, carry):
        body(pl.ds(pl.multiple_of(i * size, size), size))
        return carry

    lax.fori_loop(0, TB // size, step, 0)


class Bag(dict):
    __getattr__ = dict.__getitem__


def bags(tree):
    return Bag({k: bags(v) for k, v in tree.items()}) if isinstance(tree, dict) else tree


def scratch_tree():
    def f32(*shape):
        return pltpu.VMEM(shape, F32)

    def b16(*shape):
        return pltpu.VMEM(shape, BF16)

    dma = pltpu.SemaphoreType.DMA

    def pair(*shape):
        return (dma(shape), dma(shape))

    def line():
        return (dma((5,)), dma((4,)), dma((4,)), dma((4,)))

    def full():
        return (*line(), dma((3, 3)), dma((3, 4)))

    def scatter():
        return dict(
            part=b16(DM, DM),
            core=b16(4, TB, DM),
            plane=b16(4, 3, TB, TC),
            line=b16(6, TB, TC),
            sems=(*pair(4), *pair(4, 3), dma((3,)), dma((6,))),
        )

    def reduce(width):
        return dict(
            core=b16(4, TB, width), line=b16(6, TB, width), sems=(*pair(4), dma((3,)), dma((6,)))
        )

    return dict(
        w_qkv=b16(DM, 640),
        small=b16(NBLK, 32, 256),
        w_out=b16(DM, DM),
        d_moe=b16(DM, DM),
        hn=b16(DM, DM),
        kv=b16(DM, 256),
        w_moe=b16(DM, 768),
        comb=f32(NBLK, 16, 256),
        xn=b16(TB, DM),
        r_one=f32(TB, 1),
        r_two=f32(TB, 1),
        hidden=f32(TB, DM),
        qz=b16(NQ, TB, 128),
        oz=f32(NQ, TB, 128),
        den=f32(NQ, TB, 128),
        o_full=b16(TB, DM),
        gains=f32(8, DM),
        router_t=b16(16, DM),
        dgu=b16(DM, 512),
        cz=b16(DM, 256),
        h=scatter(),
        y=scatter(),
        dhn=b16(TB, DM),
        dc_own=f32(NBLK, 8, 256),
        dc_in=f32(NBLK, 8, 256),
        dc_plane=f32(3, NBLK, 8, 256),
        dc_t=f32(16, 256),
        g_moe=b16(DM, 768),
        acc=f32(TB, 640),
        dh=f32(TB, DM),
        dproj=b16(TB, DM),
        flat=f32(24, DM),
        sm=dict(own=f32(NBLK, 24, 256), inn=f32(NBLK, 24, 256)),
        sn=dict(own=f32(NBLK, 8, 256), inn=f32(NBLK, 8, 256)),
        g_out_sum=b16(TB, TC),
        dnz=b16(NQ, TB, 128),
        shift=f32(NQ, TB, 128),
        dq=f32(NQ, TB, 128),
        dkv=b16(DM, 256),
        dqkv=b16(TB, 640),
        g_qkv_sum=b16(TB, 640),
        dx=b16(TB, DM),
        dx_in=b16(3, TB, TC),
        dxn=b16(TB, DM),
        local_sem=dma((10,)),
        lg=dict(s=line(), w=line(), v=line(), kv=line(), c=line()),
        fg=dict(wo=full(), dm=full(), hn=full()),
        aa=dict(wm=[pair(8), pair(8)], gm=[pair(8), pair(8)], dc=pair(8), sm=pair(8), sn=pair(8)),
        pl=dict(o=pair(3), dc=pair(3), dh=pair(3), go=pair(3), gq=pair(3), xs=pair(3), xg=pair(3)),
        rd=dict(go=reduce(TC), dkv=reduce(256), gq=reduce(640)),
    )


def kernel(r):
    g_out_part = r.dgu.at[:, 0:TC]
    g_qkv_part = r.w_moe.at[:, 0:640]
    me = Place()
    pend = Pending()
    z, c, t, b = me.z, me.c, me.t, me.b

    loc = r.local_sem
    local = [
        pltpu.make_async_copy(r.wq.at[:, cols(t)], r.w_qkv.at[rows(b), 0:384], loc.at[0]),
        pltpu.make_async_copy(
            r.wk.at[:, pl.ds(pl.multiple_of(128 * t, 128), 128)],
            r.w_qkv.at[rows(b), 384:512], loc.at[1],
        ),
        pltpu.make_async_copy(
            r.wv.at[:, pl.ds(pl.multiple_of(128 * t, 128), 128)],
            r.w_qkv.at[rows(b), 512:640], loc.at[2],
        ),
        pltpu.make_async_copy(r.wo, r.w_out.at[rows(b), :], loc.at[3]),
    ]
    moe_lanes = [[pl.ds(384 * e + 128 * which, 128) for which in range(3)] for e in range(2)]
    moe_sources = [list(zip((r.gate, r.up, r.down_t), lanes)) for lanes in moe_lanes]
    own_moe = [
        pltpu.make_async_copy(
            shard.at[2 * b + e], r.w_moe.at[rows(b), lanes], loc.at[4 + 3 * e + i]
        )
        for e in range(2)
        for i, (shard, lanes) in enumerate(moe_sources[e])
    ]
    for copy in local:
        copy.start()
    for copy in own_moe:
        copy.start()
    barrier = pltpu.get_barrier_semaphore()
    for k in range(1, NBLK):
        pl.semaphore_signal(
            barrier, inc=1, device_id=me.at_block(me.other(k)), device_id_type=MESH_ID
        )
    for k in (1, 2, 3):
        pl.semaphore_signal(barrier, inc=1, device_id=me.plane(k), device_id_type=MESH_ID)
    r.small[b] = r.small_own[...]
    r.d_moe[rows(b), :] = (residual_scale * r.gout[...]).astype(BF16)
    pl.semaphore_wait(barrier, NBLK - 1 + 3)

    def line(view, sems):
        return LineGather(me, pend, view, view, sems)

    g_small = line(lambda k: r.small.at[k], r.lg.s)
    def half(h):
        return lambda k: r.w_qkv.at[pl.ds(pl.multiple_of(TB * k + 96 * h, 96), 96), :]

    g_qkv = [line(half(h), sems) for h, sems in enumerate((r.lg.w, r.lg.v))]
    kv_view = lambda k: r.kv.at[rows(k), :]
    g_kv = UpGather(me, pend, kv_view, kv_view, r.lg.kv)
    g_comb = line(lambda k: r.comb.at[k], r.lg.c)
    g_wout = FullGather(me, pend, r.w_out, r.fg.wo)
    g_dmoe = FullGather(me, pend, r.d_moe, r.fg.dm)
    g_hn = FullGather(me, pend, r.hn, r.fg.hn)

    def send_weights(e, ks):
        send, recv = r.aa.wm[e]
        for k in ks:
            peer = me.other(k)
            for shard, lanes in moe_sources[e]:
                remote(
                    shard.at[2 * peer + e],
                    r.w_moe.at[rows(b), lanes],
                    send.at[k],
                    recv.at[b],
                    me.at_block(peer),
                ).start()

    def weights_from(e, k):
        send, recv = r.aa.wm[e]
        peer = me.other(k)
        whole = r.w_moe.at[rows(peer), pl.ds(384 * e, 384)]
        return remote(whole, whole, send.at[k], recv.at[peer], me.partner())

    g_small.start()
    for copy in local[:3]:
        copy.wait()
    for g in g_qkv:
        g.start()
    local[3].wait()
    g_wout.start()

    def rms_one(chunk):
        v = r.x[chunk, :].astype(F32)
        r.r_one[chunk, :] = lax.rsqrt(jnp.mean(v * v, axis=1, keepdims=True) + norm_eps)

    row_chunks(rms_one)
    for i in range(3):
        g_small.arrive(i)
        g_small.share(i)
        for g in g_qkv:
            g.arrive(i)
            g.share(i)
        if i == 1:
            g_wout.arrive(0)
            g_wout.spread(0)
    g_small.finish()
    for k in range(NBLK):
        piece = r.small[k].astype(F32)
        r.router_t[:, TB * k : TB * (k + 1)] = piece[0:16, 0:TB].astype(BF16)
        r.gains[0:8, TB * k : TB * (k + 1)] = piece[16:24, 0:TB]

    def normalize_one(chunk):
        v = r.x[chunk, :].astype(F32)
        r.xn[chunk, :] = (v * r.r_one[chunk, :] * r.gains[0:1, :]).astype(BF16)

    row_chunks(normalize_one)
    for g in g_qkv:
        g.finish()
    qkv = jnp.dot(r.xn[...], r.w_qkv[...], preferred_element_type=F32)
    cosine, sine = r.rope_c[...], r.rope_s[...]
    key = qkv[:, 384:512]
    r.kv[rows(b), 0:128] = (key * cosine + swap_halves(key) * sine).astype(BF16)
    r.kv[rows(b), 128:256] = qkv[:, 512:640].astype(BF16)
    g_kv.start()
    for pair in range(3):
        u = qkv[:, 128 * pair : 128 * (pair + 1)]
        u = (u * cosine + swap_halves(u) * sine).astype(BF16).astype(F32)
        r.qz[2 * pair] = head_from_chunk(u, 2 * pair).astype(BF16)
        r.qz[2 * pair + 1] = head_from_chunk(u, 2 * pair + 1).astype(BF16)
    for h in range(NQ):
        r.oz[h] = jnp.zeros((TB, 128), F32)
        r.den[h] = jnp.zeros((TB, 128), F32)
    g_kv.relay()
    for i in (1, 2):
        g_wout.arrive(i)
        g_wout.spread(i)
    g_dmoe.start()
    send_weights(0, (1, 7, 2))

    g_kv.finish()

    first_block = FIRST_DOC_BLOCKS * (b // FIRST_DOC_BLOCKS)

    def allowed(kb):
        q_pos = b * TB + lax.broadcasted_iota(jnp.int32, (TB, TB), 0)
        k_pos = kb * TB + lax.broadcasted_iota(jnp.int32, (TB, TB), 1)
        same = r.seg_q[...] == r.seg_k[pl.ds(kb, 1), 0:TB]
        return (q_pos >= k_pos) & same

    def attend(kb, carry):
        keys = r.kv[rows(kb), 0:128]
        values = r.kv[rows(kb), 128:256]
        mask = allowed(kb)
        for h in range(NQ):
            scores = contract(r.qz[h], keys, 1, 1) * score_scale
            e = jnp.where(mask, jnp.exp(scores), 0.0)
            r.den[h] += jnp.broadcast_to(jnp.sum(e, axis=1, keepdims=True), (TB, 128))
            r.oz[h] += jnp.dot(e.astype(BF16), values, preferred_element_type=F32)
        return carry

    lax.fori_loop(first_block, b + 1, attend, 0)
    for pair in range(3):
        heads = []
        for h in (2 * pair, 2 * pair + 1):
            o = jnp.where(half_mask(h // 3), r.oz[h] / r.den[h], 0.0)
            r.oz[h] = o
            heads.append(o)
        chunk = chunk_from_heads(heads[0], heads[1], pair).astype(BF16)
        r.o_full[:, pl.ds(pl.multiple_of(TC * t + 128 * pair, 128), 128)] = chunk

    def plane_gather(sems, own_view, peer_view):
        send, recv = sems
        for k in (3, 1, 2):
            pend.start(
                remote(own_view, own_view, send.at[k - 1], recv.at[k - 1], me.plane(k))
            )

        def wait():
            for k in (1, 2, 3):
                piece = peer_view(k)
                remote(piece, piece, send.at[k - 1], recv.at[k - 1], me.plane(k)).wait_recv()

        return wait

    wait_o = plane_gather(
        r.pl.o, r.o_full.at[:, cols(t)], lambda k: r.o_full.at[:, cols(me.peer_t(k))]
    )
    for i in range(3):
        g_dmoe.arrive(i)
        g_dmoe.spread(i)
    send_weights(0, (6,))
    for i in range(3):
        g_wout.cross(i)
    g_wout.finish()
    wait_o()

    def project(n, carry):
        lanes = pl.ds(pl.multiple_of(n * 256, 256), 256)
        r.hidden[:, lanes] = r.x[:, lanes].astype(F32) + residual_scale * jnp.dot(
            r.o_full[...], r.w_out[:, lanes], preferred_element_type=F32
        )
        return carry

    lax.fori_loop(0, DM // 256, project, 0)

    def normalize_two(chunk):
        v = r.hidden[chunk, :]
        factor = lax.rsqrt(jnp.mean(v * v, axis=1, keepdims=True) + norm_eps)
        r.r_two[chunk, :] = factor
        r.dproj[chunk, :] = (v * factor * r.gains[1:2, :]).astype(BF16)

    row_chunks(normalize_two)
    r.hn[rows(b), :] = r.dproj[...]
    g_hn.start()
    logits = contract(r.router_t[...], r.dproj[...], 1, 1)
    chosen = r.mask_t[...] > 0.5
    top = jnp.max(jnp.where(chosen, logits, -1e30), axis=0, keepdims=True)
    weight = jnp.where(chosen, jnp.exp(jnp.where(chosen, logits - top, 0.0)), 0.0)
    combine = weight / jnp.sum(weight, axis=0, keepdims=True)
    r.comb[b, :, 0:TB] = combine
    g_comb.start()
    for i in range(3):
        g_hn.arrive(i)
        g_hn.spread(i)
        g_comb.arrive(i)
        g_comb.share(i)
        send_weights(0, (3 + i,))
    send_weights(1, (4, 3, 5, 2, 6, 1, 7))
    for i in range(3):
        g_dmoe.cross(i)
    g_dmoe.finish()
    g_comb.finish()
    for i in range(3):
        g_hn.cross(i)
    g_hn.finish()
    for copy in own_moe:
        copy.wait()
    for k in range(1, NBLK):
        weights_from(0, k).wait_recv()

    expert = lax.broadcasted_iota(jnp.int32, (16, 128), 0)
    first_row = (lax.broadcasted_iota(jnp.int32, (8, 128), 0) == 0).astype(F32)

    def core_copy(own, i):
        part = own.part.at[rows(2 * i + (1 - c)), :]
        return remote(part, own.core.at[i], own.sems[0].at[i], own.sems[1].at[i], me.partner())

    def plane_copy(own, i, k):
        piece = own.part.at[rows(2 * i + c), cols(me.peer_t(k))]
        return remote(
            piece,
            own.plane.at[i, k - 1],
            own.sems[2].at[i, k - 1],
            own.sems[3].at[i, k - 1],
            me.plane(k),
        )

    def line_copy(own, i):
        return remote(
            own.part.at[rows(2 * i + c), cols(t)],
            own.line.at[z],
            own.sems[4].at[i],
            own.sems[5].at[z],
            me.at_z(i),
        )

    def core_sum(own, i):
        core_copy(own, i).wait_recv()

        def add(chunk):
            where = pl.ds(pl.multiple_of((2 * i + c) * TB + chunk.start, 64), 64)
            own.part[where, :] = (
                own.part[where, :].astype(F32) + own.core[i, chunk, :].astype(F32)
            ).astype(BF16)

        row_chunks(add)
        for k in (3, 1, 2):
            plane_copy(own, i, k).start()

    def expert_block(e, where, block):
        base = 384 * e
        gate_up = jnp.dot(
            r.hn[where, :], r.w_moe[:, base : base + 256], preferred_element_type=F32
        )
        v = jnp.dot(
            r.d_moe[where, :], r.w_moe[:, base + 256 : base + 384], preferred_element_type=F32
        )
        g, u = gate_up[:, 0:128], gate_up[:, 128:256]
        chosen_one = (expert == 2 * b + e).astype(F32)
        scale = contract(r.comb[block, :, 0:TB], chosen_one, 0, 0, lax.Precision.HIGHEST)
        sig = 1.0 / (1.0 + jnp.exp(-g))
        silu = g * sig
        active = (silu * u).astype(BF16).astype(F32)
        r.cz[where, 128 * e : 128 * (e + 1)] = (scale * active).astype(BF16)
        dc = contract(first_row, active * v, 1, 1, lax.Precision.HIGHEST)
        r.dc_own[block, e : e + 1, 0:TB] = dc[0:1, :]
        dz = scale * v
        r.dgu[where, 256 * e : 256 * e + 128] = (dz * u * sig * (1.0 + g * (1.0 - sig))).astype(
            BF16
        )
        r.dgu[where, 256 * e + 128 : 256 * e + 256] = (dz * silu).astype(BF16)

    def expert_one(block, carry):
        expert_block(0, rows(block), block)
        return carry

    lax.fori_loop(0, NBLK, expert_one, 0)

    def weight_grads(e):
        def step(n, carry):
            lanes = pl.ds(pl.multiple_of(n * 256, 256), 256)
            base = 384 * e
            r.g_moe[lanes, base : base + 256] = contract(
                r.hn[:, lanes], r.dgu[:, 256 * e : 256 * (e + 1)], 0, 0
            ).astype(BF16)
            r.g_moe[lanes, base + 256 : base + 384] = contract(
                r.d_moe[:, lanes], r.cz[:, 128 * e : 128 * (e + 1)], 0, 0
            ).astype(BF16)
            return carry

        lax.fori_loop(0, DM // 256, step, 0)

    moe_targets = [list(zip((r.gate_out, r.up_out, r.down_out), lanes)) for lanes in moe_lanes]

    def send_grads(e, ks):
        send, recv = r.aa.gm[e]
        for k in ks:
            peer = me.other(k)
            for target, lanes in moe_targets[e]:
                remote(
                    r.g_moe.at[rows(peer), lanes],
                    target.at[2 * b + e],
                    send.at[k],
                    recv.at[b],
                    me.at_block(peer),
                ).start()

    def grads_copy(e, k):
        send, recv = r.aa.gm[e]
        peer = me.other(k)
        whole = r.g_moe.at[rows(peer), pl.ds(384 * e, 384)]
        return remote(whole, whole, send.at[k], recv.at[peer], me.partner())

    weight_grads(0)
    send_grads(0, (1, 7, 2, 6, 3))
    for k in range(1, NBLK):
        weights_from(1, k).wait_recv()

    def expert_two(step, carry):
        i = me.dest(step % 4)
        late = step // 4
        block = 2 * i + (1 - c) + late * (2 * c - 1)
        where = rows(block)
        expert_block(1, where, block)
        for n in range(3):
            lanes = slice(512 * n, 512 * (n + 1))
            r.h.part[where, lanes] = (
                contract(r.dgu[where, 0:256], r.w_moe[lanes, 0:256], 1, 1)
                + contract(r.dgu[where, 256:512], r.w_moe[lanes, 384:640], 1, 1)
            ).astype(BF16)

        @pl.when(late == 0)
        def _():
            core_copy(r.h, i).start()

        @pl.when(late == 1)
        def _():
            core_sum(r.h, i)

        return carry

    lax.fori_loop(0, NBLK, expert_two, 0)

    dc_send, dc_recv = r.aa.dc
    for k in range(1, NBLK):
        peer = me.other(k)
        pend.start(
            remote(
                r.dc_own.at[peer], r.dc_in.at[b], dc_send.at[k], dc_recv.at[b],
                me.at_block(peer),
            )
        )
    r.dc_in[b] = r.dc_own[b]

    weight_grads(1)
    class Chain:
        def __init__(self, piece, line, send, recv, arrived):
            self.piece, self.line, self.send, self.recv = piece, line, send, recv
            self.arrived = arrived

        def copy(self, j):
            i = me.dest(j)
            upper = z // 2
            inner = (z * (3 - z)) // 2
            if j == 0:
                to, slot = z + 1 - 2 * upper, i
            elif j == 1:
                to, slot = z + 1 - 2 * upper, i + inner * (4 + upper - i)
            else:
                to, slot = i, 4 + z % 2
            return remote(
                self.piece(i), self.line.at[slot], self.send.at[j], self.recv.at[slot], me.at_z(to)
            )

        def wait_slot(self, slot):
            there = self.line.at[slot]
            remote(
                there, there, self.send.at[0], self.recv.at[slot], me.partner()
            ).wait_recv()

        def step(self, j):
            i = me.dest(j)
            self.arrived(i)

            @pl.when(me.middle())
            def _():
                self.wait_slot(i)
                piece = self.piece(i)
                piece[...] = (piece[...].astype(F32) + self.line[i].astype(F32)).astype(BF16)

            self.copy(j).start()

        def total(self, acc):
            self.arrived(z)
            acc[...] = self.piece(z)[...].astype(F32)
            for slot, there in ((4, z > 0), (5, z < 3)):

                @pl.when(there)
                def _(slot=slot):
                    self.wait_slot(slot)
                    acc[...] += self.line[slot].astype(F32)

        def drain(self):
            for j in range(3):
                self.copy(j).wait_send()

    def plane_add(own, i):
        for k in (1, 2, 3):
            plane_copy(own, i, k).wait_recv()
        where = rows(2 * i + c)
        total = own.part[where, cols(t)].astype(F32)
        for k in range(3):
            total = total + own.plane[i, k].astype(F32)
        own.part[where, cols(t)] = total.astype(BF16)

    def scatter_chain(own):
        return Chain(
            lambda i: own.part.at[rows(2 * i + c), cols(t)],
            own.line,
            own.sems[4],
            own.sems[5],
            lambda i: plane_add(own, i),
        )

    def scatter_drain(own):
        def step(i, carry):
            core_copy(own, i).wait_send()
            for k in (1, 2, 3):
                plane_copy(own, i, k).wait_send()
            return carry

        lax.fori_loop(0, 4, step, 0)

    chain_h, chain_y = scatter_chain(r.h), scatter_chain(r.y)

    own_grads = [
        pltpu.make_async_copy(
            r.g_moe.at[rows(b), lanes], target.at[2 * b + e], loc.at[4 + 3 * e + i]
        )
        for e in range(2)
        for i, (target, lanes) in enumerate(moe_targets[e])
    ]
    for copy in own_grads:
        copy.start()

    for k in range(1, NBLK):
        peer = me.other(k)
        there = r.dc_in.at[peer]
        remote(there, there, dc_send.at[k], dc_recv.at[peer], me.partner()).wait_recv()
    dcp_send, dcp_recv = r.pl.dc
    dc_copies = [
        remote(
            r.dc_in, r.dc_plane.at[k - 1], dcp_send.at[k - 1], dcp_recv.at[k - 1], me.plane(k)
        )
        for k in (1, 2, 3)
    ]
    for copy in dc_copies:
        pend.start(copy)
    def output_block(step, carry):
        i = me.dest(step % 4)
        late = step // 4
        where = rows(2 * i + (1 - c) + late * (2 * c - 1))
        cz = r.cz[where, :]
        for n in range(3):
            lanes = slice(512 * n, 512 * (n + 1))
            r.y.part[where, lanes] = (
                contract(cz[:, 0:128], r.w_moe[lanes, 256:384], 1, 1)
                + contract(cz[:, 128:256], r.w_moe[lanes, 640:768], 1, 1)
            ).astype(BF16)

        @pl.when(late == 0)
        def _():
            core_copy(r.y, i).start()

        return carry

    lax.fori_loop(0, NBLK, output_block, 0)

    for j in range(3):
        chain_h.step(j)
        send_grads(0, ((5,), (4,), ())[j])
    chain_h.total(r.acc.at[:, 0:TC])
    r.dhn[:, cols(t)] = r.acc[:, 0:TC].astype(BF16)
    send_grads(1, (1, 7, 2))
    wait_dh = plane_gather(
        r.pl.dh, r.dhn.at[:, cols(t)], lambda k: r.dhn.at[:, cols(me.peer_t(k))]
    )
    for j in range(4):
        core_sum(r.y, me.dest(j))
    for copy in dc_copies:
        copy.wait_recv()
    for k in range(NBLK):
        total = r.dc_in[k] + r.dc_plane[0, k] + r.dc_plane[1, k] + r.dc_plane[2, k]
        r.dc_t[2 * k : 2 * k + 2, :] = total[0:2, :]
    dc = r.dc_t[:, 0:TB]
    combine = r.comb[b, :, 0:TB]
    d_logits = combine * (dc - jnp.sum(combine * dc, axis=0, keepdims=True))
    d_logits = d_logits.astype(BF16)
    r.flat[0:16, :] = jnp.dot(d_logits, r.hn[rows(b), :], preferred_element_type=F32)

    wait_dh()

    r.dh[...] = r.dhn[...].astype(F32) + contract(d_logits, r.router_t[...], 0, 0)
    r.flat[16:24, :] = jnp.zeros((8, DM), F32)

    def norm_two_back(chunk):
        dhn = r.dh[chunk, :]
        unit = r.hidden[chunk, :] * r.r_two[chunk, :]
        r.flat[16:17, :] += jnp.sum(dhn * unit, axis=0, keepdims=True)
        du = dhn * r.gains[1:2, :]
        mean = jnp.mean(du * unit, axis=1, keepdims=True)
        dh = r.gout[chunk, :] + r.r_two[chunk, :] * (du - unit * mean)
        r.dh[chunk, :] = dh
        r.dproj[chunk, :] = (residual_scale * dh).astype(BF16)

    row_chunks(norm_two_back)

    def to_owners(store, sems, width):
        send, recv = sems
        for k in range(NBLK):
            store.own[k, :, 0:TB] = r.flat[0:width, TB * k : TB * (k + 1)]
        store.inn[b] = store.own[b]
        for k in range(1, NBLK):
            peer = me.other(k)
            pend.start(
                remote(
                    store.own.at[peer], store.inn.at[b], send.at[k], recv.at[b],
                    me.at_block(peer),
                )
            )

        def wait():
            for k in range(1, NBLK):
                peer = me.other(k)
                there = store.inn.at[peer]
                remote(there, there, send.at[k], recv.at[peer], me.partner()).wait_recv()
            total = store.inn[0]
            for k in range(1, NBLK):
                total = total + store.inn[k]
            return total

        return wait

    wait_sm = to_owners(r.sm, r.aa.sm, 24)

    d_o = contract(r.dproj[...], r.w_out[cols(t), :], 1, 1).astype(BF16).astype(F32)
    for h in range(NQ):
        pair = h // 2
        dh_z = head_from_chunk(d_o[:, 128 * pair : 128 * (pair + 1)], h)
        den = r.den[h]
        r.dnz[h] = (dh_z / den).astype(BF16)
        r.shift[h] = (
            jnp.broadcast_to(jnp.sum(dh_z * r.oz[h], axis=1, keepdims=True), (TB, 128)) / den
        )
        r.dq[h] = jnp.zeros((TB, 128), F32)

    def out_grads(n, carry):
        lanes = pl.ds(pl.multiple_of(n * 256, 256), 256)
        g_out_part[lanes, :] = contract(
            r.o_full[:, lanes], r.dproj[:, cols(t)], 0, 0
        ).astype(BF16)
        return carry

    lax.fori_loop(0, DM // 256, out_grads, 0)

    class Reduce(Chain):
        def __init__(self, part, own):
            self.part, self.core, self.sems = part, own.core, own.sems
            super().__init__(
                lambda i: part.at[rows(2 * i + c), :], own.line, own.sems[2], own.sems[3], self.chip
            )

        def core_copy(self, i):
            return remote(
                self.part.at[rows(2 * i + (1 - c)), :],
                self.core.at[i],
                self.sems[0].at[i],
                self.sems[1].at[i],
                me.partner(),
            )

        def start(self):
            for j in range(4):
                self.core_copy(me.dest(j)).start()

        def chip(self, i):
            self.core_copy(i).wait_recv()
            piece = self.piece(i)
            piece[...] = (piece[...].astype(F32) + self.core[i].astype(F32)).astype(BF16)

        def drain(self):
            super().drain()
            self.drain_core()

        def drain_core(self):
            for i in range(4):
                self.core_copy(i).wait_send()

        def down(self):
            for i in range(4):
                self.chip(i)

            @pl.when(z == 1)
            def _():
                self.wait_slot(0)
                piece = self.piece(0)
                piece[...] = (piece[...].astype(F32) + self.line[0].astype(F32)).astype(BF16)

            for i, slot, when in (
                (0, 0, z == 2),
                (1, 5, z == 2),
                (0, 5, z == 1),
                (2, 5, z + c == 4),
            ):
                pend.start(
                    remote(
                        self.piece(i),
                        self.line.at[slot],
                        self.send.at[1 if i == 1 else 0],
                        self.recv.at[slot],
                        me.at_z(z - 1),
                    ),
                    when,
                )

        def down_total(self, acc):
            acc[...] = self.piece(z)[...].astype(F32)

            @pl.when(z < 2 + c)
            def _():
                self.wait_slot(5)
                acc[...] += self.line[5].astype(F32)

    send_grads(1, (6, 3))
    red_out = Reduce(g_out_part, r.rd.go)
    red_out.start()

    def clear(i, carry):
        r.dkv[rows(i), :] = jnp.zeros((TB, 256), BF16)
        return carry

    lax.fori_loop(0, NBLK, clear, 0)

    def attend_back(kb, carry):
        keys = r.kv[rows(kb), 0:128]
        values = r.kv[rows(kb), 128:256]
        mask = allowed(kb)
        dk = jnp.zeros((TB, 128), F32)
        dv = jnp.zeros((TB, 128), F32)
        for h in range(NQ):
            q = r.qz[h]
            dn = r.dnz[h]
            scores = contract(q, keys, 1, 1) * score_scale
            e = jnp.where(mask, jnp.exp(scores), 0.0)
            dp = contract(dn, values, 1, 1)
            ds = (e * (dp - r.shift[h][:, 0:1])).astype(BF16)
            r.dq[h] += jnp.dot(ds, keys, preferred_element_type=F32)
            dk = dk + contract(ds, q, 0, 0)
            dv = dv + contract(e.astype(BF16), dn, 0, 0)
        r.dkv[rows(kb), 0:128] = (dk * score_scale).astype(BF16)
        r.dkv[rows(kb), 128:256] = dv.astype(BF16)
        return carry

    lax.fori_loop(first_block, b + 1, attend_back, 0)
    red_kv = Reduce(r.dkv, r.rd.dkv)
    red_kv.start()
    for pair in range(3):
        heads = [
            jnp.where(half_mask(h // 3), r.dq[h] * score_scale, 0.0)
            for h in (2 * pair, 2 * pair + 1)
        ]
        u = chunk_from_heads(heads[0], heads[1], pair).astype(BF16).astype(F32)
        r.dqkv[:, 128 * pair : 128 * (pair + 1)] = (
            u * cosine - swap_halves(u) * sine
        ).astype(BF16)
    red_kv.down()
    send_grads(1, (5,))
    for j in range(3):
        red_out.step(j)
    d_kv_acc = r.acc.at[:, 384:640]
    red_kv.down_total(d_kv_acc)
    d_kv = d_kv_acc[...].astype(BF16)
    u = d_kv[:, 0:128].astype(F32)
    r.dqkv[:, 384:512] = (u * cosine - swap_halves(u) * sine).astype(BF16)
    r.dqkv[:, 512:640] = d_kv[:, 128:256]

    for n in range(3):
        lanes = slice(512 * n, 512 * (n + 1))
        r.dx[:, lanes] = contract(r.dqkv[...], r.w_qkv[lanes, :], 1, 1).astype(BF16)
    xs_send, xs_recv = r.pl.xs
    dx_copies = [
        remote(
            r.dx.at[:, cols(me.peer_t(k))], r.dx_in.at[k - 1], xs_send.at[k - 1],
            xs_recv.at[k - 1], me.plane(k),
        )
        for k in (3, 1, 2)
    ]
    for copy in dx_copies:
        pend.start(copy)

    def qkv_grads(n, carry):
        lanes = pl.ds(pl.multiple_of(n * 256, 256), 256)
        g_qkv_part[lanes, :] = contract(r.xn[:, lanes], r.dqkv[...], 0, 0).astype(BF16)
        return carry

    lax.fori_loop(0, DM // 256, qkv_grads, 0)
    red_qkv = Reduce(g_qkv_part, r.rd.gq)
    red_qkv.start()
    for j in range(3):
        red_qkv.step(j)
    send_grads(1, (4,))
    for copy in dx_copies:
        copy.wait_recv()
    total = r.dx[:, cols(t)].astype(F32)
    for k in range(3):
        total = total + r.dx_in[k].astype(F32)
    r.dxn[:, cols(t)] = total.astype(BF16)
    wait_dx = plane_gather(
        r.pl.xg, r.dxn.at[:, cols(t)], lambda k: r.dxn.at[:, cols(me.peer_t(k))]
    )
    red_out.total(r.acc.at[:, 0:TC])
    r.g_out_sum[...] = r.acc[:, 0:TC].astype(BF16)
    go_send, go_recv = r.pl.go
    own_go = pltpu.make_async_copy(r.g_out_sum, r.g_out_out.at[:, cols(t)], loc.at[0])
    own_go.start()
    for k in (3, 1, 2):
        pend.start(
            remote(
                r.g_out_sum, r.g_out_out.at[:, cols(t)], go_send.at[k - 1], go_recv.at[k - 1],
                me.plane(k),
            )
        )
    for j in range(3):
        chain_y.step(j)
    wait_dx()
    r.flat[0:8, :] = jnp.zeros((8, DM), F32)

    def norm_one_back(chunk):
        dxn = r.dxn[chunk, :].astype(F32)
        factor = r.r_one[chunk, :]
        unit = r.x[chunk, :].astype(F32) * factor
        r.flat[0:1, :] += jnp.sum(dxn * unit, axis=0, keepdims=True)
        du = dxn * r.gains[0:1, :]
        mean = jnp.mean(du * unit, axis=1, keepdims=True)
        r.grad_in[chunk, :] = r.dh[chunk, :] + factor * (du - unit * mean)

    row_chunks(norm_one_back)
    wait_sn = to_owners(r.sn, r.aa.sn, 8)
    red_qkv.total(r.acc)
    r.g_qkv_sum[...] = r.acc[...].astype(BF16)
    gq_send, gq_recv = r.pl.gq
    own_gq = pltpu.make_async_copy(r.g_qkv_sum, r.g_qkv_out.at[t], loc.at[1])
    own_gq.start()
    for k in (3, 1, 2):
        pend.start(
            remote(
                r.g_qkv_sum, r.g_qkv_out.at[t], gq_send.at[k - 1], gq_recv.at[k - 1],
                me.plane(k),
            )
        )
    chain_y.total(r.acc.at[:, 0:TC])
    r.block_out[...] = r.hidden[:, cols(t)] + residual_scale * r.acc[:, 0:TC]
    r.sm_out[...] = wait_sm()
    r.sn_out[...] = wait_sn()

    for k in (1, 2, 3):
        there = r.g_out_out.at[:, cols(me.peer_t(k))]
        remote(there, there, go_send.at[k - 1], go_recv.at[k - 1], me.plane(k)).wait_recv()
        there = r.g_qkv_out.at[me.peer_t(k)]
        remote(there, there, gq_send.at[k - 1], gq_recv.at[k - 1], me.plane(k)).wait_recv()
    own_go.wait()
    own_gq.wait()
    for copy in own_grads:
        copy.wait()
    for k in range(1, NBLK):
        for e in range(2):
            grads_copy(e, k).wait()
            weights_from(e, k).wait_send()
    scatter_drain(r.h)
    scatter_drain(r.y)
    chain_h.drain()
    chain_y.drain()
    red_out.drain()
    red_kv.drain_core()
    red_qkv.drain()
    pend.drain()


def fast_body(
    block_input,
    segments,
    routes,
    attn_gain,
    ffn_gain,
    query_weight,
    key_matrix,
    value_matrix,
    out_weight,
    router_weight,
    gate_weight,
    up_weight,
    down_weight,
    grad_output,
):
    block = 2 * lax.axis_index("fsdp") + lax.axis_index("heads")
    start = block * TB
    positions = start + jnp.arange(TB, dtype=jnp.int32)
    half = HEAD_DIM // 2
    inverse = rope_base ** (-(jnp.arange(half, dtype=F32) * 2.0 / HEAD_DIM))
    angles = positions[:, None].astype(F32) * inverse[None, :]
    cosine, sine = jnp.cos(angles), jnp.sin(angles)
    rope_c = jnp.concatenate([cosine] * 4, axis=1)
    rope_s = jnp.concatenate([-sine, sine, -sine, sine], axis=1)
    seg_rows = segments.reshape(NBLK, TB)
    seg_k = jnp.pad(seg_rows, ((0, 0), (0, 256 - TB)))
    seg_q = lax.dynamic_slice_in_dim(segments, start, TB, 0)[:, None]
    mask_t = jnp.sum(
        (routes.T[:, None, :] == jnp.arange(E, dtype=jnp.int32)[None, :, None]).astype(F32), axis=0
    )
    small = jnp.concatenate(
        [router_weight.T, attn_gain[None], ffn_gain[None], jnp.zeros((14, TB), BF16)], axis=0
    )
    small = jnp.pad(small, ((0, 0), (0, 256 - TB)))
    down_t = down_weight.transpose(0, 2, 1)

    vmem, hbm = pl.BlockSpec(memory_space=pltpu.VMEM), pl.BlockSpec(memory_space=pl.ANY)
    ins = dict(
        x=(block_input, vmem), gout=(grad_output, vmem), rope_c=(rope_c, vmem),
        rope_s=(rope_s, vmem), seg_q=(seg_q, vmem), seg_k=(seg_k, vmem), mask_t=(mask_t, vmem),
        small_own=(small, vmem), wq=(query_weight, hbm), wk=(key_matrix, hbm),
        wv=(value_matrix, hbm), wo=(out_weight, hbm), gate=(gate_weight, hbm),
        up=(up_weight, hbm), down_t=(down_t, hbm),
    )
    outs = dict(
        block_out=((TB, TC), F32, vmem),
        grad_in=((TB, DM), F32, vmem),
        sm_out=((24, 256), F32, vmem),
        sn_out=((8, 256), F32, vmem),
        g_qkv_out=((4, TB, 640), BF16, hbm),
        g_out_out=((TB, DM), BF16, hbm),
        gate_out=((E, TB, 128), BF16, hbm),
        up_out=((E, TB, 128), BF16, hbm),
        down_out=((E, TB, 128), BF16, hbm),
    )
    leaves, tree = jax.tree.flatten(scratch_tree())

    def entry(*refs):
        table = bags(jax.tree.unflatten(tree, refs[len(ins) + len(outs) :]))
        table.update(zip((*ins, *outs), refs))
        kernel(table)

    results = pl.pallas_call(
        entry,
        name="layer",
        out_shape=[jax.ShapeDtypeStruct(shape, kind) for shape, kind, _ in outs.values()],
        in_specs=[spec for _, spec in ins.values()],
        out_specs=[spec for _, _, spec in outs.values()],
        scratch_shapes=leaves,
        compiler_params=pltpu.CompilerParams(
            collective_id=0, has_side_effects=True, vmem_limit_bytes=VMEM_BYTES
        ),
    )(*[value for value, _ in ins.values()])
    res = Bag(zip(outs, results))
    g_qkv = res.g_qkv_out.astype(F32).transpose(1, 0, 2)
    return (
        res.block_out,
        res.grad_in,
        res.sn_out[0, :TB],
        res.sm_out[16, :TB],
        g_qkv[:, :, 0:384].reshape(TB, DM),
        g_qkv[:, :, 384:512].reshape(TB, 512),
        g_qkv[:, :, 512:640].reshape(TB, 512),
        res.g_out_out.astype(F32),
        res.sm_out[0:16, :TB].T,
        res.gate_out.astype(F32),
        res.up_out.astype(F32),
        res.down_out.astype(F32).transpose(0, 2, 1),
    )


VMEM_BYTES = 67043328


def fits(mesh):
    return (mesh.shape["fsdp"], mesh.shape["heads"], mesh.shape["tensor"]) == (4, 2, 4)


def solution(mesh):
    in_specs = (
        P(("fsdp", "heads"), None),
        P(),
        P(("fsdp", "heads"), None),
        P(("fsdp", "heads")),
        P(("fsdp", "heads")),
        P(("fsdp", "heads"), None),
        P(("fsdp", "heads"), None),
        P(("fsdp", "heads"), None),
        P(("fsdp", "heads"), None),
        P(("fsdp", "heads"), None),
        P(None, ("fsdp", "heads"), "tensor"),
        P(None, ("fsdp", "heads"), "tensor"),
        P(None, "tensor", ("fsdp", "heads")),
        P(("fsdp", "heads"), None),
    )
    out_specs = (
        P(("fsdp", "heads"), "tensor"),
        P(("fsdp", "heads"), None),
        P(("fsdp", "heads")),
        P(("fsdp", "heads")),
        P(("fsdp", "heads"), None),
        P(("fsdp", "heads"), None),
        P(("fsdp", "heads"), None),
        P(("fsdp", "heads"), None),
        P(("fsdp", "heads"), None),
        P(None, ("fsdp", "heads"), "tensor"),
        P(None, ("fsdp", "heads"), "tensor"),
        P(None, "tensor", ("fsdp", "heads")),
    )
    chosen = fast_body if fits(mesh) else body
    return jax.shard_map(chosen, mesh=mesh, in_specs=in_specs, out_specs=out_specs, check_vma=False)
```

```python
import math

import jax
import jax.numpy as jnp
import numpy as np
from jax import lax
from jax.experimental import pallas as pl
from jax.experimental.pallas import tpu as pltpu
from jax.sharding import PartitionSpec as P

QUERY_HEADS = 24
KEY_VALUE_HEADS = 8
HEAD_DIM = 64
E = 16


norm_eps = 1e-06
score_scale = 0.015625
residual_scale = 0.22
rope_base = 10000.0


def rotary_table(token_positions, head_size):
    half_size = head_size // 2
    inverse = rope_base ** (-(jnp.arange(half_size, dtype=jnp.float32) * 2.0 / head_size))
    angles = token_positions[:, None].astype(jnp.float32) * inverse[None, :]
    return (jnp.cos(angles)[:, None, :], jnp.sin(angles)[:, None, :])


def apply_rotary(vectors, cosine_lookup, sine_lookup):
    half_size = vectors.shape[-1] // 2
    first_half = vectors[..., :half_size]
    second_half = vectors[..., half_size:]
    return jnp.concatenate(
        [
            first_half * cosine_lookup - second_half * sine_lookup,
            second_half * cosine_lookup + first_half * sine_lookup,
        ],
        axis=-1,
    )


def reverse_rotary(gradient, cosine_lookup, sine_lookup):
    half_size = gradient.shape[-1] // 2
    first_half = gradient[..., :half_size]
    second_half = gradient[..., half_size:]
    return jnp.concatenate(
        [
            first_half * cosine_lookup + second_half * sine_lookup,
            second_half * cosine_lookup - first_half * sine_lookup,
        ],
        axis=-1,
    )


def body(
    block_input,
    segments,
    routes,
    attn_gain,
    ffn_gain,
    query_weight,
    key_matrix,
    value_matrix,
    out_weight,
    router_weight,
    gate_weight,
    up_weight,
    down_weight,
    grad_output,
):
    head_count = lax.axis_size("heads")
    n_tensor = lax.axis_size("tensor")
    n_fsdp = lax.axis_size("fsdp")
    fsdp_index = lax.axis_index("fsdp")
    heads_index = lax.axis_index("heads")
    tensor_index = lax.axis_index("tensor")
    token_rows = block_input.shape[0]
    model_width = block_input.shape[1]
    query_rows = token_rows * head_count
    seq_rows = query_rows * n_fsdp
    key_value_local = KEY_VALUE_HEADS // head_count
    heads_per_group = QUERY_HEADS // KEY_VALUE_HEADS
    slice_width = model_width // n_tensor
    gathered = (
        lax.all_gather(attn_gain, ("fsdp", "heads"), axis=0, tiled=True),
        lax.all_gather(ffn_gain, ("fsdp", "heads"), axis=0, tiled=True),
        lax.all_gather(query_weight, ("fsdp", "heads"), axis=0, tiled=True),
        lax.all_gather(key_matrix, ("fsdp", "heads"), axis=0, tiled=True),
        lax.all_gather(value_matrix, ("fsdp", "heads"), axis=0, tiled=True),
        lax.all_gather(out_weight, ("fsdp", "heads"), axis=0, tiled=True),
        lax.all_gather(router_weight, ("fsdp", "heads"), axis=0, tiled=True),
        lax.all_gather(gate_weight, ("fsdp", "heads"), axis=1, tiled=True),
        lax.all_gather(up_weight, ("fsdp", "heads"), axis=1, tiled=True),
        lax.all_gather(down_weight, ("fsdp", "heads"), axis=2, tiled=True),
    )
    gain_attn = gathered[0].astype(jnp.float32)
    gain_ffn = gathered[1].astype(jnp.float32)
    full_query, full_key, full_value, full_out, full_router, full_gate, full_up, full_down = (
        gathered[2:]
    )
    inputs = block_input.astype(jnp.float32)
    scale_one = lax.rsqrt(jnp.mean(inputs * inputs, axis=-1, keepdims=True) + norm_eps)
    unit_one = inputs * scale_one
    normalized_input = (unit_one * gain_attn).astype(jnp.bfloat16)
    query_lin = jnp.dot(normalized_input, full_query, preferred_element_type=jnp.float32)
    key_linear = jnp.dot(normalized_input, full_key, preferred_element_type=jnp.float32)
    value_lin = jnp.dot(normalized_input, full_value, preferred_element_type=jnp.float32)
    own_start = (fsdp_index * head_count + heads_index) * token_rows
    token_positions = own_start + jnp.arange(token_rows, dtype=jnp.int32)
    cosine_lookup, sine_lookup = rotary_table(token_positions, HEAD_DIM)
    query_send = (
        apply_rotary(
            query_lin.reshape(token_rows, QUERY_HEADS, HEAD_DIM), cosine_lookup, sine_lookup
        )
        .reshape(token_rows, QUERY_HEADS * HEAD_DIM)
        .astype(jnp.bfloat16)
    )
    key_send = (
        apply_rotary(
            key_linear.reshape(token_rows, KEY_VALUE_HEADS, HEAD_DIM), cosine_lookup, sine_lookup
        )
        .reshape(token_rows, KEY_VALUE_HEADS * HEAD_DIM)
        .astype(jnp.bfloat16)
    )
    value_send = value_lin.astype(jnp.bfloat16)
    query_heads, key_local, value_local = (
        lax.all_to_all(query_send, "heads", split_axis=1, concat_axis=0, tiled=True),
        lax.all_to_all(key_send, "heads", split_axis=1, concat_axis=0, tiled=True),
        lax.all_to_all(value_send, "heads", split_axis=1, concat_axis=0, tiled=True),
    )
    query_vectors = query_heads.reshape(query_rows, key_value_local, heads_per_group, HEAD_DIM)
    query_start = fsdp_index * query_rows
    query_pos = query_start + jnp.arange(query_rows, dtype=jnp.int32)
    query_seg = lax.dynamic_slice_in_dim(segments, query_start, query_rows, 0)

    def masked_exp(key_block, key_start):
        block_rows = key_block.shape[0]
        raw_scores = (
            jnp.einsum(
                "qkgd,jkd->kgqj", query_vectors, key_block, preferred_element_type=jnp.float32
            )
            * score_scale
        )
        key_pos = key_start + jnp.arange(block_rows, dtype=jnp.int32)
        key_seg = lax.dynamic_slice_in_dim(segments, key_start, block_rows, 0)
        allowed = (query_pos[:, None] >= key_pos[None, :]) & (
            query_seg[:, None] == key_seg[None, :]
        )
        return jnp.where(allowed[None, None], jnp.exp(raw_scores), 0.0)

    def split_blocks(key_piece):
        keys_piece, values_piece = key_piece
        piece_rows = keys_piece.shape[0]
        block_rows = math.gcd(piece_rows, query_rows)
        block_count = piece_rows // block_rows
        starts = jnp.arange(block_count, dtype=jnp.int32) * block_rows
        return (
            keys_piece.reshape(block_count, block_rows, key_value_local, HEAD_DIM),
            values_piece.reshape(block_count, block_rows, key_value_local, HEAD_DIM),
            starts,
        )

    start_state = (
        jnp.zeros((key_value_local, heads_per_group, query_rows), jnp.float32),
        jnp.zeros((key_value_local, heads_per_group, query_rows, HEAD_DIM), jnp.float32),
    )
    fold_state = start_state

    def block_step(running, block_item):
        denominator, numerator = running
        key_block, value_block, key_start = block_item
        weights = masked_exp(key_block, key_start)
        denominator = denominator + jnp.sum(weights, axis=-1)
        numerator = numerator + jnp.einsum(
            "kgqj,jkd->kgqd",
            weights.astype(jnp.bfloat16),
            value_block,
            preferred_element_type=jnp.float32,
        )
        return ((denominator, numerator), None)

    fold_state, _ = lax.scan(
        block_step,
        fold_state,
        split_blocks(
            (
                lax.all_gather(key_local, "fsdp", axis=0, tiled=True),
                lax.all_gather(value_local, "fsdp", axis=0, tiled=True),
            )
        ),
    )
    denominator, numerator = fold_state
    attn_full = numerator / denominator[..., None]
    attn_send = (
        attn_full.transpose(2, 0, 1, 3)
        .reshape(query_rows, key_value_local * heads_per_group * HEAD_DIM)
        .astype(jnp.bfloat16)
    )
    attn_back = lax.all_to_all(attn_send, "heads", split_axis=0, concat_axis=1, tiled=True)
    attn_proj = jnp.dot(attn_back, full_out, preferred_element_type=jnp.float32)
    hidden = inputs + residual_scale * attn_proj
    scale_two = lax.rsqrt(jnp.mean(hidden * hidden, axis=-1, keepdims=True) + norm_eps)
    unit_two = hidden * scale_two
    normed_two = (unit_two * gain_ffn).astype(jnp.bfloat16)
    logits = jnp.dot(normed_two, full_router, preferred_element_type=jnp.float32)
    onehot = (routes[:, :, None] == jnp.arange(E, dtype=jnp.int32)[None, None, :]).astype(
        jnp.float32
    )
    picked = jnp.sum(onehot * logits[:, None, :], axis=-1)
    route_probs = jax.nn.softmax(picked, axis=-1)
    combine = jnp.sum(onehot * route_probs[:, :, None], axis=1)
    gate_pre = jnp.einsum("td,edf->etf", normed_two, full_gate, preferred_element_type=jnp.float32)
    up_pre = jnp.einsum("td,edf->etf", normed_two, full_up, preferred_element_type=jnp.float32)
    sigmoid_gate = jax.nn.sigmoid(gate_pre)
    silu_gate = gate_pre * sigmoid_gate
    active = (silu_gate * up_pre).astype(jnp.bfloat16)
    expert_out = jnp.einsum("etf,efd->etd", active, full_down, preferred_element_type=jnp.float32)
    mixed_part = jnp.sum(combine.T[:, :, None] * expert_out, axis=0)
    mixed_sum = lax.psum_scatter(
        mixed_part.astype(jnp.bfloat16), "tensor", scatter_dimension=1, tiled=True
    ).astype(jnp.float32)
    hidden_mine = lax.dynamic_slice_in_dim(hidden, tensor_index * slice_width, slice_width, 1)
    block_output = hidden_mine + residual_scale * mixed_sum
    mixed_grad = residual_scale * grad_output
    expert_grad = (combine.T[:, :, None] * mixed_grad[None]).astype(jnp.bfloat16)
    combine_part = jnp.sum(expert_out * mixed_grad[None], axis=-1).T
    active_grad = jnp.einsum(
        "etd,efd->etf", expert_grad, full_down, preferred_element_type=jnp.float32
    )
    gate_grad = (
        active_grad * up_pre * sigmoid_gate * (1.0 + gate_pre * (1.0 - sigmoid_gate))
    ).astype(jnp.bfloat16)
    up_grad = (active_grad * silu_gate).astype(jnp.bfloat16)
    normed_part = jnp.einsum(
        "etf,edf->td", gate_grad, full_gate, preferred_element_type=jnp.float32
    ) + jnp.einsum("etf,edf->td", up_grad, full_up, preferred_element_type=jnp.float32)
    gate_full = jnp.einsum("td,etf->edf", normed_two, gate_grad, preferred_element_type=jnp.float32)
    up_full = jnp.einsum("td,etf->edf", normed_two, up_grad, preferred_element_type=jnp.float32)
    down_full = jnp.einsum("etf,etd->efd", active, expert_grad, preferred_element_type=jnp.float32)
    grad_gate, grad_up, grad_down = (
        lax.psum_scatter(gate_full.astype(jnp.bfloat16), ("fsdp", "heads"), scatter_dimension=1, tiled=True),
        lax.psum_scatter(up_full.astype(jnp.bfloat16), ("fsdp", "heads"), scatter_dimension=1, tiled=True),
        lax.psum_scatter(down_full.astype(jnp.bfloat16), ("fsdp", "heads"), scatter_dimension=2, tiled=True),
    )
    normed_grad, combine_grad = lax.psum((normed_part, combine_part), "tensor")
    pick_grad = jnp.sum(onehot * combine_grad[:, None, :], axis=-1)
    picked_grad = route_probs * (
        pick_grad - jnp.sum(route_probs * pick_grad, axis=-1, keepdims=True)
    )
    logit_grad = jnp.sum(onehot * picked_grad[:, :, None], axis=1).astype(jnp.bfloat16)
    router_full = jnp.dot(normed_two.T, logit_grad, preferred_element_type=jnp.float32)
    normed_grad = normed_grad + jnp.dot(
        logit_grad, full_router.T, preferred_element_type=jnp.float32
    )
    gain_ffn_full = jnp.sum(normed_grad * unit_two, axis=0)
    unit_grad = normed_grad * gain_ffn
    hidden_grad = grad_output + scale_two * (
        unit_grad - unit_two * jnp.mean(unit_grad * unit_two, axis=-1, keepdims=True)
    )
    proj_grad = (residual_scale * hidden_grad).astype(jnp.bfloat16)
    out_full = jnp.dot(attn_back.T, proj_grad, preferred_element_type=jnp.float32)
    attn_grad = jnp.dot(proj_grad, full_out.T, preferred_element_type=jnp.float32).astype(
        jnp.bfloat16
    )
    grad_heads = lax.all_to_all(attn_grad, "heads", split_axis=1, concat_axis=0, tiled=True)
    grad_float = (
        grad_heads.reshape(query_rows, key_value_local, heads_per_group, HEAD_DIM)
        .transpose(1, 2, 0, 3)
        .astype(jnp.float32)
    )
    scaled_grad = (grad_float / denominator[..., None]).astype(jnp.bfloat16)
    shift_term = jnp.sum(grad_float * attn_full, axis=-1) / denominator
    start_back = (
        jnp.zeros((key_value_local, heads_per_group, query_rows, HEAD_DIM), jnp.float32),
        jnp.zeros((seq_rows, key_value_local * HEAD_DIM), jnp.float32),
        jnp.zeros((seq_rows, key_value_local * HEAD_DIM), jnp.float32),
    )
    fold_state = start_back

    def block_step(running, block_item):
        query_acc, key_acc, value_acc = running
        key_block, value_block, key_start = block_item
        block_rows = key_block.shape[0]
        weights = masked_exp(key_block, key_start)
        dot_grad = jnp.einsum(
            "kgqd,jkd->kgqj", scaled_grad, value_block, preferred_element_type=jnp.float32
        )
        score_grad = (weights * (dot_grad - shift_term[..., None])).astype(jnp.bfloat16)
        query_acc = (
            query_acc
            + jnp.einsum(
                "kgqj,jkd->kgqd", score_grad, key_block, preferred_element_type=jnp.float32
            )
            * score_scale
        )
        key_part = (
            jnp.einsum(
                "kgqj,qkgd->jkd", score_grad, query_vectors, preferred_element_type=jnp.float32
            )
            * score_scale
        )
        value_part = jnp.einsum(
            "kgqj,kgqd->jkd",
            weights.astype(jnp.bfloat16),
            scaled_grad,
            preferred_element_type=jnp.float32,
        )
        key_old = lax.dynamic_slice_in_dim(key_acc, key_start, block_rows, 0)
        value_old = lax.dynamic_slice_in_dim(value_acc, key_start, block_rows, 0)
        key_acc = lax.dynamic_update_slice_in_dim(
            key_acc,
            key_old + key_part.reshape(block_rows, key_value_local * HEAD_DIM),
            key_start,
            0,
        )
        value_acc = lax.dynamic_update_slice_in_dim(
            value_acc,
            value_old + value_part.reshape(block_rows, key_value_local * HEAD_DIM),
            key_start,
            0,
        )
        return ((query_acc, key_acc, value_acc), None)

    fold_state, _ = lax.scan(
        block_step,
        fold_state,
        split_blocks(
            (
                lax.all_gather(key_local, "fsdp", axis=0, tiled=True),
                lax.all_gather(value_local, "fsdp", axis=0, tiled=True),
            )
        ),
    )
    query_acc, key_acc, value_acc = fold_state
    key_mine, value_mine = (
        lax.psum_scatter(key_acc, "fsdp", scatter_dimension=0, tiled=True),
        lax.psum_scatter(value_acc, "fsdp", scatter_dimension=0, tiled=True),
    )
    query_send_back = (
        query_acc.transpose(2, 0, 1, 3)
        .reshape(query_rows, key_value_local * heads_per_group * HEAD_DIM)
        .astype(jnp.bfloat16)
    )
    query_ret, key_returned, value_ret = (
        lax.all_to_all(query_send_back, "heads", split_axis=0, concat_axis=1, tiled=True),
        lax.all_to_all(
            key_mine.astype(jnp.bfloat16), "heads", split_axis=0, concat_axis=1, tiled=True
        ),
        lax.all_to_all(
            value_mine.astype(jnp.bfloat16), "heads", split_axis=0, concat_axis=1, tiled=True
        ),
    )
    query_lin_grad = (
        reverse_rotary(
            query_ret.astype(jnp.float32).reshape(token_rows, QUERY_HEADS, HEAD_DIM),
            cosine_lookup,
            sine_lookup,
        )
        .reshape(token_rows, QUERY_HEADS * HEAD_DIM)
        .astype(jnp.bfloat16)
    )
    key_lin_grad = (
        reverse_rotary(
            key_returned.astype(jnp.float32).reshape(token_rows, KEY_VALUE_HEADS, HEAD_DIM),
            cosine_lookup,
            sine_lookup,
        )
        .reshape(token_rows, KEY_VALUE_HEADS * HEAD_DIM)
        .astype(jnp.bfloat16)
    )
    query_full = jnp.dot(normalized_input.T, query_lin_grad, preferred_element_type=jnp.float32)
    key_full = jnp.dot(normalized_input.T, key_lin_grad, preferred_element_type=jnp.float32)
    value_full = jnp.dot(normalized_input.T, value_ret, preferred_element_type=jnp.float32)
    normed_one_grad = jnp.dot(query_lin_grad, full_query.T, preferred_element_type=jnp.float32)
    normed_one_grad = normed_one_grad + jnp.dot(
        key_lin_grad, full_key.T, preferred_element_type=jnp.float32
    )
    normed_one_grad = normed_one_grad + jnp.dot(
        value_ret, full_value.T, preferred_element_type=jnp.float32
    )
    gain_attn_full = jnp.sum(normed_one_grad * unit_one, axis=0)
    unit_one_grad = normed_one_grad * gain_attn
    grad_input = hidden_grad + scale_one * (
        unit_one_grad - unit_one * jnp.mean(unit_one_grad * unit_one, axis=-1, keepdims=True)
    )
    grad_attn_gain, grad_ffn_gain, grad_query, grad_key, grad_value, grad_out_proj, grad_router = (
        lax.psum_scatter(gain_attn_full, ("fsdp", "heads"), scatter_dimension=0, tiled=True),
        lax.psum_scatter(gain_ffn_full, ("fsdp", "heads"), scatter_dimension=0, tiled=True),
        lax.psum_scatter(query_full.astype(jnp.bfloat16), ("fsdp", "heads"), scatter_dimension=0, tiled=True),
        lax.psum_scatter(key_full.astype(jnp.bfloat16), ("fsdp", "heads"), scatter_dimension=0, tiled=True),
        lax.psum_scatter(value_full.astype(jnp.bfloat16), ("fsdp", "heads"), scatter_dimension=0, tiled=True),
        lax.psum_scatter(out_full.astype(jnp.bfloat16), ("fsdp", "heads"), scatter_dimension=0, tiled=True),
        lax.psum_scatter(router_full, ("fsdp", "heads"), scatter_dimension=0, tiled=True),
    )
    grad_query, grad_key, grad_value, grad_out_proj, grad_gate, grad_up, grad_down = (
        g.astype(jnp.float32)
        for g in (grad_query, grad_key, grad_value, grad_out_proj, grad_gate, grad_up, grad_down)
    )
    return (
        block_output,
        grad_input,
        grad_attn_gain,
        grad_ffn_gain,
        grad_query,
        grad_key,
        grad_value,
        grad_out_proj,
        grad_router,
        grad_gate,
        grad_up,
        grad_down,
    )


MESH_ID = pl.DeviceIdType.MESH
F32 = jnp.float32
BF16 = jnp.bfloat16

TB = 192
DM = 1536
TC = 384
HALF = 96
NBLK = 8
NQ = 6
TOPK = 8
FIRST_DOC_BLOCKS = 5


def contract(left, right, left_dim, right_dim, precision=None):
    return lax.dot_general(
        left,
        right,
        (((left_dim,), (right_dim,)), ((), ())),
        preferred_element_type=F32,
        precision=precision,
    )


def rows(index):
    return pl.ds(pl.multiple_of(index * TB, TB), TB)


def cols(index):
    return pl.ds(pl.multiple_of(index * TC, 128), TC)


class Place:
    def __init__(self):
        self.z = lax.axis_index("fsdp")
        self.c = lax.axis_index("heads")
        self.t = lax.axis_index("tensor")
        self.b = 2 * self.z + self.c

    def partner(self):
        return (self.z, 1 - self.c, self.t)

    def at_z(self, z):
        return (z, self.c, self.t)

    def at_block(self, block):
        return (block // 2, block % 2, self.t)

    def peer_t(self, k):
        if k == 1:
            return self.t + 1 - 2 * (self.t % 2)
        if k == 2:
            return (self.t + 2) % 4
        return 3 - self.t

    def plane(self, k):
        return (self.z, self.c, self.peer_t(k))

    def other(self, k):
        return (self.b + k) % NBLK

    def arrival(self, i):
        if i == 0:
            return self.z + 1 - 2 * (self.z % 2)
        if i == 1:
            return 2 - self.z // 2
        return 3 - 3 * (self.z // 2)

    def forward_to(self, i):
        return 3 - self.z if i == 0 else 3 * (self.z - 1)

    def middle(self):
        return self.z * (3 - self.z) > 0

    def dest(self, j):
        inner = (self.z * (3 - self.z)) // 2
        turned = j + inner * (j // 2) * (1 - 2 * (j % 2))
        upper = self.z // 2
        return 3 * (1 - upper) + (2 * upper - 1) * turned


def remote(src, dst, send_sem, recv_sem, device):
    return pltpu.make_async_remote_copy(
        src_ref=src,
        dst_ref=dst,
        send_sem=send_sem,
        recv_sem=recv_sem,
        device_id=device,
        device_id_type=MESH_ID,
    )


class Pending:
    def __init__(self):
        self.items = []

    def start(self, copy, when=None):
        self.begin(copy, when)
        self.later(copy, when)

    def begin(self, copy, when=None):
        if when is None:
            copy.start()
        else:

            @pl.when(when)
            def _():
                copy.start()

    def later(self, copy, when=None):
        self.items.append((copy, when))

    def drain(self):
        for copy, when in self.items:
            if when is None:
                copy.wait_send()
            else:

                @pl.when(when)
                def _(copy=copy):
                    copy.wait_send()

        self.items = []


class LineGather:
    def __init__(self, me, pend, view, line_view, several, several_line, sems):
        self.me, self.pend, self.view, self.line_view = me, pend, view, line_view
        self.several, self.several_line = several, several_line
        self.send, self.recv, self.psend, self.precv = sems

    def bytes_of(self, ref, send_sem, recv_sem):
        return remote(ref, ref, send_sem.at[0], recv_sem.at[0], self.me.partner())

    def start(self):
        me = self.me
        own = self.line_view(me.b)
        for dz, when in ((1, me.z < 3), (-1, me.z > 0)):
            self.pend.begin(
                remote(own, own, self.send.at[0], self.recv.at[me.z], me.at_z(me.z + dz)), when
            )
        for count, when in ((5, me.middle()), (1, me.z * (3 - me.z) == 0)):
            self.pend.later(self.bytes_of(self.several_line(count), self.send, self.recv), when)
        self.share_own()

    def share_own(self):
        self.share_block(self.me.b)
        self.pend.later(self.bytes_of(self.several(4), self.psend, self.precv))

    def share_block(self, block):
        whole = self.view(block)
        self.pend.begin(
            remote(whole, whole, self.psend.at[0], self.precv.at[0], self.me.partner())
        )

    def arrive(self, i):
        me = self.me
        source = me.arrival(i)
        block = self.line_view(2 * source + me.c)
        remote(block, block, self.send.at[0], self.recv.at[source], me.partner()).wait_recv()
        self.pend.begin(
            remote(
                block, block, self.send.at[0], self.recv.at[source], me.at_z(me.forward_to(i))
            ),
            me.middle(),
        )

    def share(self, i):
        self.share_block(2 * self.me.arrival(i) + self.me.c)

    def finish(self):
        self.bytes_of(self.several(4), self.psend, self.precv).wait_recv()


class UpGather(LineGather):
    def __init__(self, me, pend, view, sems):
        self.me, self.pend, self.view = me, pend, view
        self.send, self.recv, self.psend, self.precv = sems

    def start(self):
        me = self.me
        own = self.view(me.b)
        self.pend.start(
            remote(own, own, self.send.at[0], self.recv.at[me.z], me.at_z(me.z + 1)),
            me.z < 2 + me.c,
        )
        self.pend.start(remote(own, own, self.psend.at[3], self.precv.at[me.z], me.partner()))

    def near(self, core):
        return self.me.z * (3 + core - self.me.z) > 0

    def take(self, source):
        block = self.view(2 * source + self.me.c)
        remote(
            block, block, self.send.at[0], self.recv.at[source], self.me.partner()
        ).wait_recv()
        return block

    def relay(self):
        me = self.me

        @pl.when(self.near(me.c))
        def _():
            self.take(me.z - 1)

        block = self.view(2 * (me.z - 1) + me.c)
        self.pend.start(
            remote(block, block, self.send.at[1], self.recv.at[me.z - 1], me.at_z(me.z + 1)),
            me.z == 1,
        )
        self.pend.start(
            remote(block, block, self.psend.at[0], self.precv.at[me.z - 1], me.partner()),
            self.near(me.c),
        )

        @pl.when(me.z == 2)
        def _():
            self.take(0)

        block = self.view(me.c)
        self.pend.start(
            remote(block, block, self.psend.at[1], self.precv.at[0], me.partner()), me.z == 2
        )

    def finish(self):
        me = self.me

        def take(source):
            block = self.view(2 * source + (1 - me.c))
            remote(
                block, block, self.psend.at[0], self.precv.at[source], me.partner()
            ).wait_recv()

        take(me.z)

        @pl.when(self.near(1 - me.c))
        def _():
            take(me.z - 1)

        @pl.when(me.z == 2)
        def _():
            take(0)


class FullGather(LineGather):
    def __init__(self, me, pend, buffer, sems):
        super().__init__(
            me,
            pend,
            lambda block: buffer.at[rows(block), :],
            lambda block: buffer.at[rows(block), cols(me.t)],
            lambda count: buffer.at[0 : TB * count, :],
            lambda count: buffer.at[0 : TB * count, 0:TC],
            sems[:4],
        )
        self.buffer = buffer
        self.xsend, self.xrecv = sems[4:]

    def piece(self, i, k):
        lanes = cols(self.me.t if k == 0 else self.me.peer_t(k))
        return self.buffer.at[rows(2 * self.me.arrival(i) + self.me.c), lanes]

    def part(self, i, k, half):
        start = (2 * self.me.arrival(i) + self.me.c) * TB + HALF * half
        return self.buffer.at[pl.ds(pl.multiple_of(start, HALF), HALF), cols(self.me.peer_t(k))]

    def copy(self, view, i, relayed, k):
        return remote(
            view,
            view,
            self.xsend.at[0],
            self.xrecv.at[relayed, self.me.arrival(i)],
            self.me.plane(k),
        )

    def spread(self, i):
        for k in (1, 2):
            self.pend.begin(self.copy(self.piece(i, 0), i, 0, k))
        if i == 2:
            nine = self.buffer.at[0:864, 0:768]
            self.pend.later(self.copy(nine, i, 0, 1))

    def relay(self, i):
        self.copy(self.buffer.at[0 : 2 * TB, 0:TC], i, 0, 1).wait_recv()
        for k in (1, 2):
            self.pend.begin(self.copy(self.part(i, k, k - 1), i, 1, 3 - k))

    def cross(self, i):
        self.copy(self.buffer.at[0:TB, 0:TC], i, 1, 1).wait_recv()
        self.share(i)


def swap_halves(u):
    lane = lax.broadcasted_iota(jnp.int32, u.shape, 1)
    return jnp.where(lane % 64 < 32, pltpu.roll(u, 96, 1), pltpu.roll(u, 32, 1))


def half_mask(half):
    lane = lax.broadcasted_iota(jnp.int32, (TB, 128), 1)
    return (lane // 64) == half


def head_from_chunk(chunk, h):
    if h % 2 != h // 3:
        chunk = pltpu.roll(chunk, 64, 1)
    return jnp.where(half_mask(h // 3), chunk, 0.0)


def chunk_from_heads(first, second, pair):
    if (2 * pair) // 3 != 0:
        first = pltpu.roll(first, 64, 1)
    if (2 * pair + 1) // 3 != 1:
        second = pltpu.roll(second, 64, 1)
    return jnp.where(half_mask(0), first, second)


def row_chunks(body, size=64):
    def step(i, carry):
        body(pl.ds(pl.multiple_of(i * size, size), size))
        return carry

    lax.fori_loop(0, TB // size, step, 0)


class Bag(dict):
    __getattr__ = dict.__getitem__


def bags(tree):
    return Bag({k: bags(v) for k, v in tree.items()}) if isinstance(tree, dict) else tree


def scratch_tree():
    def f32(*shape):
        return pltpu.VMEM(shape, F32)

    def b16(*shape):
        return pltpu.VMEM(shape, BF16)

    dma = pltpu.SemaphoreType.DMA

    def pair(*shape):
        return (dma(shape), dma(shape))

    def line():
        return (dma((1,)), dma((4,)), dma((1,)), dma((1,)))

    def up():
        return (dma((2,)), dma((4,)), dma((4,)), dma((4,)))

    def full():
        return (*line(), dma((1,)), dma((2, 4)))

    def scatter():
        return dict(
            part=b16(DM, DM),
            core=b16(4, TB, DM),
            plane=b16(4, 2, TB, TC),
            diagonal=b16(4, 2, HALF, TC),
            line=b16(6, TB, TC),
            sems=(dma((1,)), dma((4,)), dma((1,)), dma((4, 2)), dma((1,)), dma((6,))),
        )

    def reduce(width):
        return dict(
            core=b16(4, TB, width),
            line=b16(6, TB, width),
            sems=(dma((1,)), dma((4,)), dma((2,)), dma((6,))),
        )

    return dict(
        w_qkv=b16(DM, 640),
        small=f32(NBLK, 24, 256),
        w_out=b16(DM, DM),
        d_moe=b16(DM, DM),
        hn=b16(DM, DM),
        kv=b16(DM, 256),
        w_moe=b16(DM, 768),
        comb=f32(NBLK, 16, 256),
        xn=b16(TB, DM),
        r_one=f32(TB, 1),
        r_two=f32(TB, 1),
        hidden=f32(TB, DM),
        qz=b16(NQ, TB, 128),
        oz=f32(NQ, TB, 128),
        den=f32(NQ, TB, 128),
        o_full=b16(TB, DM),
        gains=f32(8, DM),
        router_t=b16(16, DM),
        dgu=b16(DM, 512),
        cz=b16(DM, 256),
        h=scatter(),
        y=scatter(),
        dhn=b16(TB, DM),
        dc_own=f32(NBLK, 8, 256),
        dc_in=f32(NBLK, 8, 256),
        dc_plane=f32(3, NBLK, 8, 256),
        dc_t=f32(16, 256),
        g_moe=b16(DM, 768),
        acc=f32(TB, TC),
        dh=f32(TB, DM),
        dproj=b16(TB, DM),
        flat=f32(24, DM),
        sm=dict(own=f32(NBLK, 24, 256), inn=f32(NBLK, 24, 256)),
        sn=dict(own=f32(NBLK, 8, 256), inn=f32(NBLK, 8, 256)),
        g_out_sum=b16(TB, TC),
        dnz=b16(NQ, TB, 128),
        dkv=b16(DM, 256),
        dqkv=b16(TB, 640),
        g_qkv_sum=b16(TB, 640),
        dx=b16(TB, DM),
        dx_in=b16(3, TB, TC),
        dxn=b16(TB, DM),
        local_sem=dma((11,)),
        lg=dict(s=line(), w=line(), v=line(), o=line(), kv=up(), c=line()),
        fg=dict(wo=full(), dm=full(), hn=full()),
        aa=dict(
            wm=[pair(1), pair(1)], gm=[pair(1), pair(1)], dc=pair(1), sm=pair(1), sn=pair(1)
        ),
        pl=dict(
            o=pair(1), hc=pair(1), dc=pair(1), dh=pair(1), go=pair(1), gq=pair(1), gk=pair(1),
            gv=pair(1), xs=pair(1), xg=pair(1),
        ),
        rd=dict(go=reduce(TC), dkv=reduce(256), gq=reduce(TC), gkv=reduce(256)),
    )


def kernel(r):
    g_out_part = r.dgu.at[:, 0:TC]
    w_column = r.y.part.at[:, 0:TC]
    g_q_part, g_kv_part = r.w_moe.at[:, 0:TC], r.w_moe.at[:, TC:640]
    me = Place()
    pend = Pending()
    z, c, t, b = me.z, me.c, me.t, me.b

    loc = r.local_sem
    local = [
        pltpu.make_async_copy(r.wq.at[:, cols(t)], r.w_qkv.at[rows(b), 0:384], loc.at[0]),
        pltpu.make_async_copy(
            r.wk.at[:, pl.ds(pl.multiple_of(128 * t, 128), 128)],
            r.w_qkv.at[rows(b), 384:512], loc.at[1],
        ),
        pltpu.make_async_copy(
            r.wv.at[:, pl.ds(pl.multiple_of(128 * t, 128), 128)],
            r.w_qkv.at[rows(b), 512:640], loc.at[2],
        ),
        pltpu.make_async_copy(r.wo.at[:, cols(t)], w_column.at[rows(b), :], loc.at[3]),
        pltpu.make_async_copy(r.wo, r.w_out.at[rows(b), :], loc.at[10]),
    ]
    moe_lanes = [[pl.ds(384 * e + 128 * which, 128) for which in range(3)] for e in range(2)]
    moe_sources = [list(zip((r.gate, r.up, r.down_t), lanes)) for lanes in moe_lanes]
    own_moe = [
        pltpu.make_async_copy(
            shard.at[2 * b + e], r.w_moe.at[rows(b), lanes], loc.at[4 + 3 * e + i]
        )
        for e in range(2)
        for i, (shard, lanes) in enumerate(moe_sources[e])
    ]
    for copy in local:
        copy.start()
    for copy in own_moe:
        copy.start()
    barrier = pltpu.get_barrier_semaphore()
    for k in range(1, NBLK):
        pl.semaphore_signal(
            barrier, inc=1, device_id=me.at_block(me.other(k)), device_id_type=MESH_ID
        )
    for k in (1, 2, 3):
        pl.semaphore_signal(barrier, inc=1, device_id=me.plane(k), device_id_type=MESH_ID)
    r.small[b, 0:16, 0:TB] = r.router_own[...].astype(F32)
    for n in range(2):
        r.small[b, 16 + n : 17 + n, 0:128] = r.vectors[12 + 2 * n : 13 + 2 * n, :]
        r.small[b, 16 + n : 17 + n, 128:TB] = r.vectors[13 + 2 * n : 14 + 2 * n, 0:64]
    r.d_moe[rows(b), :] = (residual_scale * r.gout[...]).astype(BF16)
    pl.semaphore_wait(barrier, NBLK - 1 + 3)

    def line(view, several, sems):
        return LineGather(me, pend, view, view, several, several, sems)

    g_small = line(lambda k: r.small.at[k], lambda n: r.small.at[0:n], r.lg.s)
    def half(h):
        return lambda k: r.w_qkv.at[pl.ds(pl.multiple_of(TB * k + 96 * h, 96), 96), :]

    g_qkv = [
        line(half(h), lambda n: r.w_qkv.at[0 : 96 * n, :], sems)
        for h, sems in enumerate((r.lg.w, r.lg.v))
    ]
    g_kv = UpGather(me, pend, lambda k: r.kv.at[rows(k), :], r.lg.kv)
    g_comb = line(lambda k: r.comb.at[k], lambda n: r.comb.at[0:n], r.lg.c)
    early = Pending()
    wcol_view = lambda k: w_column.at[rows(k), :]
    wcol_several = lambda n: w_column.at[0 : TB * n, :]
    g_wcol = LineGather(me, early, wcol_view, wcol_view, wcol_several, wcol_several, r.lg.o)
    g_wout = FullGather(me, pend, r.w_out, r.fg.wo)
    g_dmoe = FullGather(me, pend, r.d_moe, r.fg.dm)
    g_hn = FullGather(me, pend, r.hn, r.fg.hn)

    def send_weights_to(e, peer):
        send, recv = r.aa.wm[e]
        for shard, lanes in moe_sources[e]:
            remote(
                shard.at[2 * peer + e],
                r.w_moe.at[rows(b), lanes],
                send.at[0],
                recv.at[0],
                me.at_block(peer),
            ).start()

    end_chip = z * (3 - z) == 0

    def send_weights_end(e, ks):
        @pl.when(end_chip)
        def _():
            for k in ks:
                send_weights_to(e, me.other(k))

    def send_weights_inner(e, ks):
        for k in ks:
            peer = me.other(k)

            @pl.when(me.middle() & (peer // 2 + z != 3))
            def _(peer=peer):
                send_weights_to(e, peer)

    def send_weights_middle(e):
        @pl.when(me.middle())
        def _():
            for j in range(2):
                peer = 6 - 2 * z + j
                send_weights_to(e, peer)

    def seven_blocks(sems):
        whole = r.w_moe.at[0 : 7 * TB, 0:TC]
        return remote(whole, whole, sems[0].at[0], sems[1].at[0], me.partner())

    g_small.start()
    for copy in local[:3]:
        copy.wait()
    for g in g_qkv:
        g.start()
    local[3].wait()
    g_wcol.start()

    def rms_one(chunk):
        v = r.x[chunk, :].astype(F32)
        r.r_one[chunk, :] = lax.rsqrt(jnp.mean(v * v, axis=1, keepdims=True) + norm_eps)

    row_chunks(rms_one)
    for i in range(3):
        g_small.arrive(i)
        g_small.share(i)
        for g in g_qkv:
            g.arrive(i)
            g.share(i)
        if i == 1:
            g_wcol.arrive(0)
            g_wcol.share(0)
    send_weights_middle(0)
    g_small.finish()
    for k in range(NBLK):
        piece = r.small[k]
        r.router_t[:, TB * k : TB * (k + 1)] = piece[0:16, 0:TB].astype(BF16)
        r.gains[0:8, TB * k : TB * (k + 1)] = piece[16:24, 0:TB]

    def normalize_one(chunk):
        v = r.x[chunk, :].astype(F32)
        r.xn[chunk, :] = (v * r.r_one[chunk, :] * r.gains[0:1, :]).astype(BF16)

    row_chunks(normalize_one)
    for g in g_qkv:
        g.finish()
    qkv = jnp.dot(r.xn[...], r.w_qkv[...], preferred_element_type=F32)
    base_c, base_s = r.rope_block[0, pl.ds(b, 1), :], r.rope_block[1, pl.ds(b, 1), :]
    row_c, row_s = r.rope_row[0], r.rope_row[1]
    first_half = lax.broadcasted_iota(jnp.int32, (TB, 128), 1) % 64 < 32
    cosine = base_c * row_c - base_s * row_s
    sine = base_s * row_c + base_c * row_s
    sine = jnp.where(first_half, -sine, sine)
    key = qkv[:, 384:512]
    r.kv[rows(b), 0:128] = (key * cosine + swap_halves(key) * sine).astype(BF16)
    r.kv[rows(b), 128:256] = qkv[:, 512:640].astype(BF16)
    g_kv.start()
    g_dmoe.start()
    for pair in range(3):
        u = qkv[:, 128 * pair : 128 * (pair + 1)]
        u = (u * cosine + swap_halves(u) * sine).astype(BF16).astype(F32)
        r.qz[2 * pair] = head_from_chunk(u, 2 * pair).astype(BF16)
        r.qz[2 * pair + 1] = head_from_chunk(u, 2 * pair + 1).astype(BF16)
    for h in range(NQ):
        r.oz[h] = jnp.zeros((TB, 128), F32)
        r.den[h] = jnp.zeros((TB, 128), F32)
    g_kv.relay()
    send_weights_middle(1)
    for i in (1, 2):
        g_wcol.arrive(i)
        g_wcol.share(i)
    g_dmoe.arrive(0)
    g_dmoe.spread(0)
    send_weights_inner(0, (1, 7, 2))
    send_weights_end(0, (1, 7, 2, 6))

    g_kv.finish()

    first_block = FIRST_DOC_BLOCKS * (b // FIRST_DOC_BLOCKS)

    second_end = (r.vectors[0:12, :] < 1.5).astype(F32)
    second_end = jnp.sum(jnp.sum(second_end, axis=0, keepdims=True), axis=1, keepdims=True)

    def allowed(kb):
        q_pos = b * TB + lax.broadcasted_iota(jnp.int32, (TB, TB), 0)
        k_pos = kb * TB + lax.broadcasted_iota(jnp.int32, (TB, TB), 1)
        q_first = (q_pos.astype(F32) < second_end).astype(F32)
        k_first = (k_pos.astype(F32) < second_end).astype(F32)
        return (q_pos >= k_pos) & (q_first == k_first)

    def attend(kb, carry):
        keys = r.kv[rows(kb), 0:128]
        values = r.kv[rows(kb), 128:256]
        mask = allowed(kb)
        for g in range(2):
            heads = pl.ds(3 * g, 3)
            q = r.qz[heads].reshape(3 * TB, 128)
            e = jnp.exp(contract(q, keys, 1, 1) * score_scale).reshape(3, TB, TB)
            e = jnp.where(mask[None], e, 0.0)
            r.den[heads] += jnp.broadcast_to(jnp.sum(e, axis=2, keepdims=True), (3, TB, 128))
            e = e.reshape(3 * TB, TB).astype(BF16)
            r.oz[heads] += jnp.dot(e, values, preferred_element_type=F32).reshape(3, TB, 128)
        return carry

    lax.fori_loop(first_block, b + 1, attend, 0)
    for pair in range(3):
        heads = []
        for h in (2 * pair, 2 * pair + 1):
            o = jnp.where(half_mask(h // 3), r.oz[h] / r.den[h], 0.0)
            r.oz[h] = o
            heads.append(o)
        chunk = chunk_from_heads(heads[0], heads[1], pair).astype(BF16)
        r.o_full[:, pl.ds(pl.multiple_of(TC * t + 128 * pair, 128), 128)] = chunk

    def to_plane(sems, copies_of, three, pend=pend):
        send, recv = sems
        for k in (3, 1, 2):
            src, dst = copies_of(k)
            pend.begin(remote(src, dst, send.at[0], recv.at[0], me.plane(k)))
        all_three = remote(three, three, send.at[0], recv.at[0], me.plane(1))
        pend.later(all_three)
        return all_three.wait_recv

    def plane_gather(sems, buffer, pend=pend):
        own = buffer.at[:, cols(t)]
        return to_plane(sems, lambda k: (own, own), buffer.at[:, 0 : 3 * TC], pend)

    wait_o = plane_gather(r.pl.o, r.o_full)
    send_weights_inner(0, (6, 3))
    send_weights_end(0, (3, 5))
    g_wcol.finish()
    wait_o()

    column = jnp.dot(r.o_full[...], w_column[...], preferred_element_type=F32)
    r.dx[:, cols(t)] = column.astype(BF16)
    wait_column = plane_gather(r.pl.hc, r.dx, early)
    wait_column()

    def normalize_two(chunk):
        v = r.x[chunk, :].astype(F32) + residual_scale * r.dx[chunk, :].astype(F32)
        r.hidden[chunk, :] = v
        factor = lax.rsqrt(jnp.mean(v * v, axis=1, keepdims=True) + norm_eps)
        r.r_two[chunk, :] = factor
        r.dproj[chunk, :] = (v * factor * r.gains[1:2, :]).astype(BF16)

    row_chunks(normalize_two)
    r.hn[rows(b), :] = r.dproj[...]
    g_hn.start()
    logits = contract(r.router_t[...], r.dproj[...], 1, 1)
    chosen_expert = lax.broadcasted_iota(jnp.int32, (E, TB), 0)
    chosen = chosen_expert == r.routes_t[0:1, :]
    for k in range(1, TOPK):
        chosen = chosen | (chosen_expert == r.routes_t[k : k + 1, :])
    top = jnp.max(jnp.where(chosen, logits, -1e30), axis=0, keepdims=True)
    weight = jnp.where(chosen, jnp.exp(jnp.where(chosen, logits - top, 0.0)), 0.0)
    combine = weight / jnp.sum(weight, axis=0, keepdims=True)
    r.comb[b, :, 0:TB] = combine
    g_comb.start()
    g_dmoe.relay(0)
    for i in (1, 2):
        g_dmoe.arrive(i)
        g_dmoe.spread(i)
    for i in range(3):
        g_hn.arrive(i)
        g_hn.spread(i)
        g_comb.arrive(i)
        g_comb.share(i)
    send_weights_end(0, (4,))
    send_weights_end(1, (4, 3, 5, 2, 6, 1, 7))
    send_weights_inner(0, (5, 4))
    send_weights_inner(1, (4, 3, 5, 2, 6, 1, 7))
    for i in (1, 2):
        g_dmoe.relay(i)
    for i in range(3):
        g_hn.relay(i)
    for i in range(3):
        g_dmoe.cross(i)
    g_dmoe.finish()
    g_comb.finish()
    for i in range(3):
        g_hn.cross(i)
    local[4].wait()
    own_columns = []
    for i in range(3):
        where = rows(2 * me.arrival(i) + c)
        copy = pltpu.make_async_copy(
            w_column.at[where, :], r.w_out.at[where, cols(t)], loc.at[i]
        )
        copy.start()
        own_columns.append(copy)
    g_wout.share_own()
    for i in range(3):
        own_columns[i].wait()
        g_wout.spread(i)
    g_hn.finish()
    for copy in own_moe:
        copy.wait()
    seven_blocks(r.aa.wm[0]).wait_recv()

    expert = lax.broadcasted_iota(jnp.int32, (16, 128), 0)
    first_row = (lax.broadcasted_iota(jnp.int32, (8, 128), 0) == 0).astype(F32)

    def core_copy(own, i):
        part = own.part.at[rows(2 * i + (1 - c)), :]
        return remote(part, own.core.at[i], own.sems[0].at[0], own.sems[1].at[i], me.partner())

    def plane_copy(own, i, k):
        return remote(
            own.part.at[rows(2 * i + c), cols(me.peer_t(k))],
            own.plane.at[i, k - 1],
            own.sems[2].at[0],
            own.sems[3].at[i, 0],
            me.plane(k),
        )

    def half_rows(i, k):
        return pl.ds(pl.multiple_of((2 * i + c) * TB + HALF * (k - 1), HALF), HALF)

    def diagonal_copy(own, i, k):
        return remote(
            own.part.at[half_rows(i, k), cols(me.peer_t(3))],
            own.diagonal.at[i, k - 1],
            own.sems[2].at[0],
            own.sems[3].at[i, 1],
            me.plane(k),
        )

    def plane_relay(own, i):
        both = own.diagonal.at[i]
        remote(both, both, own.sems[2].at[0], own.sems[3].at[i, 1], me.plane(1)).wait_recv()
        for k in (1, 2):
            where, lanes = half_rows(i, k), cols(me.peer_t(3 - k))
            own.part[where, lanes] = (
                own.part[where, lanes].astype(F32) + own.diagonal[i, k - 1].astype(F32)
            ).astype(BF16)
        for k in (1, 2):
            plane_copy(own, i, k).start()

    def core_sum(own, i):
        core_copy(own, i).wait_recv()

        def add(chunk):
            where = pl.ds(pl.multiple_of((2 * i + c) * TB + chunk.start, 64), 64)
            own.part[where, :] = (
                own.part[where, :].astype(F32) + own.core[i, chunk, :].astype(F32)
            ).astype(BF16)

        row_chunks(add)
        for k in (1, 2):
            diagonal_copy(own, i, k).start()

    def expert_block(e, where, block):
        base = 384 * e
        gate_up = jnp.dot(
            r.hn[where, :], r.w_moe[:, base : base + 256], preferred_element_type=F32
        )
        v = jnp.dot(
            r.d_moe[where, :], r.w_moe[:, base + 256 : base + 384], preferred_element_type=F32
        )
        g, u = gate_up[:, 0:128], gate_up[:, 128:256]
        chosen_one = (expert == 2 * b + e).astype(F32)
        scale = contract(r.comb[block, :, 0:TB], chosen_one, 0, 0, lax.Precision.HIGHEST)
        sig = 1.0 / (1.0 + jnp.exp(-g))
        silu = g * sig
        active = (silu * u).astype(BF16).astype(F32)
        r.cz[where, 128 * e : 128 * (e + 1)] = (scale * active).astype(BF16)
        dc = contract(first_row, active * v, 1, 1, lax.Precision.HIGHEST)
        r.dc_own[block, e : e + 1, 0:TB] = dc[0:1, :]
        dz = scale * v
        r.dgu[where, 256 * e : 256 * e + 128] = (dz * u * sig * (1.0 + g * (1.0 - sig))).astype(
            BF16
        )
        r.dgu[where, 256 * e + 128 : 256 * e + 256] = (dz * silu).astype(BF16)

    def expert_one(block, carry):
        expert_block(0, rows(block), block)
        return carry

    lax.fori_loop(0, NBLK, expert_one, 0)

    def weight_grads(e):
        def step(n, carry):
            lanes = pl.ds(pl.multiple_of(n * 256, 256), 256)
            base = 384 * e
            r.g_moe[lanes, base : base + 256] = contract(
                r.hn[:, lanes], r.dgu[:, 256 * e : 256 * (e + 1)], 0, 0
            ).astype(BF16)
            r.g_moe[lanes, base + 256 : base + 384] = contract(
                r.d_moe[:, lanes], r.cz[:, 128 * e : 128 * (e + 1)], 0, 0
            ).astype(BF16)
            return carry

        lax.fori_loop(0, DM // 256, step, 0)

    moe_targets = [list(zip((r.gate_out, r.up_out, r.down_out), lanes)) for lanes in moe_lanes]

    def send_grads(e, ks):
        send, recv = r.aa.gm[e]
        for k in ks:
            peer = me.other(k)
            for target, lanes in moe_targets[e]:
                remote(
                    r.g_moe.at[rows(peer), lanes],
                    target.at[2 * b + e],
                    send.at[0],
                    recv.at[0],
                    me.at_block(peer),
                ).start()

    weight_grads(0)
    send_grads(0, (4, 3, 5, 2, 6, 1, 7))

    def hidden_one(block, carry):
        where = rows(block)
        for n in range(3):
            lanes = slice(512 * n, 512 * (n + 1))
            r.h.part[where, lanes] = contract(
                r.dgu[where, 0:256], r.w_moe[lanes, 0:256], 1, 1
            ).astype(BF16)
        return carry

    lax.fori_loop(0, NBLK, hidden_one, 0)
    for i in range(3):
        g_wout.relay(i)
    seven_blocks(r.aa.wm[1]).wait_recv()
    early.drain()

    class Chain:
        def __init__(self, piece, line, send, recv, arrived):
            self.piece, self.line, self.send, self.recv = piece, line, send, recv
            self.arrived = arrived

        def copy(self, j):
            i = me.dest(j)
            upper = z // 2
            inner = (z * (3 - z)) // 2
            if j == 0:
                to, slot = z + 1 - 2 * upper, i
            elif j == 1:
                to, slot = z + 1 - 2 * upper, i + inner * (4 + upper - i)
            else:
                to, slot = i, 4 + z % 2
            return remote(
                self.piece(i), self.line.at[slot], self.send.at[0], self.recv.at[slot], me.at_z(to)
            )

        def wait_slot(self, slot):
            there = self.line.at[slot]
            remote(
                there, there, self.send.at[0], self.recv.at[slot], me.partner()
            ).wait_recv()

        def step(self, j):
            i = me.dest(j)
            self.arrived(i)

            @pl.when(me.middle())
            def _():
                self.wait_slot(i)
                piece = self.piece(i)
                piece[...] = (piece[...].astype(F32) + self.line[i].astype(F32)).astype(BF16)

            self.copy(j).start()

        def steps(self, when=None):
            if when is None:
                for j in range(3):
                    self.step(j)
            else:
                pl.when(when)(self.steps)

        def total(self, acc):
            self.arrived(z)
            acc[...] = self.piece(z)[...].astype(F32)
            for slot, there in ((4, z > 0), (5, z < 3)):

                @pl.when(there)
                def _(slot=slot):
                    self.wait_slot(slot)
                    acc[...] += self.line[slot].astype(F32)

        def drain(self):
            three = self.line.at[0:3]
            remote(three, three, self.send.at[0], self.recv.at[0], me.partner()).wait_send()

    def plane_add(own, i):
        both = own.plane.at[i]
        remote(both, both, own.sems[2].at[0], own.sems[3].at[i, 0], me.plane(1)).wait_recv()
        where = rows(2 * i + c)
        total = own.part[where, cols(t)].astype(F32)
        for k in range(2):
            total = total + own.plane[i, k].astype(F32)
        own.part[where, cols(t)] = total.astype(BF16)

    def scatter_chain(own):
        return Chain(
            lambda i: own.part.at[rows(2 * i + c), cols(t)],
            own.line,
            own.sems[4],
            own.sems[5],
            lambda i: plane_add(own, i),
        )

    def scatter_drain(own):
        remote(own.core, own.core, own.sems[0].at[0], own.sems[1].at[0], me.partner()).wait_send()
        twelve = own.part.at[0:576, :]
        remote(twelve, twelve, own.sems[2].at[0], own.sems[3].at[0, 0], me.plane(1)).wait_send()

    chain_h, chain_y = scatter_chain(r.h), scatter_chain(r.y)

    def expert_two(step, carry):
        i = me.dest(step // 2)
        late = step % 2
        block = 2 * i + (1 - c) + late * (2 * c - 1)
        where = rows(block)
        expert_block(1, where, block)
        for n in range(3):
            lanes = slice(512 * n, 512 * (n + 1))
            r.h.part[where, lanes] = (
                r.h.part[where, lanes].astype(F32)
                + contract(r.dgu[where, 256:512], r.w_moe[lanes, 384:640], 1, 1)
            ).astype(BF16)

        @pl.when(late == 0)
        def _():
            core_copy(r.h, i).start()

        for n in range(3):
            lanes = slice(512 * n, 512 * (n + 1))
            r.y.part[where, lanes] = (
                contract(r.cz[where, 0:128], r.w_moe[lanes, 256:384], 1, 1)
                + contract(r.cz[where, 128:256], r.w_moe[lanes, 640:768], 1, 1)
            ).astype(BF16)

        @pl.when(late == 0)
        def _():
            core_copy(r.y, i).start()

        @pl.when(late == 1)
        def _():
            core_sum(r.h, i)

        @pl.when((late == 1) & (step > 1))
        def _():
            plane_relay(r.h, me.dest(step // 2 - 1))

        for j in range(2):

            @pl.when(end_chip & (step == 2 * j + 5))
            def _(j=j):
                chain_h.step(j)

        return carry

    lax.fori_loop(0, NBLK, expert_two, 0)

    plane_relay(r.h, z)
    dc_send, dc_recv = r.aa.dc
    for k in range(1, NBLK):
        peer = me.other(k)
        pend.begin(
            remote(
                r.dc_own.at[peer], r.dc_in.at[b], dc_send.at[0], dc_recv.at[0],
                me.at_block(peer),
            )
        )
    dc_seven = r.dc_own.at[0:7]
    dc_all = remote(dc_seven, dc_seven, dc_send.at[0], dc_recv.at[0], me.partner())
    pend.later(dc_all)
    r.dc_in[b] = r.dc_own[b]


    @pl.when(me.middle())
    def _():
        chain_h.step(0)
        chain_h.step(1)

    chain_h.step(2)
    weight_grads(1)
    own_grads = [
        pltpu.make_async_copy(
            r.g_moe.at[rows(b), lanes], target.at[2 * b + e], loc.at[4 + 3 * e + i]
        )
        for e in range(2)
        for i, (target, lanes) in enumerate(moe_targets[e])
    ]
    for copy in own_grads:
        copy.start()

    dc_all.wait_recv()
    wait_dc = to_plane(r.pl.dc, lambda k: (r.dc_in, r.dc_plane.at[k - 1]), r.dc_plane)
    send_grads(1, (1, 7, 2))
    chain_h.total(r.acc.at[:, 0:TC])
    r.dhn[:, cols(t)] = r.acc[:, 0:TC].astype(BF16)
    send_grads(1, (6, 3, 5))
    wait_dh = plane_gather(r.pl.dh, r.dhn)
    for j in range(4):
        core_sum(r.y, me.dest(j))
    wait_dc()
    for k in range(NBLK):
        total = r.dc_in[k] + r.dc_plane[0, k] + r.dc_plane[1, k] + r.dc_plane[2, k]
        r.dc_t[2 * k : 2 * k + 2, :] = total[0:2, :]
    dc = r.dc_t[:, 0:TB]
    combine = r.comb[b, :, 0:TB]
    d_logits = combine * (dc - jnp.sum(combine * dc, axis=0, keepdims=True))
    d_logits = d_logits.astype(BF16)
    r.flat[0:16, :] = jnp.dot(d_logits, r.hn[rows(b), :], preferred_element_type=F32)

    wait_dh()

    r.dh[...] = r.dhn[...].astype(F32) + contract(d_logits, r.router_t[...], 0, 0)
    r.flat[16:24, :] = jnp.zeros((8, DM), F32)

    def norm_two_back(chunk):
        dhn = r.dh[chunk, :]
        unit = r.hidden[chunk, :] * r.r_two[chunk, :]
        r.flat[16:17, :] += jnp.sum(dhn * unit, axis=0, keepdims=True)
        du = dhn * r.gains[1:2, :]
        mean = jnp.mean(du * unit, axis=1, keepdims=True)
        dh = r.gout[chunk, :] + r.r_two[chunk, :] * (du - unit * mean)
        r.dh[chunk, :] = dh
        r.dproj[chunk, :] = (residual_scale * dh).astype(BF16)

    row_chunks(norm_two_back)

    def to_owners(store, sems, width):
        send, recv = sems
        for k in range(NBLK):
            store.own[k, :, 0:TB] = r.flat[0:width, TB * k : TB * (k + 1)]
        store.inn[b] = store.own[b]
        for k in range(1, NBLK):
            peer = me.other(k)
            pend.begin(
                remote(
                    store.own.at[peer], store.inn.at[b], send.at[0], recv.at[0],
                    me.at_block(peer),
                )
            )
        seven = store.own.at[0:7]
        all_seven = remote(seven, seven, send.at[0], recv.at[0], me.partner())
        pend.later(all_seven)

        def wait():
            all_seven.wait_recv()
            total = store.inn[0]
            for k in range(1, NBLK):
                total = total + store.inn[k]
            return total

        return wait

    wait_sm = to_owners(r.sm, r.aa.sm, 24)

    for i in range(3):
        g_wout.cross(i)
    g_wout.finish()
    d_o = contract(r.dproj[...], r.w_out[cols(t), :], 1, 1).astype(BF16).astype(F32)
    for h in range(NQ):
        pair = h // 2
        dh_z = head_from_chunk(d_o[:, 128 * pair : 128 * (pair + 1)], h)
        den = r.den[h]
        r.dnz[h] = (dh_z / den).astype(BF16)
        r.den[h] = (
            jnp.broadcast_to(jnp.sum(dh_z * r.oz[h], axis=1, keepdims=True), (TB, 128)) / den
        )
        r.oz[h] = jnp.zeros((TB, 128), F32)

    def out_grads(n, carry):
        lanes = pl.ds(pl.multiple_of(n * 256, 256), 256)
        g_out_part[lanes, :] = contract(
            r.o_full[:, lanes], r.dproj[:, cols(t)], 0, 0
        ).astype(BF16)
        return carry

    lax.fori_loop(0, DM // 256, out_grads, 0)

    class Reduce(Chain):
        def __init__(self, part, own):
            self.part, self.core, self.sems = part, own.core, own.sems
            super().__init__(
                lambda i: part.at[rows(2 * i + c), :], own.line, own.sems[2], own.sems[3], self.chip
            )

        def core_copy(self, i):
            return remote(
                self.part.at[rows(2 * i + (1 - c)), :],
                self.core.at[i],
                self.sems[0].at[0],
                self.sems[1].at[i],
                me.partner(),
            )

        def start(self):
            for j in range(4):
                self.core_copy(me.dest(j)).start()

        def chip(self, i):
            self.core_copy(i).wait_recv()
            piece = self.piece(i)
            piece[...] = (piece[...].astype(F32) + self.core[i].astype(F32)).astype(BF16)

        def drain(self):
            super().drain()
            self.drain_core()

        def drain_core(self):
            remote(
                self.core, self.core, self.sems[0].at[0], self.sems[1].at[0], me.partner()
            ).wait_send()

        def down(self):
            for i in range(4):
                self.chip(i)

            @pl.when(z == 1)
            def _():
                self.wait_slot(0)
                piece = self.piece(0)
                piece[...] = (piece[...].astype(F32) + self.line[0].astype(F32)).astype(BF16)

            for i, slot, when in (
                (0, 0, z == 2),
                (1, 5, z == 2),
                (0, 5, z == 1),
                (2, 5, z + c == 4),
            ):
                pend.start(
                    remote(
                        self.piece(i),
                        self.line.at[slot],
                        self.send.at[1 if i == 1 else 0],
                        self.recv.at[slot],
                        me.at_z(z - 1),
                    ),
                    when,
                )

        def down_total(self, acc):
            acc[...] = self.piece(z)[...].astype(F32)

            @pl.when(z < 2 + c)
            def _():
                self.wait_slot(5)
                acc[...] += self.line[5].astype(F32)

    red_out = Reduce(g_out_part, r.rd.go)
    red_out.start()
    red_out.steps(z * (3 - z) == 0)

    for j in range(4):
        plane_relay(r.y, me.dest(j))
    def clear(i, carry):
        r.dkv[rows(i), :] = jnp.zeros((TB, 256), BF16)
        return carry

    lax.fori_loop(0, NBLK, clear, 0)

    def attend_back(kb, carry):
        keys = r.kv[rows(kb), 0:128]
        values = r.kv[rows(kb), 128:256]
        mask = allowed(kb)
        dk = jnp.zeros((TB, 128), F32)
        dv = jnp.zeros((TB, 128), F32)
        for g in range(2):
            heads = pl.ds(3 * g, 3)
            q = r.qz[heads].reshape(3 * TB, 128)
            dn = r.dnz[heads].reshape(3 * TB, 128)
            e = jnp.exp(contract(q, keys, 1, 1) * score_scale).reshape(3, TB, TB)
            e = jnp.where(mask[None], e, 0.0)
            dp = contract(dn, values, 1, 1).reshape(3, TB, TB)
            ds = (e * (dp - r.den[heads][:, :, 0:1])).reshape(3 * TB, TB).astype(BF16)
            e = e.reshape(3 * TB, TB).astype(BF16)
            r.oz[heads] += jnp.dot(ds, keys, preferred_element_type=F32).reshape(3, TB, 128)
            dk = dk + contract(ds, q, 0, 0)
            dv = dv + contract(e, dn, 0, 0)
        r.dkv[rows(kb), 0:128] = (dk * score_scale).astype(BF16)
        r.dkv[rows(kb), 128:256] = dv.astype(BF16)
        return carry

    lax.fori_loop(first_block, b + 1, attend_back, 0)
    red_kv = Reduce(r.dkv, r.rd.dkv)
    red_kv.start()
    for pair in range(3):
        heads = [
            jnp.where(half_mask(h // 3), r.oz[h] * score_scale, 0.0)
            for h in (2 * pair, 2 * pair + 1)
        ]
        u = chunk_from_heads(heads[0], heads[1], pair).astype(BF16).astype(F32)
        r.dqkv[:, 128 * pair : 128 * (pair + 1)] = (
            u * cosine - swap_halves(u) * sine
        ).astype(BF16)
    red_kv.down()

    def q_grads(n, carry):
        lanes = pl.ds(pl.multiple_of(n * 256, 256), 256)
        g_q_part[lanes, :] = contract(r.xn[:, lanes], r.dqkv[:, 0:TC], 0, 0).astype(BF16)
        return carry

    lax.fori_loop(0, DM // 256, q_grads, 0)
    red_gq = Reduce(g_q_part, r.rd.gq)
    red_gq.start()
    red_gq.steps()
    d_kv_acc = r.acc.at[:, 0:256]
    red_kv.down_total(d_kv_acc)
    d_kv = d_kv_acc[...].astype(BF16)
    u = d_kv[:, 0:128].astype(F32)
    r.dqkv[:, 384:512] = (u * cosine - swap_halves(u) * sine).astype(BF16)
    r.dqkv[:, 512:640] = d_kv[:, 128:256]

    for n in range(3):
        lanes = slice(512 * n, 512 * (n + 1))
        r.dx[:, lanes] = contract(r.dqkv[...], r.w_qkv[lanes, :], 1, 1).astype(BF16)
    wait_xs = to_plane(
        r.pl.xs, lambda k: (r.dx.at[:, cols(me.peer_t(k))], r.dx_in.at[k - 1]), r.dx_in
    )

    def kv_grads(n, carry):
        lanes = pl.ds(pl.multiple_of(n * 256, 256), 256)
        g_kv_part[lanes, :] = contract(r.xn[:, lanes], r.dqkv[:, TC:640], 0, 0).astype(BF16)
        return carry

    lax.fori_loop(0, DM // 256, kv_grads, 0)
    red_gkv = Reduce(g_kv_part, r.rd.gkv)
    red_gkv.start()
    red_gq.total(r.acc.at[:, 0:TC])
    r.g_qkv_sum[:, 0:TC] = r.acc[:, 0:TC].astype(BF16)
    for j in range(3):
        red_gkv.step(j)
    red_out.steps(me.middle())
    send_grads(1, (4,))
    wait_xs()
    total = r.dx[:, cols(t)].astype(F32)
    for k in range(3):
        total = total + r.dx_in[k].astype(F32)
    r.dxn[:, cols(t)] = total.astype(BF16)
    wait_dx = plane_gather(r.pl.xg, r.dxn)
    wait_dx()
    r.flat[0:8, :] = jnp.zeros((8, DM), F32)

    def norm_one_back(chunk):
        dxn = r.dxn[chunk, :].astype(F32)
        factor = r.r_one[chunk, :]
        unit = r.x[chunk, :].astype(F32) * factor
        r.flat[0:1, :] += jnp.sum(dxn * unit, axis=0, keepdims=True)
        du = dxn * r.gains[0:1, :]
        mean = jnp.mean(du * unit, axis=1, keepdims=True)
        r.grad_in[chunk, :] = r.dh[chunk, :] + factor * (du - unit * mean)

    row_chunks(norm_one_back)
    wait_sn = to_owners(r.sn, r.aa.sn, 8)
    own_qkv, from_qkv = [], []

    def give(n, start, width, target, sems, three):
        def lanes(index):
            return pl.ds(pl.multiple_of(width * index, 128), width)

        piece = r.g_qkv_sum.at[:, start : start + width]
        there = target.at[:, lanes(t)]
        own = pltpu.make_async_copy(piece, there, loc.at[1 + n])
        own.start()
        own_qkv.append(own)
        from_qkv.append(to_plane(sems, lambda k: (piece, there), three))

    give(0, 0, TC, r.gq_out, r.pl.gq, r.dx_in)
    red_gkv.total(r.acc.at[:, 0:256])
    r.g_qkv_sum[:, TC:640] = r.acc[:, 0:256].astype(BF16)
    give(1, 384, 128, r.gk_out, r.pl.gk, r.g_qkv_sum.at[:, 0:TC])
    give(2, 512, 128, r.gv_out, r.pl.gv, r.g_qkv_sum.at[:, 0:TC])
    red_out.total(r.acc.at[:, 0:TC])
    r.g_out_sum[...] = r.acc[:, 0:TC].astype(BF16)
    own_go = pltpu.make_async_copy(r.g_out_sum, r.g_out_out.at[:, cols(t)], loc.at[0])
    own_go.start()
    go_there = r.g_out_out.at[:, cols(t)]
    wait_go = to_plane(r.pl.go, lambda k: (r.g_out_sum, go_there), r.dx_in)
    chain_y.steps()
    chain_y.total(r.acc.at[:, 0:TC])
    r.block_out[...] = r.hidden[:, cols(t)] + residual_scale * r.acc[:, 0:TC]
    r.sm_out[...] = wait_sm()
    r.sn_out[...] = wait_sn()

    wait_go()
    for wait in from_qkv:
        wait()
    own_go.wait()
    for copy in own_qkv:
        copy.wait()
    for copy in own_grads:
        copy.wait()
    for e in range(2):
        seven_blocks(r.aa.gm[e]).wait()
        seven_blocks(r.aa.wm[e]).wait_send()
    scatter_drain(r.h)
    scatter_drain(r.y)
    chain_h.drain()
    chain_y.drain()
    red_out.drain()
    red_kv.drain_core()
    red_gq.drain()
    red_gkv.drain()
    pend.drain()


def fast_body(
    block_input,
    segments,
    routes,
    attn_gain,
    ffn_gain,
    query_weight,
    key_matrix,
    value_matrix,
    out_weight,
    router_weight,
    gate_weight,
    up_weight,
    down_weight,
    grad_output,
):
    half = HEAD_DIM // 2
    inverse = rope_base ** (-(np.arange(half, dtype=np.float64) * 2.0 / HEAD_DIM))
    inverse = np.tile(inverse.astype(np.float32).astype(np.float64), 4)

    def table(positions):
        angles = positions[:, None] * inverse[None, :]
        return np.stack([np.cos(angles), np.sin(angles)]).astype(np.float32)

    vectors = (
        jnp.pad(segments, (0, 512)).astype(F32)
        + jnp.pad(attn_gain.astype(F32), (DM, 320))
        + jnp.pad(ffn_gain.astype(F32), (DM + 256, 64))
    ).reshape(16, 128)
    vmem, hbm = pl.BlockSpec(memory_space=pltpu.VMEM), pl.BlockSpec(memory_space=pl.ANY)
    ins = dict(
        x=(block_input, vmem),
        gout=(grad_output, vmem),
        rope_block=(jnp.asarray(table(np.arange(NBLK) * TB)), vmem),
        rope_row=(jnp.asarray(table(np.arange(TB))), vmem),
        vectors=(vectors, vmem),
        routes_t=(routes.T, vmem),
        router_own=(router_weight.T, vmem),
        wq=(query_weight, hbm),
        wk=(key_matrix, hbm),
        wv=(value_matrix, hbm),
        wo=(out_weight, hbm),
        gate=(gate_weight, hbm),
        up=(up_weight, hbm),
        down_t=(down_weight.transpose(0, 2, 1), hbm),
    )
    outs = dict(
        block_out=((TB, TC), F32, vmem),
        grad_in=((TB, DM), F32, vmem),
        sm_out=((24, 256), F32, vmem),
        sn_out=((8, 256), F32, vmem),
        gq_out=((TB, DM), BF16, hbm),
        gk_out=((TB, 512), BF16, hbm),
        gv_out=((TB, 512), BF16, hbm),
        g_out_out=((TB, DM), BF16, hbm),
        gate_out=((E, TB, 128), BF16, hbm),
        up_out=((E, TB, 128), BF16, hbm),
        down_out=((E, TB, 128), BF16, hbm),
    )
    leaves, tree = jax.tree.flatten(scratch_tree())

    def entry(*refs):
        table = bags(jax.tree.unflatten(tree, refs[len(ins) + len(outs) :]))
        table.update(zip((*ins, *outs), refs))
        kernel(table)

    results = pl.pallas_call(
        entry,
        name="layer",
        out_shape=[jax.ShapeDtypeStruct(shape, kind) for shape, kind, _ in outs.values()],
        in_specs=[spec for _, spec in ins.values()],
        out_specs=[spec for _, _, spec in outs.values()],
        scratch_shapes=leaves,
        compiler_params=pltpu.CompilerParams(
            collective_id=0, has_side_effects=True, vmem_limit_bytes=VMEM_BYTES
        ),
    )(*[value for value, _ in ins.values()])
    res = Bag(zip(outs, results))
    wide = widen(
        res.block_out, res.grad_in, res.gq_out, res.gk_out, res.gv_out, res.g_out_out,
        res.gate_out, res.up_out, res.down_out, res.sm_out, res.sn_out,
    )
    block_output, grad_input, g_query, g_key, g_value, g_out, gate, up, down = wide[:9]
    router, gain_two, gain_one = wide[9:]
    return (
        block_output,
        grad_input,
        gain_one.reshape(TB),
        gain_two.reshape(TB),
        g_query,
        g_key,
        g_value,
        g_out,
        router.T,
        gate,
        up,
        down.transpose(0, 2, 1),
    )


def widen(*arrays):
    steps = 4

    def spec(shape):
        rest = (0,) * (len(shape) - 1)
        return pl.BlockSpec((shape[0] // steps, *shape[1:]), lambda i: (i, *rest))

    def entry(*refs):
        count = len(arrays)
        for source, target in zip(refs[: count - 2], refs[count:]):
            target[...] = source[...].astype(F32)
        sm, sn = refs[count - 2 : count]
        router, gain_two, gain_one = refs[-3:]
        router[...] = sm[0:16, 0:TB]
        gain_two[...] = sm[16:17, 0:TB]
        gain_one[...] = sn[0:1, 0:TB]

    def whole(*shape):
        return pl.BlockSpec(shape, lambda i: (0, 0))

    specs = [spec(a.shape) for a in arrays[:-2]]
    return pl.pallas_call(
        entry,
        name="widen",
        grid=(steps,),
        in_specs=[*specs, whole(24, 256), whole(8, 256)],
        out_specs=[*specs, whole(16, TB), whole(1, TB), whole(1, TB)],
        out_shape=[
            *(jax.ShapeDtypeStruct(a.shape, F32) for a in arrays[:-2]),
            jax.ShapeDtypeStruct((16, TB), F32),
            jax.ShapeDtypeStruct((1, TB), F32),
            jax.ShapeDtypeStruct((1, TB), F32),
        ],
        cost_estimate=pl.CostEstimate(flops=4_000_000, bytes_accessed=16_000_000, transcendentals=0),
    )(*arrays)


VMEM_BYTES = 67043328


def fits(mesh):
    return (mesh.shape["fsdp"], mesh.shape["heads"], mesh.shape["tensor"]) == (4, 2, 4)


def solution(mesh):
    in_specs = (
        P(("fsdp", "heads"), None),
        P(),
        P(("fsdp", "heads"), None),
        P(("fsdp", "heads")),
        P(("fsdp", "heads")),
        P(("fsdp", "heads"), None),
        P(("fsdp", "heads"), None),
        P(("fsdp", "heads"), None),
        P(("fsdp", "heads"), None),
        P(("fsdp", "heads"), None),
        P(None, ("fsdp", "heads"), "tensor"),
        P(None, ("fsdp", "heads"), "tensor"),
        P(None, "tensor", ("fsdp", "heads")),
        P(("fsdp", "heads"), None),
    )
    out_specs = (
        P(("fsdp", "heads"), "tensor"),
        P(("fsdp", "heads"), None),
        P(("fsdp", "heads")),
        P(("fsdp", "heads")),
        P(("fsdp", "heads"), None),
        P(("fsdp", "heads"), None),
        P(("fsdp", "heads"), None),
        P(("fsdp", "heads"), None),
        P(("fsdp", "heads"), None),
        P(None, ("fsdp", "heads"), "tensor"),
        P(None, ("fsdp", "heads"), "tensor"),
        P(None, "tensor", ("fsdp", "heads")),
    )
    chosen = fast_body if fits(mesh) else body
    return jax.shard_map(chosen, mesh=mesh, in_specs=in_specs, out_specs=out_specs, check_vma=False)
```

```python
import math

import jax
import jax.numpy as jnp
import numpy as np
from jax import lax
from jax.experimental import pallas as pl
from jax.experimental.pallas import tpu as pltpu
from jax.sharding import PartitionSpec as P

QUERY_HEADS = 24
KEY_VALUE_HEADS = 8
HEAD_DIM = 64
E = 16


norm_eps = 1e-06
score_scale = 0.015625
residual_scale = 0.22
rope_base = 10000.0


def rotary_table(token_positions, head_size):
    half_size = head_size // 2
    inverse = rope_base ** (-(jnp.arange(half_size, dtype=jnp.float32) * 2.0 / head_size))
    angles = token_positions[:, None].astype(jnp.float32) * inverse[None, :]
    return (jnp.cos(angles)[:, None, :], jnp.sin(angles)[:, None, :])


def apply_rotary(vectors, cosine_lookup, sine_lookup):
    half_size = vectors.shape[-1] // 2
    first_half = vectors[..., :half_size]
    second_half = vectors[..., half_size:]
    return jnp.concatenate(
        [
            first_half * cosine_lookup - second_half * sine_lookup,
            second_half * cosine_lookup + first_half * sine_lookup,
        ],
        axis=-1,
    )


def reverse_rotary(gradient, cosine_lookup, sine_lookup):
    half_size = gradient.shape[-1] // 2
    first_half = gradient[..., :half_size]
    second_half = gradient[..., half_size:]
    return jnp.concatenate(
        [
            first_half * cosine_lookup + second_half * sine_lookup,
            second_half * cosine_lookup - first_half * sine_lookup,
        ],
        axis=-1,
    )


def body(
    block_input,
    segments,
    routes,
    attn_gain,
    ffn_gain,
    query_weight,
    key_matrix,
    value_matrix,
    out_weight,
    router_weight,
    gate_weight,
    up_weight,
    down_weight,
    grad_output,
):
    head_count = lax.axis_size("heads")
    n_tensor = lax.axis_size("tensor")
    n_fsdp = lax.axis_size("fsdp")
    fsdp_index = lax.axis_index("fsdp")
    heads_index = lax.axis_index("heads")
    tensor_index = lax.axis_index("tensor")
    token_rows = block_input.shape[0]
    model_width = block_input.shape[1]
    query_rows = token_rows * head_count
    seq_rows = query_rows * n_fsdp
    key_value_local = KEY_VALUE_HEADS // head_count
    heads_per_group = QUERY_HEADS // KEY_VALUE_HEADS
    slice_width = model_width // n_tensor
    gathered = (
        lax.all_gather(attn_gain, ("fsdp", "heads"), axis=0, tiled=True),
        lax.all_gather(ffn_gain, ("fsdp", "heads"), axis=0, tiled=True),
        lax.all_gather(query_weight, ("fsdp", "heads"), axis=0, tiled=True),
        lax.all_gather(key_matrix, ("fsdp", "heads"), axis=0, tiled=True),
        lax.all_gather(value_matrix, ("fsdp", "heads"), axis=0, tiled=True),
        lax.all_gather(out_weight, ("fsdp", "heads"), axis=0, tiled=True),
        lax.all_gather(router_weight, ("fsdp", "heads"), axis=0, tiled=True),
        lax.all_gather(gate_weight, ("fsdp", "heads"), axis=1, tiled=True),
        lax.all_gather(up_weight, ("fsdp", "heads"), axis=1, tiled=True),
        lax.all_gather(down_weight, ("fsdp", "heads"), axis=2, tiled=True),
    )
    gain_attn = gathered[0].astype(jnp.float32)
    gain_ffn = gathered[1].astype(jnp.float32)
    full_query, full_key, full_value, full_out, full_router, full_gate, full_up, full_down = (
        gathered[2:]
    )
    inputs = block_input.astype(jnp.float32)
    scale_one = lax.rsqrt(jnp.mean(inputs * inputs, axis=-1, keepdims=True) + norm_eps)
    unit_one = inputs * scale_one
    normalized_input = (unit_one * gain_attn).astype(jnp.bfloat16)
    query_lin = jnp.dot(normalized_input, full_query, preferred_element_type=jnp.float32)
    key_linear = jnp.dot(normalized_input, full_key, preferred_element_type=jnp.float32)
    value_lin = jnp.dot(normalized_input, full_value, preferred_element_type=jnp.float32)
    own_start = (fsdp_index * head_count + heads_index) * token_rows
    token_positions = own_start + jnp.arange(token_rows, dtype=jnp.int32)
    cosine_lookup, sine_lookup = rotary_table(token_positions, HEAD_DIM)
    query_send = (
        apply_rotary(
            query_lin.reshape(token_rows, QUERY_HEADS, HEAD_DIM), cosine_lookup, sine_lookup
        )
        .reshape(token_rows, QUERY_HEADS * HEAD_DIM)
        .astype(jnp.bfloat16)
    )
    key_send = (
        apply_rotary(
            key_linear.reshape(token_rows, KEY_VALUE_HEADS, HEAD_DIM), cosine_lookup, sine_lookup
        )
        .reshape(token_rows, KEY_VALUE_HEADS * HEAD_DIM)
        .astype(jnp.bfloat16)
    )
    value_send = value_lin.astype(jnp.bfloat16)
    query_heads, key_local, value_local = (
        lax.all_to_all(query_send, "heads", split_axis=1, concat_axis=0, tiled=True),
        lax.all_to_all(key_send, "heads", split_axis=1, concat_axis=0, tiled=True),
        lax.all_to_all(value_send, "heads", split_axis=1, concat_axis=0, tiled=True),
    )
    query_vectors = query_heads.reshape(query_rows, key_value_local, heads_per_group, HEAD_DIM)
    query_start = fsdp_index * query_rows
    query_pos = query_start + jnp.arange(query_rows, dtype=jnp.int32)
    query_seg = lax.dynamic_slice_in_dim(segments, query_start, query_rows, 0)

    def masked_exp(key_block, key_start):
        block_rows = key_block.shape[0]
        raw_scores = (
            jnp.einsum(
                "qkgd,jkd->kgqj", query_vectors, key_block, preferred_element_type=jnp.float32
            )
            * score_scale
        )
        key_pos = key_start + jnp.arange(block_rows, dtype=jnp.int32)
        key_seg = lax.dynamic_slice_in_dim(segments, key_start, block_rows, 0)
        allowed = (query_pos[:, None] >= key_pos[None, :]) & (
            query_seg[:, None] == key_seg[None, :]
        )
        return jnp.where(allowed[None, None], jnp.exp(raw_scores), 0.0)

    def split_blocks(key_piece):
        keys_piece, values_piece = key_piece
        piece_rows = keys_piece.shape[0]
        block_rows = math.gcd(piece_rows, query_rows)
        block_count = piece_rows // block_rows
        starts = jnp.arange(block_count, dtype=jnp.int32) * block_rows
        return (
            keys_piece.reshape(block_count, block_rows, key_value_local, HEAD_DIM),
            values_piece.reshape(block_count, block_rows, key_value_local, HEAD_DIM),
            starts,
        )

    start_state = (
        jnp.zeros((key_value_local, heads_per_group, query_rows), jnp.float32),
        jnp.zeros((key_value_local, heads_per_group, query_rows, HEAD_DIM), jnp.float32),
    )
    fold_state = start_state

    def block_step(running, block_item):
        denominator, numerator = running
        key_block, value_block, key_start = block_item
        weights = masked_exp(key_block, key_start)
        denominator = denominator + jnp.sum(weights, axis=-1)
        numerator = numerator + jnp.einsum(
            "kgqj,jkd->kgqd",
            weights.astype(jnp.bfloat16),
            value_block,
            preferred_element_type=jnp.float32,
        )
        return ((denominator, numerator), None)

    fold_state, _ = lax.scan(
        block_step,
        fold_state,
        split_blocks(
            (
                lax.all_gather(key_local, "fsdp", axis=0, tiled=True),
                lax.all_gather(value_local, "fsdp", axis=0, tiled=True),
            )
        ),
    )
    denominator, numerator = fold_state
    attn_full = numerator / denominator[..., None]
    attn_send = (
        attn_full.transpose(2, 0, 1, 3)
        .reshape(query_rows, key_value_local * heads_per_group * HEAD_DIM)
        .astype(jnp.bfloat16)
    )
    attn_back = lax.all_to_all(attn_send, "heads", split_axis=0, concat_axis=1, tiled=True)
    attn_proj = jnp.dot(attn_back, full_out, preferred_element_type=jnp.float32)
    hidden = inputs + residual_scale * attn_proj
    scale_two = lax.rsqrt(jnp.mean(hidden * hidden, axis=-1, keepdims=True) + norm_eps)
    unit_two = hidden * scale_two
    normed_two = (unit_two * gain_ffn).astype(jnp.bfloat16)
    logits = jnp.dot(normed_two, full_router, preferred_element_type=jnp.float32)
    onehot = (routes[:, :, None] == jnp.arange(E, dtype=jnp.int32)[None, None, :]).astype(
        jnp.float32
    )
    picked = jnp.sum(onehot * logits[:, None, :], axis=-1)
    route_probs = jax.nn.softmax(picked, axis=-1)
    combine = jnp.sum(onehot * route_probs[:, :, None], axis=1)
    gate_pre = jnp.einsum("td,edf->etf", normed_two, full_gate, preferred_element_type=jnp.float32)
    up_pre = jnp.einsum("td,edf->etf", normed_two, full_up, preferred_element_type=jnp.float32)
    sigmoid_gate = jax.nn.sigmoid(gate_pre)
    silu_gate = gate_pre * sigmoid_gate
    active = (silu_gate * up_pre).astype(jnp.bfloat16)
    expert_out = jnp.einsum("etf,efd->etd", active, full_down, preferred_element_type=jnp.float32)
    mixed_part = jnp.sum(combine.T[:, :, None] * expert_out, axis=0)
    mixed_sum = lax.psum_scatter(
        mixed_part.astype(jnp.bfloat16), "tensor", scatter_dimension=1, tiled=True
    ).astype(jnp.float32)
    hidden_mine = lax.dynamic_slice_in_dim(hidden, tensor_index * slice_width, slice_width, 1)
    block_output = hidden_mine + residual_scale * mixed_sum
    mixed_grad = residual_scale * grad_output
    expert_grad = (combine.T[:, :, None] * mixed_grad[None]).astype(jnp.bfloat16)
    combine_part = jnp.sum(expert_out * mixed_grad[None], axis=-1).T
    active_grad = jnp.einsum(
        "etd,efd->etf", expert_grad, full_down, preferred_element_type=jnp.float32
    )
    gate_grad = (
        active_grad * up_pre * sigmoid_gate * (1.0 + gate_pre * (1.0 - sigmoid_gate))
    ).astype(jnp.bfloat16)
    up_grad = (active_grad * silu_gate).astype(jnp.bfloat16)
    normed_part = jnp.einsum(
        "etf,edf->td", gate_grad, full_gate, preferred_element_type=jnp.float32
    ) + jnp.einsum("etf,edf->td", up_grad, full_up, preferred_element_type=jnp.float32)
    gate_full = jnp.einsum("td,etf->edf", normed_two, gate_grad, preferred_element_type=jnp.float32)
    up_full = jnp.einsum("td,etf->edf", normed_two, up_grad, preferred_element_type=jnp.float32)
    down_full = jnp.einsum("etf,etd->efd", active, expert_grad, preferred_element_type=jnp.float32)
    grad_gate, grad_up, grad_down = (
        lax.psum_scatter(gate_full.astype(jnp.bfloat16), ("fsdp", "heads"), scatter_dimension=1, tiled=True),
        lax.psum_scatter(up_full.astype(jnp.bfloat16), ("fsdp", "heads"), scatter_dimension=1, tiled=True),
        lax.psum_scatter(down_full.astype(jnp.bfloat16), ("fsdp", "heads"), scatter_dimension=2, tiled=True),
    )
    normed_grad, combine_grad = lax.psum((normed_part, combine_part), "tensor")
    pick_grad = jnp.sum(onehot * combine_grad[:, None, :], axis=-1)
    picked_grad = route_probs * (
        pick_grad - jnp.sum(route_probs * pick_grad, axis=-1, keepdims=True)
    )
    logit_grad = jnp.sum(onehot * picked_grad[:, :, None], axis=1).astype(jnp.bfloat16)
    router_full = jnp.dot(normed_two.T, logit_grad, preferred_element_type=jnp.float32)
    normed_grad = normed_grad + jnp.dot(
        logit_grad, full_router.T, preferred_element_type=jnp.float32
    )
    gain_ffn_full = jnp.sum(normed_grad * unit_two, axis=0)
    unit_grad = normed_grad * gain_ffn
    hidden_grad = grad_output + scale_two * (
        unit_grad - unit_two * jnp.mean(unit_grad * unit_two, axis=-1, keepdims=True)
    )
    proj_grad = (residual_scale * hidden_grad).astype(jnp.bfloat16)
    out_full = jnp.dot(attn_back.T, proj_grad, preferred_element_type=jnp.float32)
    attn_grad = jnp.dot(proj_grad, full_out.T, preferred_element_type=jnp.float32).astype(
        jnp.bfloat16
    )
    grad_heads = lax.all_to_all(attn_grad, "heads", split_axis=1, concat_axis=0, tiled=True)
    grad_float = (
        grad_heads.reshape(query_rows, key_value_local, heads_per_group, HEAD_DIM)
        .transpose(1, 2, 0, 3)
        .astype(jnp.float32)
    )
    scaled_grad = (grad_float / denominator[..., None]).astype(jnp.bfloat16)
    shift_term = jnp.sum(grad_float * attn_full, axis=-1) / denominator
    start_back = (
        jnp.zeros((key_value_local, heads_per_group, query_rows, HEAD_DIM), jnp.float32),
        jnp.zeros((seq_rows, key_value_local * HEAD_DIM), jnp.float32),
        jnp.zeros((seq_rows, key_value_local * HEAD_DIM), jnp.float32),
    )
    fold_state = start_back

    def block_step(running, block_item):
        query_acc, key_acc, value_acc = running
        key_block, value_block, key_start = block_item
        block_rows = key_block.shape[0]
        weights = masked_exp(key_block, key_start)
        dot_grad = jnp.einsum(
            "kgqd,jkd->kgqj", scaled_grad, value_block, preferred_element_type=jnp.float32
        )
        score_grad = (weights * (dot_grad - shift_term[..., None])).astype(jnp.bfloat16)
        query_acc = (
            query_acc
            + jnp.einsum(
                "kgqj,jkd->kgqd", score_grad, key_block, preferred_element_type=jnp.float32
            )
            * score_scale
        )
        key_part = (
            jnp.einsum(
                "kgqj,qkgd->jkd", score_grad, query_vectors, preferred_element_type=jnp.float32
            )
            * score_scale
        )
        value_part = jnp.einsum(
            "kgqj,kgqd->jkd",
            weights.astype(jnp.bfloat16),
            scaled_grad,
            preferred_element_type=jnp.float32,
        )
        key_old = lax.dynamic_slice_in_dim(key_acc, key_start, block_rows, 0)
        value_old = lax.dynamic_slice_in_dim(value_acc, key_start, block_rows, 0)
        key_acc = lax.dynamic_update_slice_in_dim(
            key_acc,
            key_old + key_part.reshape(block_rows, key_value_local * HEAD_DIM),
            key_start,
            0,
        )
        value_acc = lax.dynamic_update_slice_in_dim(
            value_acc,
            value_old + value_part.reshape(block_rows, key_value_local * HEAD_DIM),
            key_start,
            0,
        )
        return ((query_acc, key_acc, value_acc), None)

    fold_state, _ = lax.scan(
        block_step,
        fold_state,
        split_blocks(
            (
                lax.all_gather(key_local, "fsdp", axis=0, tiled=True),
                lax.all_gather(value_local, "fsdp", axis=0, tiled=True),
            )
        ),
    )
    query_acc, key_acc, value_acc = fold_state
    key_mine, value_mine = (
        lax.psum_scatter(key_acc, "fsdp", scatter_dimension=0, tiled=True),
        lax.psum_scatter(value_acc, "fsdp", scatter_dimension=0, tiled=True),
    )
    query_send_back = (
        query_acc.transpose(2, 0, 1, 3)
        .reshape(query_rows, key_value_local * heads_per_group * HEAD_DIM)
        .astype(jnp.bfloat16)
    )
    query_ret, key_returned, value_ret = (
        lax.all_to_all(query_send_back, "heads", split_axis=0, concat_axis=1, tiled=True),
        lax.all_to_all(
            key_mine.astype(jnp.bfloat16), "heads", split_axis=0, concat_axis=1, tiled=True
        ),
        lax.all_to_all(
            value_mine.astype(jnp.bfloat16), "heads", split_axis=0, concat_axis=1, tiled=True
        ),
    )
    query_lin_grad = (
        reverse_rotary(
            query_ret.astype(jnp.float32).reshape(token_rows, QUERY_HEADS, HEAD_DIM),
            cosine_lookup,
            sine_lookup,
        )
        .reshape(token_rows, QUERY_HEADS * HEAD_DIM)
        .astype(jnp.bfloat16)
    )
    key_lin_grad = (
        reverse_rotary(
            key_returned.astype(jnp.float32).reshape(token_rows, KEY_VALUE_HEADS, HEAD_DIM),
            cosine_lookup,
            sine_lookup,
        )
        .reshape(token_rows, KEY_VALUE_HEADS * HEAD_DIM)
        .astype(jnp.bfloat16)
    )
    query_full = jnp.dot(normalized_input.T, query_lin_grad, preferred_element_type=jnp.float32)
    key_full = jnp.dot(normalized_input.T, key_lin_grad, preferred_element_type=jnp.float32)
    value_full = jnp.dot(normalized_input.T, value_ret, preferred_element_type=jnp.float32)
    normed_one_grad = jnp.dot(query_lin_grad, full_query.T, preferred_element_type=jnp.float32)
    normed_one_grad = normed_one_grad + jnp.dot(
        key_lin_grad, full_key.T, preferred_element_type=jnp.float32
    )
    normed_one_grad = normed_one_grad + jnp.dot(
        value_ret, full_value.T, preferred_element_type=jnp.float32
    )
    gain_attn_full = jnp.sum(normed_one_grad * unit_one, axis=0)
    unit_one_grad = normed_one_grad * gain_attn
    grad_input = hidden_grad + scale_one * (
        unit_one_grad - unit_one * jnp.mean(unit_one_grad * unit_one, axis=-1, keepdims=True)
    )
    grad_attn_gain, grad_ffn_gain, grad_query, grad_key, grad_value, grad_out_proj, grad_router = (
        lax.psum_scatter(gain_attn_full, ("fsdp", "heads"), scatter_dimension=0, tiled=True),
        lax.psum_scatter(gain_ffn_full, ("fsdp", "heads"), scatter_dimension=0, tiled=True),
        lax.psum_scatter(query_full.astype(jnp.bfloat16), ("fsdp", "heads"), scatter_dimension=0, tiled=True),
        lax.psum_scatter(key_full.astype(jnp.bfloat16), ("fsdp", "heads"), scatter_dimension=0, tiled=True),
        lax.psum_scatter(value_full.astype(jnp.bfloat16), ("fsdp", "heads"), scatter_dimension=0, tiled=True),
        lax.psum_scatter(out_full.astype(jnp.bfloat16), ("fsdp", "heads"), scatter_dimension=0, tiled=True),
        lax.psum_scatter(router_full, ("fsdp", "heads"), scatter_dimension=0, tiled=True),
    )
    grad_query, grad_key, grad_value, grad_out_proj, grad_gate, grad_up, grad_down = (
        g.astype(jnp.float32)
        for g in (grad_query, grad_key, grad_value, grad_out_proj, grad_gate, grad_up, grad_down)
    )
    return (
        block_output,
        grad_input,
        grad_attn_gain,
        grad_ffn_gain,
        grad_query,
        grad_key,
        grad_value,
        grad_out_proj,
        grad_router,
        grad_gate,
        grad_up,
        grad_down,
    )


MESH_ID = pl.DeviceIdType.MESH
F32 = jnp.float32
BF16 = jnp.bfloat16

TB = 192
DM = 1536
TC = 384
HALF = 96
NBLK = 8
NQ = 6
TOPK = 8
FIRST_DOC_BLOCKS = 5


def contract(left, right, left_dim, right_dim, precision=None):
    return lax.dot_general(
        left,
        right,
        (((left_dim,), (right_dim,)), ((), ())),
        preferred_element_type=F32,
        precision=precision,
    )


def rows(index):
    return pl.ds(pl.multiple_of(index * TB, TB), TB)


def cols(index):
    return pl.ds(pl.multiple_of(index * TC, 128), TC)


class Place:
    def __init__(self):
        self.z = lax.axis_index("fsdp")
        self.c = lax.axis_index("heads")
        self.t = lax.axis_index("tensor")
        self.b = 2 * self.z + self.c

    def partner(self):
        return (self.z, 1 - self.c, self.t)

    def at_z(self, z):
        return (z, self.c, self.t)

    def at_block(self, block):
        return (block // 2, block % 2, self.t)

    def peer_t(self, k):
        if k == 1:
            return self.t + 1 - 2 * (self.t % 2)
        if k == 2:
            return (self.t + 2) % 4
        return 3 - self.t

    def plane(self, k):
        return (self.z, self.c, self.peer_t(k))

    def other(self, k):
        return (self.b + k) % NBLK

    def arrival(self, i):
        if i == 0:
            return self.z + 1 - 2 * (self.z % 2)
        if i == 1:
            return 2 - self.z // 2
        return 3 - 3 * (self.z // 2)

    def forward_to(self, i):
        return 3 - self.z if i == 0 else 3 * (self.z - 1)

    def middle(self):
        return self.z * (3 - self.z) > 0

    def dest(self, j):
        inner = (self.z * (3 - self.z)) // 2
        turned = j + inner * (j // 2) * (1 - 2 * (j % 2))
        upper = self.z // 2
        return 3 * (1 - upper) + (2 * upper - 1) * turned


def remote(src, dst, send_sem, recv_sem, device):
    return pltpu.make_async_remote_copy(
        src_ref=src,
        dst_ref=dst,
        send_sem=send_sem,
        recv_sem=recv_sem,
        device_id=device,
        device_id_type=MESH_ID,
    )


class Pending:
    def __init__(self):
        self.items = []

    def start(self, copy, when=None):
        self.begin(copy, when)
        self.later(copy, when)

    def begin(self, copy, when=None):
        if when is None:
            copy.start()
        else:

            @pl.when(when)
            def _():
                copy.start()

    def later(self, copy, when=None):
        self.items.append((copy, when))

    def drain(self):
        for copy, when in self.items:
            if when is None:
                copy.wait_send()
            else:

                @pl.when(when)
                def _(copy=copy):
                    copy.wait_send()

        self.items = []


class LineGather:
    def __init__(self, me, pend, view, line_view, several, several_line, sems):
        self.me, self.pend, self.view, self.line_view = me, pend, view, line_view
        self.several, self.several_line = several, several_line
        self.send, self.recv, self.psend, self.precv = sems

    def bytes_of(self, ref, send_sem, recv_sem):
        return remote(ref, ref, send_sem.at[0], recv_sem.at[0], self.me.partner())

    def start(self):
        self.send_own()
        self.register()

    def register(self):
        me = self.me
        for count, when in ((5, me.middle()), (1, me.z * (3 - me.z) == 0)):
            self.pend.later(self.bytes_of(self.several_line(count), self.send, self.recv), when)
        self.register_shares()

    def send_own(self):
        me = self.me
        own = self.line_view(me.b)
        for dz, when in ((1, me.z < 3), (-1, me.z > 0)):
            self.pend.begin(
                remote(own, own, self.send.at[0], self.recv.at[me.z], me.at_z(me.z + dz)), when
            )
        self.share_block(me.b)

    def register_shares(self):
        self.pend.later(self.bytes_of(self.several(4), self.psend, self.precv))

    def share_own(self):
        self.share_block(self.me.b)
        self.register_shares()

    def share_block(self, block):
        whole = self.view(block)
        self.pend.begin(
            remote(whole, whole, self.psend.at[0], self.precv.at[0], self.me.partner())
        )

    def arrive(self, i):
        me = self.me
        source = me.arrival(i)
        block = self.line_view(2 * source + me.c)
        remote(block, block, self.send.at[0], self.recv.at[source], me.partner()).wait_recv()
        self.pend.begin(
            remote(
                block, block, self.send.at[0], self.recv.at[source], me.at_z(me.forward_to(i))
            ),
            me.middle(),
        )

    def share(self, i):
        self.share_block(2 * self.me.arrival(i) + self.me.c)

    def finish(self):
        self.bytes_of(self.several(4), self.psend, self.precv).wait_recv()


class UpGather(LineGather):
    def __init__(self, me, pend, view, sems):
        self.me, self.pend, self.view = me, pend, view
        self.send, self.recv, self.psend, self.precv = sems

    def start(self):
        me = self.me
        own = self.view(me.b)
        self.pend.start(
            remote(own, own, self.send.at[0], self.recv.at[me.z], me.at_z(me.z + 1)),
            me.z < 2 + me.c,
        )
        self.pend.start(remote(own, own, self.psend.at[3], self.precv.at[me.z], me.partner()))

    def near(self, core):
        return self.me.z * (3 + core - self.me.z) > 0

    def take(self, source):
        block = self.view(2 * source + self.me.c)
        remote(
            block, block, self.send.at[0], self.recv.at[source], self.me.partner()
        ).wait_recv()
        return block

    def relay(self):
        me = self.me

        @pl.when(self.near(me.c))
        def _():
            self.take(me.z - 1)

        block = self.view(2 * (me.z - 1) + me.c)
        self.pend.start(
            remote(block, block, self.send.at[1], self.recv.at[me.z - 1], me.at_z(me.z + 1)),
            me.z == 1,
        )
        self.pend.start(
            remote(block, block, self.psend.at[0], self.precv.at[me.z - 1], me.partner()),
            self.near(me.c),
        )

        @pl.when(me.z == 2)
        def _():
            self.take(0)

        block = self.view(me.c)
        self.pend.start(
            remote(block, block, self.psend.at[1], self.precv.at[0], me.partner()), me.z == 2
        )

    def finish(self):
        me = self.me

        def take(source):
            block = self.view(2 * source + (1 - me.c))
            remote(
                block, block, self.psend.at[0], self.precv.at[source], me.partner()
            ).wait_recv()

        take(me.z)

        @pl.when(self.near(1 - me.c))
        def _():
            take(me.z - 1)

        @pl.when(me.z == 2)
        def _():
            take(0)


class FullGather(LineGather):
    def __init__(self, me, pend, buffer, sems):
        super().__init__(
            me,
            pend,
            lambda block: buffer.at[rows(block), :],
            lambda block: buffer.at[rows(block), cols(me.t)],
            lambda count: buffer.at[0 : TB * count, :],
            lambda count: buffer.at[0 : TB * count, 0:TC],
            sems[:4],
        )
        self.buffer = buffer
        self.xsend, self.xrecv = sems[4:]

    def piece(self, i, k):
        lanes = cols(self.me.t if k == 0 else self.me.peer_t(k))
        return self.buffer.at[rows(2 * self.me.arrival(i) + self.me.c), lanes]

    def part(self, i, k, half):
        start = (2 * self.me.arrival(i) + self.me.c) * TB + HALF * half
        return self.buffer.at[pl.ds(pl.multiple_of(start, HALF), HALF), cols(self.me.peer_t(k))]

    def copy(self, view, i, relayed, k):
        return remote(
            view,
            view,
            self.xsend.at[0],
            self.xrecv.at[relayed, self.me.arrival(i)],
            self.me.plane(k),
        )

    def spread(self, i, last=True):
        for k in (1, 2):
            self.pend.begin(self.copy(self.piece(i, 0), i, 0, k))
        if i == 2 and last:
            self.register_spread()

    def register_spread(self):
        nine = self.buffer.at[0:864, 0:768]
        self.pend.later(self.copy(nine, 2, 0, 1))

    def relay(self, i):
        self.copy(self.buffer.at[0 : 2 * TB, 0:TC], i, 0, 1).wait_recv()
        for k in (1, 2):
            self.pend.begin(self.copy(self.part(i, k, k - 1), i, 1, 3 - k))

    def cross(self, i):
        self.copy(self.buffer.at[0:TB, 0:TC], i, 1, 1).wait_recv()
        self.share(i)


def swap_halves(u):
    lane = lax.broadcasted_iota(jnp.int32, u.shape, 1)
    return jnp.where(lane % 64 < 32, pltpu.roll(u, 96, 1), pltpu.roll(u, 32, 1))


def half_mask(half):
    lane = lax.broadcasted_iota(jnp.int32, (TB, 128), 1)
    return (lane // 64) == half


def head_from_chunk(chunk, h):
    if h % 2 != h // 3:
        chunk = pltpu.roll(chunk, 64, 1)
    return jnp.where(half_mask(h // 3), chunk, 0.0)


def chunk_from_heads(first, second, pair):
    if (2 * pair) // 3 != 0:
        first = pltpu.roll(first, 64, 1)
    if (2 * pair + 1) // 3 != 1:
        second = pltpu.roll(second, 64, 1)
    return jnp.where(half_mask(0), first, second)


def row_chunks(body, size=64):
    def step(i, carry):
        body(pl.ds(pl.multiple_of(i * size, size), size))
        return carry

    lax.fori_loop(0, TB // size, step, 0)


class Bag(dict):
    __getattr__ = dict.__getitem__


def bags(tree):
    return Bag({k: bags(v) for k, v in tree.items()}) if isinstance(tree, dict) else tree


def scratch_tree():
    def f32(*shape):
        return pltpu.VMEM(shape, F32)

    def b16(*shape):
        return pltpu.VMEM(shape, BF16)

    dma = pltpu.SemaphoreType.DMA

    def pair(*shape):
        return (dma(shape), dma(shape))

    def line():
        return (dma((1,)), dma((4,)), dma((1,)), dma((1,)))

    def up():
        return (dma((2,)), dma((4,)), dma((4,)), dma((4,)))

    def full():
        return (*line(), dma((1,)), dma((2, 4)))

    def scatter():
        return dict(
            part=b16(DM, DM),
            core=b16(4, TB, DM),
            plane=b16(4, 2, TB, TC),
            diagonal=b16(4, 2, HALF, TC),
            line=b16(6, TB, TC),
            sems=(dma((1,)), dma((4,)), dma((1,)), dma((4, 2)), dma((1,)), dma((6,))),
        )

    def reduce(width):
        return dict(
            core=b16(4, TB, width),
            line=b16(6, TB, width),
            sems=(dma((1,)), dma((4,)), dma((2,)), dma((6,))),
        )

    return dict(
        w_qkv=b16(DM, 640),
        small=f32(NBLK, 24, 256),
        w_out=b16(DM, DM),
        d_moe=b16(DM, DM),
        hn=b16(DM, DM),
        kv=b16(DM, 256),
        w_moe=b16(DM, 768),
        comb=f32(NBLK, 16, 256),
        xn=b16(TB, DM),
        r_one=f32(TB, 1),
        r_two=f32(TB, 1),
        hidden=f32(TB, DM),
        qz=b16(NQ, TB, 128),
        oz=f32(NQ, TB, 128),
        den=f32(NQ, TB, 128),
        o_full=b16(TB, DM),
        gains=f32(8, DM),
        router_t=b16(16, DM),
        dgu=b16(DM, 512),
        cz=b16(DM, 256),
        h=scatter(),
        y=scatter(),
        dhn=b16(TB, DM),
        dc_own=f32(NBLK, 8, 256),
        dc_in=f32(NBLK, 8, 256),
        dc_plane=f32(3, NBLK, 8, 256),
        dc_t=f32(16, 256),
        g_moe=b16(DM, 768),
        acc=f32(TB, TC),
        dh=f32(TB, DM),
        dproj=b16(TB, DM),
        flat=f32(24, DM),
        sm=dict(own=f32(NBLK, 24, 256), inn=f32(NBLK, 24, 256)),
        sn=dict(own=f32(NBLK, 8, 256), inn=f32(NBLK, 8, 256)),
        g_out_sum=b16(TB, TC),
        dnz=b16(NQ, TB, 128),
        dkv=b16(DM, 256),
        dqkv=b16(TB, 640),
        g_qkv_sum=b16(TB, 640),
        dx=b16(TB, DM),
        dx_in=b16(3, TB, TC),
        dxn=b16(TB, DM),
        local_sem=dma((11,)),
        lg=dict(s=line(), w=line(), v=line(), o=line(), kv=up(), c=line()),
        fg=dict(wo=full(), dm=full(), hn=full()),
        aa=dict(
            wm=[pair(1), pair(1)], gm=[pair(1), pair(1)], dc=pair(1), sm=pair(1), sn=pair(1)
        ),
        pl=dict(
            o=pair(1), hc=pair(1), dc=pair(1), dh=pair(1), go=pair(1), gq=pair(1), gk=pair(1),
            gv=pair(1), xs=pair(1), xg=pair(1),
        ),
        rd=dict(go=reduce(TC), dkv=reduce(256), gq=reduce(TC), gkv=reduce(256)),
    )


def kernel(r):
    g_out_part = r.dgu.at[:, 0:TC]
    w_column = r.y.part.at[:, 0:TC]
    g_q_part, g_kv_part = r.w_moe.at[:, 0:TC], r.w_moe.at[:, TC:640]
    me = Place()
    pend = Pending()
    z, c, t, b = me.z, me.c, me.t, me.b

    loc = r.local_sem
    local = [
        pltpu.make_async_copy(r.wq.at[:, cols(t)], r.w_qkv.at[rows(b), 0:384], loc.at[0]),
        pltpu.make_async_copy(
            r.wk.at[:, pl.ds(pl.multiple_of(128 * t, 128), 128)],
            r.w_qkv.at[rows(b), 384:512], loc.at[1],
        ),
        pltpu.make_async_copy(
            r.wv.at[:, pl.ds(pl.multiple_of(128 * t, 128), 128)],
            r.w_qkv.at[rows(b), 512:640], loc.at[2],
        ),
        pltpu.make_async_copy(r.wo.at[:, cols(t)], w_column.at[rows(b), :], loc.at[3]),
        pltpu.make_async_copy(r.wo, r.w_out.at[rows(b), :], loc.at[10]),
    ]
    moe_lanes = [[pl.ds(384 * e + 128 * which, 128) for which in range(3)] for e in range(2)]
    moe_sources = [list(zip((r.gate, r.up, r.down_t), lanes)) for lanes in moe_lanes]
    own_moe = [
        pltpu.make_async_copy(
            shard.at[2 * b + e], r.w_moe.at[rows(b), lanes], loc.at[4 + 3 * e + i]
        )
        for e in range(2)
        for i, (shard, lanes) in enumerate(moe_sources[e])
    ]
    for copy in local:
        copy.start()
    for copy in own_moe:
        copy.start()
    barrier = pltpu.get_barrier_semaphore()
    for k in range(1, NBLK):
        pl.semaphore_signal(
            barrier, inc=1, device_id=me.at_block(me.other(k)), device_id_type=MESH_ID
        )
    for k in (1, 2, 3):
        pl.semaphore_signal(barrier, inc=1, device_id=me.plane(k), device_id_type=MESH_ID)
    r.small[b, 0:16, 0:TB] = r.router_own[...].astype(F32)
    for n in range(2):
        r.small[b, 16 + n : 17 + n, 0:128] = r.vectors[12 + 2 * n : 13 + 2 * n, :]
        r.small[b, 16 + n : 17 + n, 128:TB] = r.vectors[13 + 2 * n : 14 + 2 * n, 0:64]
    r.d_moe[rows(b), :] = (residual_scale * r.gout[...]).astype(BF16)
    pl.semaphore_wait(barrier, NBLK - 1 + 3)

    def line(view, several, sems):
        return LineGather(me, pend, view, view, several, several, sems)

    g_small = line(lambda k: r.small.at[k], lambda n: r.small.at[0:n], r.lg.s)
    def columns(lanes, sems):
        return line(
            lambda k: r.w_qkv.at[rows(k), lanes], lambda n: r.w_qkv.at[0 : TB * n, lanes], sems
        )

    g_keys = columns(slice(TC, 640), r.lg.w)
    g_query = columns(slice(0, TC), r.lg.v)
    g_kv = UpGather(me, pend, lambda k: r.kv.at[rows(k), :], r.lg.kv)
    g_comb = line(lambda k: r.comb.at[k], lambda n: r.comb.at[0:n], r.lg.c)
    early = Pending()
    wcol_view = lambda k: w_column.at[rows(k), :]
    wcol_several = lambda n: w_column.at[0 : TB * n, :]
    g_wcol = LineGather(me, early, wcol_view, wcol_view, wcol_several, wcol_several, r.lg.o)
    g_wout = FullGather(me, pend, r.w_out, r.fg.wo)
    g_dmoe = FullGather(me, pend, r.d_moe, r.fg.dm)
    g_hn = FullGather(me, pend, r.hn, r.fg.hn)

    def send_weights_to(e, peer):
        send, recv = r.aa.wm[e]
        for shard, lanes in moe_sources[e]:
            remote(
                shard.at[2 * peer + e],
                r.w_moe.at[rows(b), lanes],
                send.at[0],
                recv.at[0],
                me.at_block(peer),
            ).start()

    end_chip = z * (3 - z) == 0

    def send_weights(e, ks, middle):
        for k in ks:
            peer = me.other(k)
            if middle:

                @pl.when(peer // 2 + z != 3)
                def _(peer=peer):
                    send_weights_to(e, peer)

            else:
                send_weights_to(e, peer)

    def send_weights_middle(e):
        for j in range(2):
            send_weights_to(e, 6 - 2 * z + j)

    def seven_blocks(sems):
        whole = r.w_moe.at[0 : 7 * TB, 0:TC]
        return remote(whole, whole, sems[0].at[0], sems[1].at[0], me.partner())

    g_small.start()
    for copy in local[1:3]:
        copy.wait()
    g_keys.start()
    local[0].wait()
    g_query.start()
    local[3].wait()
    g_wcol.start()

    def rms_one(chunk):
        v = r.x[chunk, :].astype(F32)
        r.r_one[chunk, :] = lax.rsqrt(jnp.mean(v * v, axis=1, keepdims=True) + norm_eps)

    row_chunks(rms_one)
    for i in range(3):
        g_small.arrive(i)
        g_small.share(i)
        g_keys.arrive(i)
        g_keys.share(i)
        if i > 0:
            g_query.arrive(i - 1)
            g_query.share(i - 1)

    @pl.when(me.middle())
    def _():
        send_weights_middle(0)

    g_small.finish()
    for k in range(NBLK):
        piece = r.small[k]
        r.router_t[:, TB * k : TB * (k + 1)] = piece[0:16, 0:TB].astype(BF16)
        r.gains[0:8, TB * k : TB * (k + 1)] = piece[16:24, 0:TB]

    def normalize_one(chunk):
        v = r.x[chunk, :].astype(F32)
        r.xn[chunk, :] = (v * r.r_one[chunk, :] * r.gains[0:1, :]).astype(BF16)

    row_chunks(normalize_one)
    g_keys.finish()
    key_value = jnp.dot(r.xn[...], r.w_qkv[:, TC:640], preferred_element_type=F32)
    base_c, base_s = r.rope_block[0, pl.ds(b, 1), :], r.rope_block[1, pl.ds(b, 1), :]
    row_c, row_s = r.rope_row[0], r.rope_row[1]
    first_half = lax.broadcasted_iota(jnp.int32, (TB, 128), 1) % 64 < 32
    cosine = base_c * row_c - base_s * row_s
    sine = base_s * row_c + base_c * row_s
    sine = jnp.where(first_half, -sine, sine)
    key = key_value[:, 0:128]
    r.kv[rows(b), 0:128] = (key * cosine + swap_halves(key) * sine).astype(BF16)
    r.kv[rows(b), 128:256] = key_value[:, 128:256].astype(BF16)
    g_kv.start()
    g_dmoe.send_own()
    g_query.arrive(2)
    g_query.share(2)
    g_wcol.arrive(0)
    g_wcol.share(0)
    g_kv.relay()
    g_query.finish()
    query = jnp.dot(r.xn[...], r.w_qkv[:, 0:TC], preferred_element_type=F32)
    for pair in range(3):
        u = query[:, 128 * pair : 128 * (pair + 1)]
        u = (u * cosine + swap_halves(u) * sine).astype(BF16).astype(F32)
        r.qz[2 * pair] = head_from_chunk(u, 2 * pair).astype(BF16)
        r.qz[2 * pair + 1] = head_from_chunk(u, 2 * pair + 1).astype(BF16)
    for h in range(NQ):
        r.oz[h] = jnp.zeros((TB, 128), F32)
        r.den[h] = jnp.zeros((TB, 128), F32)

    @pl.when(me.middle())
    def _():
        g_wcol.arrive(1)
        g_wcol.share(1)
        g_wcol.arrive(2)
        g_wcol.share(2)
        g_dmoe.arrive(0)
        g_dmoe.spread(0, False)
        send_weights_middle(1)
        send_weights(0, (1, 7, 2), True)

    @pl.when(end_chip)
    def _():
        send_weights(0, (1, 7, 2, 6), False)

    g_dmoe.register()
    g_dmoe.register_spread()
    g_kv.finish()

    first_block = FIRST_DOC_BLOCKS * (b // FIRST_DOC_BLOCKS)

    second_end = (r.vectors[0:12, :] < 1.5).astype(F32)
    second_end = jnp.sum(jnp.sum(second_end, axis=0, keepdims=True), axis=1, keepdims=True)

    def allowed(kb):
        q_pos = b * TB + lax.broadcasted_iota(jnp.int32, (TB, TB), 0)
        k_pos = kb * TB + lax.broadcasted_iota(jnp.int32, (TB, TB), 1)
        q_first = (q_pos.astype(F32) < second_end).astype(F32)
        k_first = (k_pos.astype(F32) < second_end).astype(F32)
        return (q_pos >= k_pos) & (q_first == k_first)

    def attend(kb, carry):
        keys = r.kv[rows(kb), 0:128]
        values = r.kv[rows(kb), 128:256]
        mask = allowed(kb)
        for g in range(2):
            heads = pl.ds(3 * g, 3)
            q = r.qz[heads].reshape(3 * TB, 128)
            e = jnp.exp(contract(q, keys, 1, 1) * score_scale).reshape(3, TB, TB)
            e = jnp.where(mask[None], e, 0.0)
            r.den[heads] += jnp.broadcast_to(jnp.sum(e, axis=2, keepdims=True), (3, TB, 128))
            e = e.reshape(3 * TB, TB).astype(BF16)
            r.oz[heads] += jnp.dot(e, values, preferred_element_type=F32).reshape(3, TB, 128)
        return carry

    lax.fori_loop(first_block, b + 1, attend, 0)
    for pair in range(3):
        heads = []
        for h in (2 * pair, 2 * pair + 1):
            o = jnp.where(half_mask(h // 3), r.oz[h] / r.den[h], 0.0)
            r.oz[h] = o
            heads.append(o)
        chunk = chunk_from_heads(heads[0], heads[1], pair).astype(BF16)
        r.o_full[:, pl.ds(pl.multiple_of(TC * t + 128 * pair, 128), 128)] = chunk

    def to_plane(sems, copies_of, three, pend=pend):
        send, recv = sems
        for k in (3, 1, 2):
            src, dst = copies_of(k)
            pend.begin(remote(src, dst, send.at[0], recv.at[0], me.plane(k)))
        all_three = remote(three, three, send.at[0], recv.at[0], me.plane(1))
        pend.later(all_three)
        return all_three.wait_recv

    def plane_gather(sems, buffer, pend=pend):
        own = buffer.at[:, cols(t)]
        return to_plane(sems, lambda k: (own, own), buffer.at[:, 0 : 3 * TC], pend)

    wait_o = plane_gather(r.pl.o, r.o_full)

    @pl.when(me.middle())
    def _():
        send_weights(0, (6, 3), True)

    @pl.when(end_chip)
    def _():
        g_wcol.arrive(1)
        g_wcol.share(1)
        g_wcol.arrive(2)
        g_wcol.share(2)
        g_dmoe.arrive(0)
        g_dmoe.spread(0, False)
        send_weights(0, (3, 5), False)

    g_wcol.finish()
    wait_o()

    column = jnp.dot(r.o_full[...], w_column[...], preferred_element_type=F32)
    r.dx[:, cols(t)] = column.astype(BF16)
    wait_column = plane_gather(r.pl.hc, r.dx, early)
    wait_column()

    def normalize_two(chunk):
        v = r.x[chunk, :].astype(F32) + residual_scale * r.dx[chunk, :].astype(F32)
        r.hidden[chunk, :] = v
        factor = lax.rsqrt(jnp.mean(v * v, axis=1, keepdims=True) + norm_eps)
        r.r_two[chunk, :] = factor
        r.dproj[chunk, :] = (v * factor * r.gains[1:2, :]).astype(BF16)

    row_chunks(normalize_two)
    r.hn[rows(b), :] = r.dproj[...]
    g_hn.start()
    logits = contract(r.router_t[...], r.dproj[...], 1, 1)
    chosen_expert = lax.broadcasted_iota(jnp.int32, (E, TB), 0)
    chosen = chosen_expert == r.routes_t[0:1, :]
    for k in range(1, TOPK):
        chosen = chosen | (chosen_expert == r.routes_t[k : k + 1, :])
    top = jnp.max(jnp.where(chosen, logits, -1e30), axis=0, keepdims=True)
    weight = jnp.where(chosen, jnp.exp(jnp.where(chosen, logits - top, 0.0)), 0.0)
    combine = weight / jnp.sum(weight, axis=0, keepdims=True)
    r.comb[b, :, 0:TB] = combine
    g_comb.start()
    g_dmoe.arrive(1)
    g_dmoe.spread(1, False)
    g_dmoe.arrive(2)
    g_dmoe.spread(2, False)
    g_dmoe.relay(0)
    for i in range(3):
        g_hn.arrive(i)
        g_hn.spread(i)
        g_comb.arrive(i)
        g_comb.share(i)

    @pl.when(me.middle())
    def _():
        send_weights(0, (5, 4), True)
        send_weights(1, (4, 3, 5, 2, 6, 1, 7), True)

    @pl.when(end_chip)
    def _():
        send_weights(0, (4,), False)
        send_weights(1, (4, 3, 5, 2, 6, 1, 7), False)

    g_dmoe.relay(1)
    g_dmoe.relay(2)
    for i in range(3):
        g_hn.relay(i)
    for i in range(3):
        g_dmoe.cross(i)
    g_dmoe.finish()
    g_comb.finish()
    for i in range(3):
        g_hn.cross(i)
    local[4].wait()
    own_columns = []
    for i in range(3):
        where = rows(2 * me.arrival(i) + c)
        copy = pltpu.make_async_copy(
            w_column.at[where, :], r.w_out.at[where, cols(t)], loc.at[i]
        )
        copy.start()
        own_columns.append(copy)
    g_wout.share_own()
    for i in range(3):
        own_columns[i].wait()
        g_wout.spread(i)
    g_hn.finish()
    for copy in own_moe:
        copy.wait()
    seven_blocks(r.aa.wm[0]).wait_recv()

    expert = lax.broadcasted_iota(jnp.int32, (16, 128), 0)
    first_row = (lax.broadcasted_iota(jnp.int32, (8, 128), 0) == 0).astype(F32)

    def core_copy(own, i):
        part = own.part.at[rows(2 * i + (1 - c)), :]
        return remote(part, own.core.at[i], own.sems[0].at[0], own.sems[1].at[i], me.partner())

    def plane_copy(own, i, k):
        return remote(
            own.part.at[rows(2 * i + c), cols(me.peer_t(k))],
            own.plane.at[i, k - 1],
            own.sems[2].at[0],
            own.sems[3].at[i, 0],
            me.plane(k),
        )

    def half_rows(i, k):
        return pl.ds(pl.multiple_of((2 * i + c) * TB + HALF * (k - 1), HALF), HALF)

    def diagonal_copy(own, i, k):
        return remote(
            own.part.at[half_rows(i, k), cols(me.peer_t(3))],
            own.diagonal.at[i, k - 1],
            own.sems[2].at[0],
            own.sems[3].at[i, 1],
            me.plane(k),
        )

    def plane_relay(own, i):
        both = own.diagonal.at[i]
        remote(both, both, own.sems[2].at[0], own.sems[3].at[i, 1], me.plane(1)).wait_recv()
        for k in (1, 2):
            where, lanes = half_rows(i, k), cols(me.peer_t(3 - k))
            own.part[where, lanes] = (
                own.part[where, lanes].astype(F32) + own.diagonal[i, k - 1].astype(F32)
            ).astype(BF16)
        for k in (1, 2):
            plane_copy(own, i, k).start()

    def core_sum(own, i):
        core_copy(own, i).wait_recv()

        def add(chunk):
            where = pl.ds(pl.multiple_of((2 * i + c) * TB + chunk.start, 64), 64)
            own.part[where, :] = (
                own.part[where, :].astype(F32) + own.core[i, chunk, :].astype(F32)
            ).astype(BF16)

        row_chunks(add)
        for k in (1, 2):
            diagonal_copy(own, i, k).start()

    def expert_block(e, where, block):
        base = 384 * e
        gate_up = jnp.dot(
            r.hn[where, :], r.w_moe[:, base : base + 256], preferred_element_type=F32
        )
        v = jnp.dot(
            r.d_moe[where, :], r.w_moe[:, base + 256 : base + 384], preferred_element_type=F32
        )
        g, u = gate_up[:, 0:128], gate_up[:, 128:256]
        chosen_one = (expert == 2 * b + e).astype(F32)
        scale = contract(r.comb[block, :, 0:TB], chosen_one, 0, 0, lax.Precision.HIGHEST)
        sig = 1.0 / (1.0 + jnp.exp(-g))
        silu = g * sig
        active = (silu * u).astype(BF16).astype(F32)
        r.cz[where, 128 * e : 128 * (e + 1)] = (scale * active).astype(BF16)
        dc = contract(first_row, active * v, 1, 1, lax.Precision.HIGHEST)
        r.dc_own[block, e : e + 1, 0:TB] = dc[0:1, :]
        dz = scale * v
        r.dgu[where, 256 * e : 256 * e + 128] = (dz * u * sig * (1.0 + g * (1.0 - sig))).astype(
            BF16
        )
        r.dgu[where, 256 * e + 128 : 256 * e + 256] = (dz * silu).astype(BF16)

    def expert_one(block, carry):
        expert_block(0, rows(block), block)
        return carry

    lax.fori_loop(0, NBLK, expert_one, 0)

    def weight_grads(e):
        def step(n, carry):
            lanes = pl.ds(pl.multiple_of(n * 256, 256), 256)
            base = 384 * e
            r.g_moe[lanes, base : base + 256] = contract(
                r.hn[:, lanes], r.dgu[:, 256 * e : 256 * (e + 1)], 0, 0
            ).astype(BF16)
            r.g_moe[lanes, base + 256 : base + 384] = contract(
                r.d_moe[:, lanes], r.cz[:, 128 * e : 128 * (e + 1)], 0, 0
            ).astype(BF16)
            return carry

        lax.fori_loop(0, DM // 256, step, 0)

    moe_targets = [list(zip((r.gate_out, r.up_out, r.down_out), lanes)) for lanes in moe_lanes]

    def send_grads(e, ks):
        send, recv = r.aa.gm[e]
        for k in ks:
            peer = me.other(k)
            for target, lanes in moe_targets[e]:
                remote(
                    r.g_moe.at[rows(peer), lanes],
                    target.at[2 * b + e],
                    send.at[0],
                    recv.at[0],
                    me.at_block(peer),
                ).start()

    weight_grads(0)
    send_grads(0, (4, 3, 5, 2, 6, 1, 7))

    def hidden_one(block, carry):
        where = rows(block)
        for n in range(3):
            lanes = slice(512 * n, 512 * (n + 1))
            r.h.part[where, lanes] = contract(
                r.dgu[where, 0:256], r.w_moe[lanes, 0:256], 1, 1
            ).astype(BF16)
        return carry

    lax.fori_loop(0, NBLK, hidden_one, 0)
    for i in range(3):
        g_wout.relay(i)
    seven_blocks(r.aa.wm[1]).wait_recv()
    early.drain()

    class Chain:
        def __init__(self, piece, line, send, recv, arrived):
            self.piece, self.line, self.send, self.recv = piece, line, send, recv
            self.arrived = arrived

        def copy(self, j):
            i = me.dest(j)
            upper = z // 2
            inner = (z * (3 - z)) // 2
            if j == 0:
                to, slot = z + 1 - 2 * upper, i
            elif j == 1:
                to, slot = z + 1 - 2 * upper, i + inner * (4 + upper - i)
            else:
                to, slot = i, 4 + z % 2
            return remote(
                self.piece(i), self.line.at[slot], self.send.at[0], self.recv.at[slot], me.at_z(to)
            )

        def wait_slot(self, slot):
            there = self.line.at[slot]
            remote(
                there, there, self.send.at[0], self.recv.at[slot], me.partner()
            ).wait_recv()

        def step(self, j):
            i = me.dest(j)
            self.arrived(i)

            @pl.when(me.middle())
            def _():
                self.wait_slot(i)
                piece = self.piece(i)
                piece[...] = (piece[...].astype(F32) + self.line[i].astype(F32)).astype(BF16)

            self.copy(j).start()

        def steps(self, when=None):
            if when is None:
                for j in range(3):
                    self.step(j)
            else:
                pl.when(when)(self.steps)

        def total(self, acc):
            self.arrived(z)
            acc[...] = self.piece(z)[...].astype(F32)
            for slot, there in ((4, z > 0), (5, z < 3)):

                @pl.when(there)
                def _(slot=slot):
                    self.wait_slot(slot)
                    acc[...] += self.line[slot].astype(F32)

        def drain(self):
            three = self.line.at[0:3]
            remote(three, three, self.send.at[0], self.recv.at[0], me.partner()).wait_send()

    def plane_add(own, i):
        both = own.plane.at[i]
        remote(both, both, own.sems[2].at[0], own.sems[3].at[i, 0], me.plane(1)).wait_recv()
        where = rows(2 * i + c)
        total = own.part[where, cols(t)].astype(F32)
        for k in range(2):
            total = total + own.plane[i, k].astype(F32)
        own.part[where, cols(t)] = total.astype(BF16)

    def scatter_chain(own):
        return Chain(
            lambda i: own.part.at[rows(2 * i + c), cols(t)],
            own.line,
            own.sems[4],
            own.sems[5],
            lambda i: plane_add(own, i),
        )

    def scatter_drain(own):
        remote(own.core, own.core, own.sems[0].at[0], own.sems[1].at[0], me.partner()).wait_send()
        twelve = own.part.at[0:576, :]
        remote(twelve, twelve, own.sems[2].at[0], own.sems[3].at[0, 0], me.plane(1)).wait_send()

    chain_h, chain_y = scatter_chain(r.h), scatter_chain(r.y)

    def expert_two(step, carry):
        i = me.dest(step // 2)
        late = step % 2
        block = 2 * i + (1 - c) + late * (2 * c - 1)
        where = rows(block)
        expert_block(1, where, block)
        for n in range(3):
            lanes = slice(512 * n, 512 * (n + 1))
            r.h.part[where, lanes] = (
                r.h.part[where, lanes].astype(F32)
                + contract(r.dgu[where, 256:512], r.w_moe[lanes, 384:640], 1, 1)
            ).astype(BF16)

        @pl.when(late == 0)
        def _():
            core_copy(r.h, i).start()

        for n in range(3):
            lanes = slice(512 * n, 512 * (n + 1))
            r.y.part[where, lanes] = (
                contract(r.cz[where, 0:128], r.w_moe[lanes, 256:384], 1, 1)
                + contract(r.cz[where, 128:256], r.w_moe[lanes, 640:768], 1, 1)
            ).astype(BF16)

        @pl.when(late == 0)
        def _():
            core_copy(r.y, i).start()

        @pl.when(late == 1)
        def _():
            core_sum(r.h, i)

        @pl.when((late == 1) & (step > 1))
        def _():
            plane_relay(r.h, me.dest(step // 2 - 1))

        for j in range(2):

            @pl.when(end_chip & (step == 2 * j + 5))
            def _(j=j):
                chain_h.step(j)

        return carry

    lax.fori_loop(0, NBLK, expert_two, 0)

    plane_relay(r.h, z)
    dc_send, dc_recv = r.aa.dc
    for k in range(1, NBLK):
        peer = me.other(k)
        pend.begin(
            remote(
                r.dc_own.at[peer], r.dc_in.at[b], dc_send.at[0], dc_recv.at[0],
                me.at_block(peer),
            )
        )
    dc_seven = r.dc_own.at[0:7]
    dc_all = remote(dc_seven, dc_seven, dc_send.at[0], dc_recv.at[0], me.partner())
    pend.later(dc_all)
    r.dc_in[b] = r.dc_own[b]


    @pl.when(me.middle())
    def _():
        chain_h.step(0)
        chain_h.step(1)

    chain_h.step(2)
    weight_grads(1)
    own_grads = [
        pltpu.make_async_copy(
            r.g_moe.at[rows(b), lanes], target.at[2 * b + e], loc.at[4 + 3 * e + i]
        )
        for e in range(2)
        for i, (target, lanes) in enumerate(moe_targets[e])
    ]
    for copy in own_grads:
        copy.start()

    dc_all.wait_recv()
    wait_dc = to_plane(r.pl.dc, lambda k: (r.dc_in, r.dc_plane.at[k - 1]), r.dc_plane)

    @pl.when(me.middle())
    def _():
        send_grads(1, (1, 7, 2))

    @pl.when(end_chip)
    def _():
        send_grads(1, (4, 3, 5, 2, 6, 1, 7))

    chain_h.total(r.acc.at[:, 0:TC])
    r.dhn[:, cols(t)] = r.acc[:, 0:TC].astype(BF16)

    @pl.when(me.middle())
    def _():
        send_grads(1, (6, 3, 5, 4))

    wait_dh = plane_gather(r.pl.dh, r.dhn)
    for j in range(4):
        core_sum(r.y, me.dest(j))
    wait_dc()
    for k in range(NBLK):
        total = r.dc_in[k] + r.dc_plane[0, k] + r.dc_plane[1, k] + r.dc_plane[2, k]
        r.dc_t[2 * k : 2 * k + 2, :] = total[0:2, :]
    dc = r.dc_t[:, 0:TB]
    combine = r.comb[b, :, 0:TB]
    d_logits = combine * (dc - jnp.sum(combine * dc, axis=0, keepdims=True))
    d_logits = d_logits.astype(BF16)
    r.flat[0:16, :] = jnp.dot(d_logits, r.hn[rows(b), :], preferred_element_type=F32)

    wait_dh()

    r.dh[...] = r.dhn[...].astype(F32) + contract(d_logits, r.router_t[...], 0, 0)
    r.flat[16:24, :] = jnp.zeros((8, DM), F32)

    def norm_two_back(chunk):
        dhn = r.dh[chunk, :]
        unit = r.hidden[chunk, :] * r.r_two[chunk, :]
        r.flat[16:17, :] += jnp.sum(dhn * unit, axis=0, keepdims=True)
        du = dhn * r.gains[1:2, :]
        mean = jnp.mean(du * unit, axis=1, keepdims=True)
        dh = r.gout[chunk, :] + r.r_two[chunk, :] * (du - unit * mean)
        r.dh[chunk, :] = dh
        r.dproj[chunk, :] = (residual_scale * dh).astype(BF16)

    row_chunks(norm_two_back)

    def to_owners(store, sems, width):
        send, recv = sems
        for k in range(NBLK):
            store.own[k, :, 0:TB] = r.flat[0:width, TB * k : TB * (k + 1)]
        store.inn[b] = store.own[b]
        for k in range(1, NBLK):
            peer = me.other(k)
            pend.begin(
                remote(
                    store.own.at[peer], store.inn.at[b], send.at[0], recv.at[0],
                    me.at_block(peer),
                )
            )
        seven = store.own.at[0:7]
        all_seven = remote(seven, seven, send.at[0], recv.at[0], me.partner())
        pend.later(all_seven)

        def wait():
            all_seven.wait_recv()
            total = store.inn[0]
            for k in range(1, NBLK):
                total = total + store.inn[k]
            return total

        return wait

    wait_sm = to_owners(r.sm, r.aa.sm, 24)

    for i in range(3):
        g_wout.cross(i)
    g_wout.finish()
    d_o = contract(r.dproj[...], r.w_out[cols(t), :], 1, 1).astype(BF16).astype(F32)
    for h in range(NQ):
        pair = h // 2
        dh_z = head_from_chunk(d_o[:, 128 * pair : 128 * (pair + 1)], h)
        den = r.den[h]
        r.dnz[h] = (dh_z / den).astype(BF16)
        r.den[h] = (
            jnp.broadcast_to(jnp.sum(dh_z * r.oz[h], axis=1, keepdims=True), (TB, 128)) / den
        )
        r.oz[h] = jnp.zeros((TB, 128), F32)

    def out_grads(n, carry):
        lanes = pl.ds(pl.multiple_of(n * 256, 256), 256)
        g_out_part[lanes, :] = contract(
            r.o_full[:, lanes], r.dproj[:, cols(t)], 0, 0
        ).astype(BF16)
        return carry

    lax.fori_loop(0, DM // 256, out_grads, 0)

    class Reduce(Chain):
        def __init__(self, part, own):
            self.part, self.core, self.sems = part, own.core, own.sems
            super().__init__(
                lambda i: part.at[rows(2 * i + c), :], own.line, own.sems[2], own.sems[3], self.chip
            )

        def core_copy(self, i):
            return remote(
                self.part.at[rows(2 * i + (1 - c)), :],
                self.core.at[i],
                self.sems[0].at[0],
                self.sems[1].at[i],
                me.partner(),
            )

        def start(self):
            for j in range(4):
                self.core_copy(me.dest(j)).start()

        def chip(self, i):
            self.core_copy(i).wait_recv()
            piece = self.piece(i)
            piece[...] = (piece[...].astype(F32) + self.core[i].astype(F32)).astype(BF16)

        def drain(self):
            super().drain()
            self.drain_core()

        def drain_core(self):
            remote(
                self.core, self.core, self.sems[0].at[0], self.sems[1].at[0], me.partner()
            ).wait_send()

        def down(self):
            for i in range(4):
                self.chip(i)

            @pl.when(z == 1)
            def _():
                self.wait_slot(0)
                piece = self.piece(0)
                piece[...] = (piece[...].astype(F32) + self.line[0].astype(F32)).astype(BF16)

            for i, slot, when in (
                (0, 0, z == 2),
                (1, 5, z == 2),
                (0, 5, z == 1),
                (2, 5, z + c == 4),
            ):
                pend.start(
                    remote(
                        self.piece(i),
                        self.line.at[slot],
                        self.send.at[1 if i == 1 else 0],
                        self.recv.at[slot],
                        me.at_z(z - 1),
                    ),
                    when,
                )

        def down_total(self, acc):
            acc[...] = self.piece(z)[...].astype(F32)

            @pl.when(z < 2 + c)
            def _():
                self.wait_slot(5)
                acc[...] += self.line[5].astype(F32)

    red_out = Reduce(g_out_part, r.rd.go)
    red_out.start()
    red_out.steps(z * (3 - z) == 0)

    for j in range(4):
        plane_relay(r.y, me.dest(j))
    def clear(i, carry):
        r.dkv[rows(i), :] = jnp.zeros((TB, 256), BF16)
        return carry

    lax.fori_loop(0, NBLK, clear, 0)

    def attend_back(kb, carry):
        keys = r.kv[rows(kb), 0:128]
        values = r.kv[rows(kb), 128:256]
        mask = allowed(kb)
        dk = jnp.zeros((TB, 128), F32)
        dv = jnp.zeros((TB, 128), F32)
        for g in range(2):
            heads = pl.ds(3 * g, 3)
            q = r.qz[heads].reshape(3 * TB, 128)
            dn = r.dnz[heads].reshape(3 * TB, 128)
            e = jnp.exp(contract(q, keys, 1, 1) * score_scale).reshape(3, TB, TB)
            e = jnp.where(mask[None], e, 0.0)
            dp = contract(dn, values, 1, 1).reshape(3, TB, TB)
            ds = (e * (dp - r.den[heads][:, :, 0:1])).reshape(3 * TB, TB).astype(BF16)
            e = e.reshape(3 * TB, TB).astype(BF16)
            r.oz[heads] += jnp.dot(ds, keys, preferred_element_type=F32).reshape(3, TB, 128)
            dk = dk + contract(ds, q, 0, 0)
            dv = dv + contract(e, dn, 0, 0)
        r.dkv[rows(kb), 0:128] = (dk * score_scale).astype(BF16)
        r.dkv[rows(kb), 128:256] = dv.astype(BF16)
        return carry

    lax.fori_loop(first_block, b + 1, attend_back, 0)
    red_kv = Reduce(r.dkv, r.rd.dkv)
    red_kv.start()
    for pair in range(3):
        heads = [
            jnp.where(half_mask(h // 3), r.oz[h] * score_scale, 0.0)
            for h in (2 * pair, 2 * pair + 1)
        ]
        u = chunk_from_heads(heads[0], heads[1], pair).astype(BF16).astype(F32)
        r.dqkv[:, 128 * pair : 128 * (pair + 1)] = (
            u * cosine - swap_halves(u) * sine
        ).astype(BF16)
    red_kv.down()

    def q_grads(n, carry):
        lanes = pl.ds(pl.multiple_of(n * 256, 256), 256)
        g_q_part[lanes, :] = contract(r.xn[:, lanes], r.dqkv[:, 0:TC], 0, 0).astype(BF16)
        return carry

    lax.fori_loop(0, DM // 256, q_grads, 0)
    red_gq = Reduce(g_q_part, r.rd.gq)
    red_gq.start()
    red_gq.steps(end_chip)
    d_kv_acc = r.acc.at[:, 0:256]
    red_kv.down_total(d_kv_acc)
    d_kv = d_kv_acc[...].astype(BF16)
    u = d_kv[:, 0:128].astype(F32)
    r.dqkv[:, 384:512] = (u * cosine - swap_halves(u) * sine).astype(BF16)
    r.dqkv[:, 512:640] = d_kv[:, 128:256]

    for n in range(3):
        lanes = slice(512 * n, 512 * (n + 1))
        r.dx[:, lanes] = contract(r.dqkv[...], r.w_qkv[lanes, :], 1, 1).astype(BF16)
    wait_xs = to_plane(
        r.pl.xs, lambda k: (r.dx.at[:, cols(me.peer_t(k))], r.dx_in.at[k - 1]), r.dx_in
    )

    def kv_grads(n, carry):
        lanes = pl.ds(pl.multiple_of(n * 256, 256), 256)
        g_kv_part[lanes, :] = contract(r.xn[:, lanes], r.dqkv[:, TC:640], 0, 0).astype(BF16)
        return carry

    lax.fori_loop(0, DM // 256, kv_grads, 0)
    red_gkv = Reduce(g_kv_part, r.rd.gkv)
    red_gkv.start()
    red_gq.steps(me.middle())
    red_gkv.steps(end_chip)
    chain_y.steps(end_chip)
    wait_xs()
    total = r.dx[:, cols(t)].astype(F32)
    for k in range(3):
        total = total + r.dx_in[k].astype(F32)
    r.dxn[:, cols(t)] = total.astype(BF16)
    wait_dx = plane_gather(r.pl.xg, r.dxn)
    own_qkv, from_qkv = [], []

    def give(n, start, width, target, sems, three):
        def lanes(index):
            return pl.ds(pl.multiple_of(width * index, 128), width)

        piece = r.g_qkv_sum.at[:, start : start + width]
        there = target.at[:, lanes(t)]
        own = pltpu.make_async_copy(piece, there, loc.at[1 + n])
        own.start()
        own_qkv.append(own)
        from_qkv.append(to_plane(sems, lambda k: (piece, there), three))

    red_gkv.steps(me.middle())
    red_gq.total(r.acc.at[:, 0:TC])
    r.g_qkv_sum[:, 0:TC] = r.acc[:, 0:TC].astype(BF16)
    give(0, 0, TC, r.gq_out, r.pl.gq, r.dx_in)
    red_out.steps(me.middle())
    wait_dx()
    r.flat[0:8, :] = jnp.zeros((8, DM), F32)

    def norm_one_back(chunk):
        dxn = r.dxn[chunk, :].astype(F32)
        factor = r.r_one[chunk, :]
        unit = r.x[chunk, :].astype(F32) * factor
        r.flat[0:1, :] += jnp.sum(dxn * unit, axis=0, keepdims=True)
        du = dxn * r.gains[0:1, :]
        mean = jnp.mean(du * unit, axis=1, keepdims=True)
        r.grad_in[chunk, :] = r.dh[chunk, :] + factor * (du - unit * mean)

    row_chunks(norm_one_back)
    wait_sn = to_owners(r.sn, r.aa.sn, 8)
    red_gkv.total(r.acc.at[:, 0:256])
    r.g_qkv_sum[:, TC:640] = r.acc[:, 0:256].astype(BF16)
    give(1, 384, 128, r.gk_out, r.pl.gk, r.g_qkv_sum.at[:, 0:TC])
    give(2, 512, 128, r.gv_out, r.pl.gv, r.g_qkv_sum.at[:, 0:TC])
    red_out.total(r.acc.at[:, 0:TC])
    r.g_out_sum[...] = r.acc[:, 0:TC].astype(BF16)
    own_go = pltpu.make_async_copy(r.g_out_sum, r.g_out_out.at[:, cols(t)], loc.at[0])
    own_go.start()
    go_there = r.g_out_out.at[:, cols(t)]
    wait_go = to_plane(r.pl.go, lambda k: (r.g_out_sum, go_there), r.dx_in)
    chain_y.steps(me.middle())
    chain_y.total(r.acc.at[:, 0:TC])
    r.block_out[...] = r.hidden[:, cols(t)] + residual_scale * r.acc[:, 0:TC]
    r.sm_out[...] = wait_sm()
    r.sn_out[...] = wait_sn()

    wait_go()
    for wait in from_qkv:
        wait()
    own_go.wait()
    for copy in own_qkv:
        copy.wait()
    for copy in own_grads:
        copy.wait()
    for e in range(2):
        seven_blocks(r.aa.gm[e]).wait()
        seven_blocks(r.aa.wm[e]).wait_send()
    scatter_drain(r.h)
    scatter_drain(r.y)
    chain_h.drain()
    chain_y.drain()
    red_out.drain()
    red_kv.drain_core()
    red_gq.drain()
    red_gkv.drain()
    pend.drain()


def fast_body(
    block_input,
    segments,
    routes,
    attn_gain,
    ffn_gain,
    query_weight,
    key_matrix,
    value_matrix,
    out_weight,
    router_weight,
    gate_weight,
    up_weight,
    down_weight,
    grad_output,
):
    half = HEAD_DIM // 2
    inverse = rope_base ** (-(np.arange(half, dtype=np.float64) * 2.0 / HEAD_DIM))
    inverse = np.tile(inverse.astype(np.float32).astype(np.float64), 4)

    def table(positions):
        angles = positions[:, None] * inverse[None, :]
        return np.stack([np.cos(angles), np.sin(angles)]).astype(np.float32)

    vectors = (
        jnp.pad(segments, (0, 512)).astype(F32)
        + jnp.pad(attn_gain.astype(F32), (DM, 320))
        + jnp.pad(ffn_gain.astype(F32), (DM + 256, 64))
    ).reshape(16, 128)
    vmem, hbm = pl.BlockSpec(memory_space=pltpu.VMEM), pl.BlockSpec(memory_space=pl.ANY)
    ins = dict(
        x=(block_input, vmem),
        gout=(grad_output, vmem),
        rope_block=(jnp.asarray(table(np.arange(NBLK) * TB)), vmem),
        rope_row=(jnp.asarray(table(np.arange(TB))), vmem),
        vectors=(vectors, vmem),
        routes_t=(routes.T, vmem),
        router_own=(router_weight.T, vmem),
        wq=(query_weight, hbm),
        wk=(key_matrix, hbm),
        wv=(value_matrix, hbm),
        wo=(out_weight, hbm),
        gate=(gate_weight, hbm),
        up=(up_weight, hbm),
        down_t=(down_weight.transpose(0, 2, 1), hbm),
    )
    outs = dict(
        block_out=((TB, TC), F32, vmem),
        grad_in=((TB, DM), F32, vmem),
        sm_out=((24, 256), F32, vmem),
        sn_out=((8, 256), F32, vmem),
        gq_out=((TB, DM), BF16, hbm),
        gk_out=((TB, 512), BF16, hbm),
        gv_out=((TB, 512), BF16, hbm),
        g_out_out=((TB, DM), BF16, hbm),
        gate_out=((E, TB, 128), BF16, hbm),
        up_out=((E, TB, 128), BF16, hbm),
        down_out=((E, TB, 128), BF16, hbm),
    )
    leaves, tree = jax.tree.flatten(scratch_tree())

    def entry(*refs):
        table = bags(jax.tree.unflatten(tree, refs[len(ins) + len(outs) :]))
        table.update(zip((*ins, *outs), refs))
        kernel(table)

    results = pl.pallas_call(
        entry,
        name="layer",
        out_shape=[jax.ShapeDtypeStruct(shape, kind) for shape, kind, _ in outs.values()],
        in_specs=[spec for _, spec in ins.values()],
        out_specs=[spec for _, _, spec in outs.values()],
        scratch_shapes=leaves,
        compiler_params=pltpu.CompilerParams(
            collective_id=0, has_side_effects=True, vmem_limit_bytes=VMEM_BYTES
        ),
    )(*[value for value, _ in ins.values()])
    res = Bag(zip(outs, results))
    wide = widen(
        res.block_out, res.grad_in, res.gq_out, res.gk_out, res.gv_out, res.g_out_out,
        res.gate_out, res.up_out, res.down_out, res.sm_out, res.sn_out,
    )
    block_output, grad_input, g_query, g_key, g_value, g_out, gate, up, down = wide[:9]
    router, gain_two, gain_one = wide[9:]
    return (
        block_output,
        grad_input,
        gain_one.reshape(TB),
        gain_two.reshape(TB),
        g_query,
        g_key,
        g_value,
        g_out,
        router.T,
        gate,
        up,
        down.transpose(0, 2, 1),
    )


def widen(*arrays):
    steps = 2

    def spec(array):
        rest = (0,) * (array.ndim - 1)
        return pl.BlockSpec((array.shape[0] // steps, *array.shape[1:]), lambda i: (i, *rest))

    def entry(*refs):
        count = len(arrays)
        for source, target in zip(refs[: count - 2], refs[count:]):
            target[...] = source[...].astype(F32)
        sm, sn = refs[count - 2 : count]
        router, gain_two, gain_one = refs[-3:]
        router[...] = sm[0:16, 0:TB]
        gain_two[...] = sm[16:17, 0:TB]
        gain_one[...] = sn[0:1, 0:TB]

    def whole(*shape):
        return pl.BlockSpec(shape, lambda i: (0, 0))

    specs = [spec(a) for a in arrays[:-2]]
    return pl.pallas_call(
        entry,
        name="widen",
        grid=(steps,),
        in_specs=[*specs, whole(24, 256), whole(8, 256)],
        out_specs=[*specs, whole(16, TB), whole(1, TB), whole(1, TB)],
        out_shape=[
            *(jax.ShapeDtypeStruct(a.shape, F32) for a in arrays[:-2]),
            jax.ShapeDtypeStruct((16, TB), F32),
            jax.ShapeDtypeStruct((1, TB), F32),
            jax.ShapeDtypeStruct((1, TB), F32),
        ],
        cost_estimate=pl.CostEstimate(flops=4_000_000, bytes_accessed=16_000_000, transcendentals=0),
    )(*arrays)


VMEM_BYTES = 67043328


def fits(mesh):
    return (mesh.shape["fsdp"], mesh.shape["heads"], mesh.shape["tensor"]) == (4, 2, 4)


def solution(mesh):
    in_specs = (
        P(("fsdp", "heads"), None),
        P(),
        P(("fsdp", "heads"), None),
        P(("fsdp", "heads")),
        P(("fsdp", "heads")),
        P(("fsdp", "heads"), None),
        P(("fsdp", "heads"), None),
        P(("fsdp", "heads"), None),
        P(("fsdp", "heads"), None),
        P(("fsdp", "heads"), None),
        P(None, ("fsdp", "heads"), "tensor"),
        P(None, ("fsdp", "heads"), "tensor"),
        P(None, "tensor", ("fsdp", "heads")),
        P(("fsdp", "heads"), None),
    )
    out_specs = (
        P(("fsdp", "heads"), "tensor"),
        P(("fsdp", "heads"), None),
        P(("fsdp", "heads")),
        P(("fsdp", "heads")),
        P(("fsdp", "heads"), None),
        P(("fsdp", "heads"), None),
        P(("fsdp", "heads"), None),
        P(("fsdp", "heads"), None),
        P(("fsdp", "heads"), None),
        P(None, ("fsdp", "heads"), "tensor"),
        P(None, ("fsdp", "heads"), "tensor"),
        P(None, "tensor", ("fsdp", "heads")),
    )
    chosen = fast_body if fits(mesh) else body
    return jax.shard_map(chosen, mesh=mesh, in_specs=in_specs, out_specs=out_specs, check_vma=False)
```

```python
import math

import jax
import jax.numpy as jnp
import numpy as np
from jax import lax
from jax.experimental import pallas as pl
from jax.experimental.pallas import tpu as pltpu
from jax.sharding import PartitionSpec as P

QUERY_HEADS = 24
KEY_VALUE_HEADS = 8
HEAD_DIM = 64
E = 16


norm_eps = 1e-06
score_scale = 0.015625
residual_scale = 0.22
rope_base = 10000.0


def rotary_table(token_positions, head_size):
    half_size = head_size // 2
    inverse = rope_base ** (-(jnp.arange(half_size, dtype=jnp.float32) * 2.0 / head_size))
    angles = token_positions[:, None].astype(jnp.float32) * inverse[None, :]
    return (jnp.cos(angles)[:, None, :], jnp.sin(angles)[:, None, :])


def apply_rotary(vectors, cosine_lookup, sine_lookup):
    half_size = vectors.shape[-1] // 2
    first_half = vectors[..., :half_size]
    second_half = vectors[..., half_size:]
    return jnp.concatenate(
        [
            first_half * cosine_lookup - second_half * sine_lookup,
            second_half * cosine_lookup + first_half * sine_lookup,
        ],
        axis=-1,
    )


def reverse_rotary(gradient, cosine_lookup, sine_lookup):
    half_size = gradient.shape[-1] // 2
    first_half = gradient[..., :half_size]
    second_half = gradient[..., half_size:]
    return jnp.concatenate(
        [
            first_half * cosine_lookup + second_half * sine_lookup,
            second_half * cosine_lookup - first_half * sine_lookup,
        ],
        axis=-1,
    )


def body(
    block_input,
    segments,
    routes,
    attn_gain,
    ffn_gain,
    query_weight,
    key_matrix,
    value_matrix,
    out_weight,
    router_weight,
    gate_weight,
    up_weight,
    down_weight,
    grad_output,
):
    head_count = lax.axis_size("heads")
    n_tensor = lax.axis_size("tensor")
    n_fsdp = lax.axis_size("fsdp")
    fsdp_index = lax.axis_index("fsdp")
    heads_index = lax.axis_index("heads")
    tensor_index = lax.axis_index("tensor")
    token_rows = block_input.shape[0]
    model_width = block_input.shape[1]
    query_rows = token_rows * head_count
    seq_rows = query_rows * n_fsdp
    key_value_local = KEY_VALUE_HEADS // head_count
    heads_per_group = QUERY_HEADS // KEY_VALUE_HEADS
    slice_width = model_width // n_tensor
    gathered = (
        lax.all_gather(attn_gain, ("fsdp", "heads"), axis=0, tiled=True),
        lax.all_gather(ffn_gain, ("fsdp", "heads"), axis=0, tiled=True),
        lax.all_gather(query_weight, ("fsdp", "heads"), axis=0, tiled=True),
        lax.all_gather(key_matrix, ("fsdp", "heads"), axis=0, tiled=True),
        lax.all_gather(value_matrix, ("fsdp", "heads"), axis=0, tiled=True),
        lax.all_gather(out_weight, ("fsdp", "heads"), axis=0, tiled=True),
        lax.all_gather(router_weight, ("fsdp", "heads"), axis=0, tiled=True),
        lax.all_gather(gate_weight, ("fsdp", "heads"), axis=1, tiled=True),
        lax.all_gather(up_weight, ("fsdp", "heads"), axis=1, tiled=True),
        lax.all_gather(down_weight, ("fsdp", "heads"), axis=2, tiled=True),
    )
    gain_attn = gathered[0].astype(jnp.float32)
    gain_ffn = gathered[1].astype(jnp.float32)
    full_query, full_key, full_value, full_out, full_router, full_gate, full_up, full_down = (
        gathered[2:]
    )
    inputs = block_input.astype(jnp.float32)
    scale_one = lax.rsqrt(jnp.mean(inputs * inputs, axis=-1, keepdims=True) + norm_eps)
    unit_one = inputs * scale_one
    normalized_input = (unit_one * gain_attn).astype(jnp.bfloat16)
    query_lin = jnp.dot(normalized_input, full_query, preferred_element_type=jnp.float32)
    key_linear = jnp.dot(normalized_input, full_key, preferred_element_type=jnp.float32)
    value_lin = jnp.dot(normalized_input, full_value, preferred_element_type=jnp.float32)
    own_start = (fsdp_index * head_count + heads_index) * token_rows
    token_positions = own_start + jnp.arange(token_rows, dtype=jnp.int32)
    cosine_lookup, sine_lookup = rotary_table(token_positions, HEAD_DIM)
    query_send = (
        apply_rotary(
            query_lin.reshape(token_rows, QUERY_HEADS, HEAD_DIM), cosine_lookup, sine_lookup
        )
        .reshape(token_rows, QUERY_HEADS * HEAD_DIM)
        .astype(jnp.bfloat16)
    )
    key_send = (
        apply_rotary(
            key_linear.reshape(token_rows, KEY_VALUE_HEADS, HEAD_DIM), cosine_lookup, sine_lookup
        )
        .reshape(token_rows, KEY_VALUE_HEADS * HEAD_DIM)
        .astype(jnp.bfloat16)
    )
    value_send = value_lin.astype(jnp.bfloat16)
    query_heads, key_local, value_local = (
        lax.all_to_all(query_send, "heads", split_axis=1, concat_axis=0, tiled=True),
        lax.all_to_all(key_send, "heads", split_axis=1, concat_axis=0, tiled=True),
        lax.all_to_all(value_send, "heads", split_axis=1, concat_axis=0, tiled=True),
    )
    query_vectors = query_heads.reshape(query_rows, key_value_local, heads_per_group, HEAD_DIM)
    query_start = fsdp_index * query_rows
    query_pos = query_start + jnp.arange(query_rows, dtype=jnp.int32)
    query_seg = lax.dynamic_slice_in_dim(segments, query_start, query_rows, 0)

    def masked_exp(key_block, key_start):
        block_rows = key_block.shape[0]
        raw_scores = (
            jnp.einsum(
                "qkgd,jkd->kgqj", query_vectors, key_block, preferred_element_type=jnp.float32
            )
            * score_scale
        )
        key_pos = key_start + jnp.arange(block_rows, dtype=jnp.int32)
        key_seg = lax.dynamic_slice_in_dim(segments, key_start, block_rows, 0)
        allowed = (query_pos[:, None] >= key_pos[None, :]) & (
            query_seg[:, None] == key_seg[None, :]
        )
        return jnp.where(allowed[None, None], jnp.exp(raw_scores), 0.0)

    def split_blocks(key_piece):
        keys_piece, values_piece = key_piece
        piece_rows = keys_piece.shape[0]
        block_rows = math.gcd(piece_rows, query_rows)
        block_count = piece_rows // block_rows
        starts = jnp.arange(block_count, dtype=jnp.int32) * block_rows
        return (
            keys_piece.reshape(block_count, block_rows, key_value_local, HEAD_DIM),
            values_piece.reshape(block_count, block_rows, key_value_local, HEAD_DIM),
            starts,
        )

    start_state = (
        jnp.zeros((key_value_local, heads_per_group, query_rows), jnp.float32),
        jnp.zeros((key_value_local, heads_per_group, query_rows, HEAD_DIM), jnp.float32),
    )
    fold_state = start_state

    def block_step(running, block_item):
        denominator, numerator = running
        key_block, value_block, key_start = block_item
        weights = masked_exp(key_block, key_start)
        denominator = denominator + jnp.sum(weights, axis=-1)
        numerator = numerator + jnp.einsum(
            "kgqj,jkd->kgqd",
            weights.astype(jnp.bfloat16),
            value_block,
            preferred_element_type=jnp.float32,
        )
        return ((denominator, numerator), None)

    fold_state, _ = lax.scan(
        block_step,
        fold_state,
        split_blocks(
            (
                lax.all_gather(key_local, "fsdp", axis=0, tiled=True),
                lax.all_gather(value_local, "fsdp", axis=0, tiled=True),
            )
        ),
    )
    denominator, numerator = fold_state
    attn_full = numerator / denominator[..., None]
    attn_send = (
        attn_full.transpose(2, 0, 1, 3)
        .reshape(query_rows, key_value_local * heads_per_group * HEAD_DIM)
        .astype(jnp.bfloat16)
    )
    attn_back = lax.all_to_all(attn_send, "heads", split_axis=0, concat_axis=1, tiled=True)
    attn_proj = jnp.dot(attn_back, full_out, preferred_element_type=jnp.float32)
    hidden = inputs + residual_scale * attn_proj
    scale_two = lax.rsqrt(jnp.mean(hidden * hidden, axis=-1, keepdims=True) + norm_eps)
    unit_two = hidden * scale_two
    normed_two = (unit_two * gain_ffn).astype(jnp.bfloat16)
    logits = jnp.dot(normed_two, full_router, preferred_element_type=jnp.float32)
    onehot = (routes[:, :, None] == jnp.arange(E, dtype=jnp.int32)[None, None, :]).astype(
        jnp.float32
    )
    picked = jnp.sum(onehot * logits[:, None, :], axis=-1)
    route_probs = jax.nn.softmax(picked, axis=-1)
    combine = jnp.sum(onehot * route_probs[:, :, None], axis=1)
    gate_pre = jnp.einsum("td,edf->etf", normed_two, full_gate, preferred_element_type=jnp.float32)
    up_pre = jnp.einsum("td,edf->etf", normed_two, full_up, preferred_element_type=jnp.float32)
    sigmoid_gate = jax.nn.sigmoid(gate_pre)
    silu_gate = gate_pre * sigmoid_gate
    active = (silu_gate * up_pre).astype(jnp.bfloat16)
    expert_out = jnp.einsum("etf,efd->etd", active, full_down, preferred_element_type=jnp.float32)
    mixed_part = jnp.sum(combine.T[:, :, None] * expert_out, axis=0)
    mixed_sum = lax.psum_scatter(
        mixed_part.astype(jnp.bfloat16), "tensor", scatter_dimension=1, tiled=True
    ).astype(jnp.float32)
    hidden_mine = lax.dynamic_slice_in_dim(hidden, tensor_index * slice_width, slice_width, 1)
    block_output = hidden_mine + residual_scale * mixed_sum
    mixed_grad = residual_scale * grad_output
    expert_grad = (combine.T[:, :, None] * mixed_grad[None]).astype(jnp.bfloat16)
    combine_part = jnp.sum(expert_out * mixed_grad[None], axis=-1).T
    active_grad = jnp.einsum(
        "etd,efd->etf", expert_grad, full_down, preferred_element_type=jnp.float32
    )
    gate_grad = (
        active_grad * up_pre * sigmoid_gate * (1.0 + gate_pre * (1.0 - sigmoid_gate))
    ).astype(jnp.bfloat16)
    up_grad = (active_grad * silu_gate).astype(jnp.bfloat16)
    normed_part = jnp.einsum(
        "etf,edf->td", gate_grad, full_gate, preferred_element_type=jnp.float32
    ) + jnp.einsum("etf,edf->td", up_grad, full_up, preferred_element_type=jnp.float32)
    gate_full = jnp.einsum("td,etf->edf", normed_two, gate_grad, preferred_element_type=jnp.float32)
    up_full = jnp.einsum("td,etf->edf", normed_two, up_grad, preferred_element_type=jnp.float32)
    down_full = jnp.einsum("etf,etd->efd", active, expert_grad, preferred_element_type=jnp.float32)
    grad_gate, grad_up, grad_down = (
        lax.psum_scatter(gate_full.astype(jnp.bfloat16), ("fsdp", "heads"), scatter_dimension=1, tiled=True),
        lax.psum_scatter(up_full.astype(jnp.bfloat16), ("fsdp", "heads"), scatter_dimension=1, tiled=True),
        lax.psum_scatter(down_full.astype(jnp.bfloat16), ("fsdp", "heads"), scatter_dimension=2, tiled=True),
    )
    normed_grad, combine_grad = lax.psum((normed_part, combine_part), "tensor")
    pick_grad = jnp.sum(onehot * combine_grad[:, None, :], axis=-1)
    picked_grad = route_probs * (
        pick_grad - jnp.sum(route_probs * pick_grad, axis=-1, keepdims=True)
    )
    logit_grad = jnp.sum(onehot * picked_grad[:, :, None], axis=1).astype(jnp.bfloat16)
    router_full = jnp.dot(normed_two.T, logit_grad, preferred_element_type=jnp.float32)
    normed_grad = normed_grad + jnp.dot(
        logit_grad, full_router.T, preferred_element_type=jnp.float32
    )
    gain_ffn_full = jnp.sum(normed_grad * unit_two, axis=0)
    unit_grad = normed_grad * gain_ffn
    hidden_grad = grad_output + scale_two * (
        unit_grad - unit_two * jnp.mean(unit_grad * unit_two, axis=-1, keepdims=True)
    )
    proj_grad = (residual_scale * hidden_grad).astype(jnp.bfloat16)
    out_full = jnp.dot(attn_back.T, proj_grad, preferred_element_type=jnp.float32)
    attn_grad = jnp.dot(proj_grad, full_out.T, preferred_element_type=jnp.float32).astype(
        jnp.bfloat16
    )
    grad_heads = lax.all_to_all(attn_grad, "heads", split_axis=1, concat_axis=0, tiled=True)
    grad_float = (
        grad_heads.reshape(query_rows, key_value_local, heads_per_group, HEAD_DIM)
        .transpose(1, 2, 0, 3)
        .astype(jnp.float32)
    )
    scaled_grad = (grad_float / denominator[..., None]).astype(jnp.bfloat16)
    shift_term = jnp.sum(grad_float * attn_full, axis=-1) / denominator
    start_back = (
        jnp.zeros((key_value_local, heads_per_group, query_rows, HEAD_DIM), jnp.float32),
        jnp.zeros((seq_rows, key_value_local * HEAD_DIM), jnp.float32),
        jnp.zeros((seq_rows, key_value_local * HEAD_DIM), jnp.float32),
    )
    fold_state = start_back

    def block_step(running, block_item):
        query_acc, key_acc, value_acc = running
        key_block, value_block, key_start = block_item
        block_rows = key_block.shape[0]
        weights = masked_exp(key_block, key_start)
        dot_grad = jnp.einsum(
            "kgqd,jkd->kgqj", scaled_grad, value_block, preferred_element_type=jnp.float32
        )
        score_grad = (weights * (dot_grad - shift_term[..., None])).astype(jnp.bfloat16)
        query_acc = (
            query_acc
            + jnp.einsum(
                "kgqj,jkd->kgqd", score_grad, key_block, preferred_element_type=jnp.float32
            )
            * score_scale
        )
        key_part = (
            jnp.einsum(
                "kgqj,qkgd->jkd", score_grad, query_vectors, preferred_element_type=jnp.float32
            )
            * score_scale
        )
        value_part = jnp.einsum(
            "kgqj,kgqd->jkd",
            weights.astype(jnp.bfloat16),
            scaled_grad,
            preferred_element_type=jnp.float32,
        )
        key_old = lax.dynamic_slice_in_dim(key_acc, key_start, block_rows, 0)
        value_old = lax.dynamic_slice_in_dim(value_acc, key_start, block_rows, 0)
        key_acc = lax.dynamic_update_slice_in_dim(
            key_acc,
            key_old + key_part.reshape(block_rows, key_value_local * HEAD_DIM),
            key_start,
            0,
        )
        value_acc = lax.dynamic_update_slice_in_dim(
            value_acc,
            value_old + value_part.reshape(block_rows, key_value_local * HEAD_DIM),
            key_start,
            0,
        )
        return ((query_acc, key_acc, value_acc), None)

    fold_state, _ = lax.scan(
        block_step,
        fold_state,
        split_blocks(
            (
                lax.all_gather(key_local, "fsdp", axis=0, tiled=True),
                lax.all_gather(value_local, "fsdp", axis=0, tiled=True),
            )
        ),
    )
    query_acc, key_acc, value_acc = fold_state
    key_mine, value_mine = (
        lax.psum_scatter(key_acc, "fsdp", scatter_dimension=0, tiled=True),
        lax.psum_scatter(value_acc, "fsdp", scatter_dimension=0, tiled=True),
    )
    query_send_back = (
        query_acc.transpose(2, 0, 1, 3)
        .reshape(query_rows, key_value_local * heads_per_group * HEAD_DIM)
        .astype(jnp.bfloat16)
    )
    query_ret, key_returned, value_ret = (
        lax.all_to_all(query_send_back, "heads", split_axis=0, concat_axis=1, tiled=True),
        lax.all_to_all(
            key_mine.astype(jnp.bfloat16), "heads", split_axis=0, concat_axis=1, tiled=True
        ),
        lax.all_to_all(
            value_mine.astype(jnp.bfloat16), "heads", split_axis=0, concat_axis=1, tiled=True
        ),
    )
    query_lin_grad = (
        reverse_rotary(
            query_ret.astype(jnp.float32).reshape(token_rows, QUERY_HEADS, HEAD_DIM),
            cosine_lookup,
            sine_lookup,
        )
        .reshape(token_rows, QUERY_HEADS * HEAD_DIM)
        .astype(jnp.bfloat16)
    )
    key_lin_grad = (
        reverse_rotary(
            key_returned.astype(jnp.float32).reshape(token_rows, KEY_VALUE_HEADS, HEAD_DIM),
            cosine_lookup,
            sine_lookup,
        )
        .reshape(token_rows, KEY_VALUE_HEADS * HEAD_DIM)
        .astype(jnp.bfloat16)
    )
    query_full = jnp.dot(normalized_input.T, query_lin_grad, preferred_element_type=jnp.float32)
    key_full = jnp.dot(normalized_input.T, key_lin_grad, preferred_element_type=jnp.float32)
    value_full = jnp.dot(normalized_input.T, value_ret, preferred_element_type=jnp.float32)
    normed_one_grad = jnp.dot(query_lin_grad, full_query.T, preferred_element_type=jnp.float32)
    normed_one_grad = normed_one_grad + jnp.dot(
        key_lin_grad, full_key.T, preferred_element_type=jnp.float32
    )
    normed_one_grad = normed_one_grad + jnp.dot(
        value_ret, full_value.T, preferred_element_type=jnp.float32
    )
    gain_attn_full = jnp.sum(normed_one_grad * unit_one, axis=0)
    unit_one_grad = normed_one_grad * gain_attn
    grad_input = hidden_grad + scale_one * (
        unit_one_grad - unit_one * jnp.mean(unit_one_grad * unit_one, axis=-1, keepdims=True)
    )
    grad_attn_gain, grad_ffn_gain, grad_query, grad_key, grad_value, grad_out_proj, grad_router = (
        lax.psum_scatter(gain_attn_full, ("fsdp", "heads"), scatter_dimension=0, tiled=True),
        lax.psum_scatter(gain_ffn_full, ("fsdp", "heads"), scatter_dimension=0, tiled=True),
        lax.psum_scatter(query_full.astype(jnp.bfloat16), ("fsdp", "heads"), scatter_dimension=0, tiled=True),
        lax.psum_scatter(key_full.astype(jnp.bfloat16), ("fsdp", "heads"), scatter_dimension=0, tiled=True),
        lax.psum_scatter(value_full.astype(jnp.bfloat16), ("fsdp", "heads"), scatter_dimension=0, tiled=True),
        lax.psum_scatter(out_full.astype(jnp.bfloat16), ("fsdp", "heads"), scatter_dimension=0, tiled=True),
        lax.psum_scatter(router_full, ("fsdp", "heads"), scatter_dimension=0, tiled=True),
    )
    grad_query, grad_key, grad_value, grad_out_proj, grad_gate, grad_up, grad_down = (
        g.astype(jnp.float32)
        for g in (grad_query, grad_key, grad_value, grad_out_proj, grad_gate, grad_up, grad_down)
    )
    return (
        block_output,
        grad_input,
        grad_attn_gain,
        grad_ffn_gain,
        grad_query,
        grad_key,
        grad_value,
        grad_out_proj,
        grad_router,
        grad_gate,
        grad_up,
        grad_down,
    )


MESH_ID = pl.DeviceIdType.MESH
F32 = jnp.float32
BF16 = jnp.bfloat16

TB = 192
DM = 1536
TC = 384
HALF = 96
NBLK = 8
NQ = 6
TOPK = 8
FIRST_DOC_BLOCKS = 5


def contract(left, right, left_dim, right_dim, precision=None):
    return lax.dot_general(
        left,
        right,
        (((left_dim,), (right_dim,)), ((), ())),
        preferred_element_type=F32,
        precision=precision,
    )


def rows(index):
    return pl.ds(pl.multiple_of(index * TB, TB), TB)


def cols(index):
    return pl.ds(pl.multiple_of(index * TC, 128), TC)


class Place:
    def __init__(self):
        self.z = lax.axis_index("fsdp")
        self.c = lax.axis_index("heads")
        self.t = lax.axis_index("tensor")
        self.b = 2 * self.z + self.c

    def partner(self):
        return (self.z, 1 - self.c, self.t)

    def at_z(self, z):
        return (z, self.c, self.t)

    def at_block(self, block):
        return (block // 2, block % 2, self.t)

    def peer_t(self, k):
        if k == 1:
            return self.t + 1 - 2 * (self.t % 2)
        if k == 2:
            return (self.t + 2) % 4
        return 3 - self.t

    def plane(self, k):
        return (self.z, self.c, self.peer_t(k))

    def other(self, k):
        return (self.b + k) % NBLK

    def arrival(self, i):
        if i == 0:
            return self.z + 1 - 2 * (self.z % 2)
        if i == 1:
            return 2 - self.z // 2
        return 3 - 3 * (self.z // 2)

    def forward_to(self, i):
        return 3 - self.z if i == 0 else 3 * (self.z - 1)

    def middle(self):
        return self.z * (3 - self.z) > 0

    def dest(self, j):
        inner = (self.z * (3 - self.z)) // 2
        turned = j + inner * (j // 2) * (1 - 2 * (j % 2))
        upper = self.z // 2
        return 3 * (1 - upper) + (2 * upper - 1) * turned


def remote(src, dst, send_sem, recv_sem, device):
    return pltpu.make_async_remote_copy(
        src_ref=src,
        dst_ref=dst,
        send_sem=send_sem,
        recv_sem=recv_sem,
        device_id=device,
        device_id_type=MESH_ID,
    )


class Pending:
    def __init__(self):
        self.items = []

    def start(self, copy, when=None):
        self.begin(copy, when)
        self.later(copy, when)

    def begin(self, copy, when=None):
        if when is None:
            copy.start()
        else:

            @pl.when(when)
            def _():
                copy.start()

    def later(self, copy, when=None):
        self.items.append((copy, when))

    def drain(self):
        for copy, when in self.items:
            if when is None:
                copy.wait_send()
            else:

                @pl.when(when)
                def _(copy=copy):
                    copy.wait_send()

        self.items = []


class LineGather:
    def __init__(self, me, pend, view, line_view, several, several_line, sems):
        self.me, self.pend, self.view, self.line_view = me, pend, view, line_view
        self.several, self.several_line = several, several_line
        self.send, self.recv, self.psend, self.precv = sems

    def bytes_of(self, ref, send_sem, recv_sem):
        return remote(ref, ref, send_sem.at[0], recv_sem.at[0], self.me.partner())

    def start(self):
        self.send_own()
        self.register()

    def register(self):
        me = self.me
        for count, when in ((5, me.middle()), (1, me.z * (3 - me.z) == 0)):
            self.pend.later(self.bytes_of(self.several_line(count), self.send, self.recv), when)
        self.register_shares()

    def send_own(self):
        me = self.me
        own = self.line_view(me.b)
        for dz, when in ((1, me.z < 3), (-1, me.z > 0)):
            self.pend.begin(
                remote(own, own, self.send.at[0], self.recv.at[me.z], me.at_z(me.z + dz)), when
            )
        self.share_block(me.b)

    def register_shares(self):
        self.pend.later(self.bytes_of(self.several(4), self.psend, self.precv))

    def share_own(self):
        self.share_block(self.me.b)
        self.register_shares()

    def share_block(self, block):
        whole = self.view(block)
        self.pend.begin(
            remote(whole, whole, self.psend.at[0], self.precv.at[0], self.me.partner())
        )

    def arrive(self, i):
        me = self.me
        source = me.arrival(i)
        block = self.line_view(2 * source + me.c)
        remote(block, block, self.send.at[0], self.recv.at[source], me.partner()).wait_recv()
        self.pend.begin(
            remote(
                block, block, self.send.at[0], self.recv.at[source], me.at_z(me.forward_to(i))
            ),
            me.middle(),
        )

    def share(self, i):
        self.share_block(2 * self.me.arrival(i) + self.me.c)

    def finish(self):
        self.bytes_of(self.several(4), self.psend, self.precv).wait_recv()


class UpGather(LineGather):
    def __init__(self, me, pend, view, sems):
        self.me, self.pend, self.view = me, pend, view
        self.send, self.recv, self.psend, self.precv = sems

    def start(self):
        me = self.me
        own = self.view(me.b)
        self.pend.start(
            remote(own, own, self.send.at[0], self.recv.at[me.z], me.at_z(me.z + 1)),
            me.z < 2 + me.c,
        )
        self.pend.start(remote(own, own, self.psend.at[3], self.precv.at[me.z], me.partner()))

    def near(self, core):
        return self.me.z * (3 + core - self.me.z) > 0

    def take(self, source):
        block = self.view(2 * source + self.me.c)
        remote(
            block, block, self.send.at[0], self.recv.at[source], self.me.partner()
        ).wait_recv()
        return block

    def relay(self):
        me = self.me

        @pl.when(self.near(me.c))
        def _():
            self.take(me.z - 1)

        block = self.view(2 * (me.z - 1) + me.c)
        self.pend.start(
            remote(block, block, self.send.at[1], self.recv.at[me.z - 1], me.at_z(me.z + 1)),
            me.z == 1,
        )
        self.pend.start(
            remote(block, block, self.psend.at[0], self.precv.at[me.z - 1], me.partner()),
            self.near(me.c),
        )

        @pl.when(me.z == 2)
        def _():
            self.take(0)

        block = self.view(me.c)
        self.pend.start(
            remote(block, block, self.psend.at[1], self.precv.at[0], me.partner()), me.z == 2
        )

    def finish(self):
        me = self.me

        def take(source):
            block = self.view(2 * source + (1 - me.c))
            remote(
                block, block, self.psend.at[0], self.precv.at[source], me.partner()
            ).wait_recv()

        take(me.z)

        @pl.when(self.near(1 - me.c))
        def _():
            take(me.z - 1)

        @pl.when(me.z == 2)
        def _():
            take(0)


class FullGather(LineGather):
    def __init__(self, me, pend, buffer, sems):
        super().__init__(
            me,
            pend,
            lambda block: buffer.at[rows(block), :],
            lambda block: buffer.at[rows(block), cols(me.t)],
            lambda count: buffer.at[0 : TB * count, :],
            lambda count: buffer.at[0 : TB * count, 0:TC],
            sems[:4],
        )
        self.buffer = buffer
        self.xsend, self.xrecv = sems[4:]

    def piece(self, i, k):
        lanes = cols(self.me.t if k == 0 else self.me.peer_t(k))
        return self.buffer.at[rows(2 * self.me.arrival(i) + self.me.c), lanes]

    def part(self, i, k, half):
        start = (2 * self.me.arrival(i) + self.me.c) * TB + HALF * half
        return self.buffer.at[pl.ds(pl.multiple_of(start, HALF), HALF), cols(self.me.peer_t(k))]

    def copy(self, view, i, relayed, k):
        return remote(
            view,
            view,
            self.xsend.at[0],
            self.xrecv.at[relayed, self.me.arrival(i)],
            self.me.plane(k),
        )

    def spread(self, i, last=True):
        for k in (1, 2):
            self.pend.begin(self.copy(self.piece(i, 0), i, 0, k))
        if i == 2 and last:
            self.register_spread()

    def register_spread(self):
        nine = self.buffer.at[0:864, 0:768]
        self.pend.later(self.copy(nine, 2, 0, 1))

    def relay(self, i):
        self.copy(self.buffer.at[0 : 2 * TB, 0:TC], i, 0, 1).wait_recv()
        for k in (1, 2):
            self.pend.begin(self.copy(self.part(i, k, k - 1), i, 1, 3 - k))

    def cross(self, i):
        self.copy(self.buffer.at[0:TB, 0:TC], i, 1, 1).wait_recv()
        self.share(i)


def swap_halves(u):
    lane = lax.broadcasted_iota(jnp.int32, u.shape, 1)
    return jnp.where(lane % 64 < 32, pltpu.roll(u, 96, 1), pltpu.roll(u, 32, 1))


def half_mask(half):
    lane = lax.broadcasted_iota(jnp.int32, (TB, 128), 1)
    return (lane // 64) == half


def head_from_chunk(chunk, h):
    if h % 2 != h // 3:
        chunk = pltpu.roll(chunk, 64, 1)
    return jnp.where(half_mask(h // 3), chunk, 0.0)


def chunk_from_heads(first, second, pair):
    if (2 * pair) // 3 != 0:
        first = pltpu.roll(first, 64, 1)
    if (2 * pair + 1) // 3 != 1:
        second = pltpu.roll(second, 64, 1)
    return jnp.where(half_mask(0), first, second)


def row_chunks(body, size=64):
    def step(i, carry):
        body(pl.ds(pl.multiple_of(i * size, size), size))
        return carry

    lax.fori_loop(0, TB // size, step, 0)


class Bag(dict):
    __getattr__ = dict.__getitem__


def bags(tree):
    return Bag({k: bags(v) for k, v in tree.items()}) if isinstance(tree, dict) else tree


def scratch_tree():
    def f32(*shape):
        return pltpu.VMEM(shape, F32)

    def b16(*shape):
        return pltpu.VMEM(shape, BF16)

    dma = pltpu.SemaphoreType.DMA

    def pair(*shape):
        return (dma(shape), dma(shape))

    def line():
        return (dma((1,)), dma((4,)), dma((1,)), dma((1,)))

    def up():
        return (dma((2,)), dma((4,)), dma((4,)), dma((4,)))

    def full():
        return (*line(), dma((1,)), dma((2, 4)))

    def scatter():
        return dict(
            part=b16(DM, DM),
            core=b16(4, TB, DM),
            plane=b16(4, 2, TB, TC),
            diagonal=b16(4, 2, HALF, TC),
            line=b16(6, TB, TC),
            sems=(dma((1,)), dma((4,)), dma((1,)), dma((4, 2)), dma((1,)), dma((6,))),
        )

    def reduce(width):
        return dict(
            core=b16(4, TB, width),
            line=b16(6, TB, width),
            sems=(dma((1,)), dma((4,)), dma((2,)), dma((6,))),
        )

    return dict(
        w_qkv=b16(DM, 640),
        small=f32(NBLK, 24, 256),
        w_out=b16(DM, DM),
        d_moe=b16(DM, DM),
        hn=b16(DM, DM),
        kv=b16(DM, 256),
        w_moe=b16(DM, 768),
        comb=f32(NBLK, 16, 256),
        xn=b16(TB, DM),
        r_one=f32(TB, 1),
        r_two=f32(TB, 1),
        hidden=f32(TB, DM),
        qz=b16(NQ, TB, 128),
        oz=f32(NQ, TB, 128),
        den=f32(NQ, TB, 128),
        o_full=b16(TB, DM),
        gains=f32(8, DM),
        router_t=b16(16, DM),
        dgu=b16(DM, 512),
        cz=b16(DM, 256),
        h=scatter(),
        y=scatter(),
        dhn=b16(TB, DM),
        dc_own=f32(NBLK, 8, 256),
        dc_in=f32(NBLK, 8, 256),
        dc_plane=f32(3, NBLK, 8, 256),
        dc_t=f32(16, 256),
        g_moe=b16(DM, 768),
        acc=f32(TB, TC),
        dh=f32(TB, DM),
        dproj=b16(TB, DM),
        flat=f32(24, DM),
        sm=dict(own=f32(NBLK, 24, 256), inn=f32(NBLK, 24, 256)),
        sn=dict(own=f32(NBLK, 8, 256), inn=f32(NBLK, 8, 256)),
        g_out_sum=b16(TB, TC),
        dnz=b16(NQ, TB, 128),
        dkv=b16(DM, 256),
        dqkv=b16(TB, 640),
        g_qkv_sum=b16(TB, 640),
        dx=b16(TB, DM),
        dx_in=b16(3, TB, TC),
        dxn=b16(TB, DM),
        local_sem=dma((11,)),
        lg=dict(s=line(), w=line(), v=line(), o=line(), kv=up(), c=line()),
        fg=dict(wo=full(), dm=full(), hn=full()),
        aa=dict(
            wm=[pair(1), pair(1)], gm=[pair(1), pair(1)], dc=pair(1), sm=pair(1), sn=pair(1)
        ),
        pl=dict(
            o=pair(1), hc=pair(1), dc=pair(1), dh=pair(1), go=pair(1), gq=pair(1), gk=pair(1),
            gv=pair(1), xs=pair(1), xg=pair(1),
        ),
        rd=dict(go=reduce(TC), dkv=reduce(256), gq=reduce(TC), gkv=reduce(256)),
    )


def kernel(r):
    g_out_part = r.dgu.at[:, 0:TC]
    w_column = r.y.part.at[:, 0:TC]
    g_q_part, g_kv_part = r.w_moe.at[:, 0:TC], r.w_moe.at[:, TC:640]
    me = Place()
    pend = Pending()
    z, c, t, b = me.z, me.c, me.t, me.b

    loc = r.local_sem
    local = [
        pltpu.make_async_copy(r.wq.at[:, cols(t)], r.w_qkv.at[rows(b), 0:384], loc.at[0]),
        pltpu.make_async_copy(
            r.wk.at[:, pl.ds(pl.multiple_of(128 * t, 128), 128)],
            r.w_qkv.at[rows(b), 384:512], loc.at[1],
        ),
        pltpu.make_async_copy(
            r.wv.at[:, pl.ds(pl.multiple_of(128 * t, 128), 128)],
            r.w_qkv.at[rows(b), 512:640], loc.at[2],
        ),
        pltpu.make_async_copy(r.wo.at[:, cols(t)], w_column.at[rows(b), :], loc.at[3]),
        pltpu.make_async_copy(r.wo, r.w_out.at[rows(b), :], loc.at[10]),
    ]
    moe_lanes = [[pl.ds(384 * e + 128 * which, 128) for which in range(3)] for e in range(2)]
    moe_sources = [list(zip((r.gate, r.up, r.down_t), lanes)) for lanes in moe_lanes]
    own_moe = [
        pltpu.make_async_copy(
            shard.at[2 * b + e], r.w_moe.at[rows(b), lanes], loc.at[4 + 3 * e + i]
        )
        for e in range(2)
        for i, (shard, lanes) in enumerate(moe_sources[e])
    ]
    for copy in local:
        copy.start()
    for copy in own_moe:
        copy.start()
    barrier = pltpu.get_barrier_semaphore()
    for k in range(1, NBLK):
        pl.semaphore_signal(
            barrier, inc=1, device_id=me.at_block(me.other(k)), device_id_type=MESH_ID
        )
    for k in (1, 2, 3):
        pl.semaphore_signal(barrier, inc=1, device_id=me.plane(k), device_id_type=MESH_ID)
    r.small[b, 0:16, 0:TB] = r.router_own[...].astype(F32)
    for n in range(2):
        r.small[b, 16 + n : 17 + n, 0:128] = r.vectors[12 + 2 * n : 13 + 2 * n, :]
        r.small[b, 16 + n : 17 + n, 128:TB] = r.vectors[13 + 2 * n : 14 + 2 * n, 0:64]
    r.d_moe[rows(b), :] = (residual_scale * r.gout[...]).astype(BF16)
    pl.semaphore_wait(barrier, NBLK - 1 + 3)

    def line(view, several, sems):
        return LineGather(me, pend, view, view, several, several, sems)

    g_small = line(lambda k: r.small.at[k], lambda n: r.small.at[0:n], r.lg.s)
    def columns(lanes, sems):
        return line(
            lambda k: r.w_qkv.at[rows(k), lanes], lambda n: r.w_qkv.at[0 : TB * n, lanes], sems
        )

    g_keys = columns(slice(TC, 640), r.lg.w)
    g_query = columns(slice(0, TC), r.lg.v)
    g_kv = UpGather(me, pend, lambda k: r.kv.at[rows(k), :], r.lg.kv)
    g_comb = line(lambda k: r.comb.at[k], lambda n: r.comb.at[0:n], r.lg.c)
    early = Pending()
    wcol_view = lambda k: w_column.at[rows(k), :]
    wcol_several = lambda n: w_column.at[0 : TB * n, :]
    g_wcol = LineGather(me, early, wcol_view, wcol_view, wcol_several, wcol_several, r.lg.o)
    g_wout = FullGather(me, pend, r.w_out, r.fg.wo)
    g_dmoe = FullGather(me, pend, r.d_moe, r.fg.dm)
    g_hn = FullGather(me, pend, r.hn, r.fg.hn)

    def send_weights_to(e, peer):
        send, recv = r.aa.wm[e]
        for shard, lanes in moe_sources[e]:
            remote(
                shard.at[2 * peer + e],
                r.w_moe.at[rows(b), lanes],
                send.at[0],
                recv.at[0],
                me.at_block(peer),
            ).start()

    end_chip = z * (3 - z) == 0

    def send_weights(e, ks, middle):
        for k in ks:
            peer = me.other(k)
            if middle:

                @pl.when(peer // 2 + z != 3)
                def _(peer=peer):
                    send_weights_to(e, peer)

            else:
                send_weights_to(e, peer)

    def send_weights_middle(e):
        for j in range(2):
            send_weights_to(e, 6 - 2 * z + j)

    def seven_blocks(sems):
        whole = r.w_moe.at[0 : 7 * TB, 0:TC]
        return remote(whole, whole, sems[0].at[0], sems[1].at[0], me.partner())

    g_small.start()
    for copy in local[1:3]:
        copy.wait()
    g_keys.start()
    local[0].wait()
    g_query.start()
    local[3].wait()
    g_wcol.start()

    def rms_one(chunk):
        v = r.x[chunk, :].astype(F32)
        r.r_one[chunk, :] = lax.rsqrt(jnp.mean(v * v, axis=1, keepdims=True) + norm_eps)

    row_chunks(rms_one)
    for i in range(3):
        g_small.arrive(i)
        g_small.share(i)
        g_keys.arrive(i)
        g_keys.share(i)
        if i > 0:
            g_query.arrive(i - 1)
            g_query.share(i - 1)

    @pl.when(me.middle())
    def _():
        send_weights_middle(0)

    g_small.finish()
    for k in range(NBLK):
        piece = r.small[k]
        r.router_t[:, TB * k : TB * (k + 1)] = piece[0:16, 0:TB].astype(BF16)
        r.gains[0:8, TB * k : TB * (k + 1)] = piece[16:24, 0:TB]

    def normalize_one(chunk):
        v = r.x[chunk, :].astype(F32)
        r.xn[chunk, :] = (v * r.r_one[chunk, :] * r.gains[0:1, :]).astype(BF16)

    row_chunks(normalize_one)
    g_keys.finish()
    key_value = jnp.dot(r.xn[...], r.w_qkv[:, TC:640], preferred_element_type=F32)
    base_c, base_s = r.rope_block[0, pl.ds(b, 1), :], r.rope_block[1, pl.ds(b, 1), :]
    row_c, row_s = r.rope_row[0], r.rope_row[1]
    first_half = lax.broadcasted_iota(jnp.int32, (TB, 128), 1) % 64 < 32
    cosine = base_c * row_c - base_s * row_s
    sine = base_s * row_c + base_c * row_s
    sine = jnp.where(first_half, -sine, sine)
    key = key_value[:, 0:128]
    r.kv[rows(b), 0:128] = (key * cosine + swap_halves(key) * sine).astype(BF16)
    r.kv[rows(b), 128:256] = key_value[:, 128:256].astype(BF16)
    g_kv.start()
    g_dmoe.send_own()
    g_query.arrive(2)
    g_query.share(2)
    g_wcol.arrive(0)
    g_wcol.share(0)
    g_kv.relay()
    g_query.finish()
    query = jnp.dot(r.xn[...], r.w_qkv[:, 0:TC], preferred_element_type=F32)
    for pair in range(3):
        u = query[:, 128 * pair : 128 * (pair + 1)]
        u = (u * cosine + swap_halves(u) * sine).astype(BF16).astype(F32)
        r.qz[2 * pair] = head_from_chunk(u, 2 * pair).astype(BF16)
        r.qz[2 * pair + 1] = head_from_chunk(u, 2 * pair + 1).astype(BF16)
    for h in range(NQ):
        r.oz[h] = jnp.zeros((TB, 128), F32)
        r.den[h] = jnp.zeros((TB, 128), F32)

    @pl.when(me.middle())
    def _():
        g_wcol.arrive(1)
        g_wcol.share(1)
        g_wcol.arrive(2)
        g_wcol.share(2)
        g_dmoe.arrive(0)
        g_dmoe.spread(0, False)
        send_weights_middle(1)
        send_weights(0, (1, 7, 2), True)

    @pl.when(end_chip)
    def _():
        send_weights(0, (1, 7, 2, 6), False)

    g_dmoe.register()
    g_dmoe.register_spread()
    g_kv.finish()

    first_block = FIRST_DOC_BLOCKS * (b // FIRST_DOC_BLOCKS)

    second_end = (r.vectors[0:12, :] < 1.5).astype(F32)
    second_end = jnp.sum(jnp.sum(second_end, axis=0, keepdims=True), axis=1, keepdims=True)

    def allowed(kb):
        q_pos = b * TB + lax.broadcasted_iota(jnp.int32, (TB, TB), 0)
        k_pos = kb * TB + lax.broadcasted_iota(jnp.int32, (TB, TB), 1)
        q_first = (q_pos.astype(F32) < second_end).astype(F32)
        k_first = (k_pos.astype(F32) < second_end).astype(F32)
        return (q_pos >= k_pos) & (q_first == k_first)

    def attend(kb, carry):
        keys = r.kv[rows(kb), 0:128]
        values = r.kv[rows(kb), 128:256]
        mask = allowed(kb)
        for g in range(2):
            heads = pl.ds(3 * g, 3)
            q = r.qz[heads].reshape(3 * TB, 128)
            e = jnp.exp(contract(q, keys, 1, 1) * score_scale).reshape(3, TB, TB)
            e = jnp.where(mask[None], e, 0.0)
            r.den[heads] += jnp.broadcast_to(jnp.sum(e, axis=2, keepdims=True), (3, TB, 128))
            e = e.reshape(3 * TB, TB).astype(BF16)
            r.oz[heads] += jnp.dot(e, values, preferred_element_type=F32).reshape(3, TB, 128)
        return carry

    lax.fori_loop(first_block, b + 1, attend, 0)
    for pair in range(3):
        heads = []
        for h in (2 * pair, 2 * pair + 1):
            o = jnp.where(half_mask(h // 3), r.oz[h] / r.den[h], 0.0)
            r.oz[h] = o
            heads.append(o)
        chunk = chunk_from_heads(heads[0], heads[1], pair).astype(BF16)
        r.o_full[:, pl.ds(pl.multiple_of(TC * t + 128 * pair, 128), 128)] = chunk

    def to_plane(sems, copies_of, three, pend=pend):
        send, recv = sems
        for k in (3, 1, 2):
            src, dst = copies_of(k)
            pend.begin(remote(src, dst, send.at[0], recv.at[0], me.plane(k)))
        all_three = remote(three, three, send.at[0], recv.at[0], me.plane(1))
        pend.later(all_three)
        return all_three.wait_recv

    def plane_gather(sems, buffer, pend=pend):
        own = buffer.at[:, cols(t)]
        return to_plane(sems, lambda k: (own, own), buffer.at[:, 0 : 3 * TC], pend)

    wait_o = plane_gather(r.pl.o, r.o_full)

    @pl.when(me.middle())
    def _():
        send_weights(0, (6, 3), True)

    @pl.when(end_chip)
    def _():
        g_wcol.arrive(1)
        g_wcol.share(1)
        g_wcol.arrive(2)
        g_wcol.share(2)
        g_dmoe.arrive(0)
        g_dmoe.spread(0, False)
        send_weights(0, (3, 5), False)

    g_wcol.finish()
    wait_o()

    column = jnp.dot(r.o_full[...], w_column[...], preferred_element_type=F32)
    r.dx[:, cols(t)] = column.astype(BF16)
    wait_column = plane_gather(r.pl.hc, r.dx, early)
    wait_column()

    def normalize_two(chunk):
        v = r.x[chunk, :].astype(F32) + residual_scale * r.dx[chunk, :].astype(F32)
        r.hidden[chunk, :] = v
        factor = lax.rsqrt(jnp.mean(v * v, axis=1, keepdims=True) + norm_eps)
        r.r_two[chunk, :] = factor
        r.dproj[chunk, :] = (v * factor * r.gains[1:2, :]).astype(BF16)

    row_chunks(normalize_two)
    r.hn[rows(b), :] = r.dproj[...]
    g_hn.start()
    logits = contract(r.router_t[...], r.dproj[...], 1, 1)
    chosen_expert = lax.broadcasted_iota(jnp.int32, (E, TB), 0)
    chosen = chosen_expert == r.routes_t[0:1, :]
    for k in range(1, TOPK):
        chosen = chosen | (chosen_expert == r.routes_t[k : k + 1, :])
    top = jnp.max(jnp.where(chosen, logits, -1e30), axis=0, keepdims=True)
    weight = jnp.where(chosen, jnp.exp(jnp.where(chosen, logits - top, 0.0)), 0.0)
    combine = weight / jnp.sum(weight, axis=0, keepdims=True)
    r.comb[b, :, 0:TB] = combine
    g_comb.start()
    g_dmoe.arrive(1)
    g_dmoe.spread(1, False)
    g_dmoe.arrive(2)
    g_dmoe.spread(2, False)
    g_dmoe.relay(0)
    for i in range(3):
        g_hn.arrive(i)
        g_hn.spread(i)
        g_comb.arrive(i)
        g_comb.share(i)

    @pl.when(me.middle())
    def _():
        send_weights(0, (5, 4), True)
        send_weights(1, (4, 3, 5, 2, 6, 1, 7), True)

    @pl.when(end_chip)
    def _():
        send_weights(0, (4,), False)
        send_weights(1, (4, 3, 5, 2, 6, 1, 7), False)

    g_dmoe.relay(1)
    g_dmoe.relay(2)
    for i in range(3):
        g_hn.relay(i)
    for i in range(3):
        g_dmoe.cross(i)
    g_dmoe.finish()
    g_comb.finish()
    for i in range(3):
        g_hn.cross(i)
    local[4].wait()
    own_columns = []
    for i in range(3):
        where = rows(2 * me.arrival(i) + c)
        copy = pltpu.make_async_copy(
            w_column.at[where, :], r.w_out.at[where, cols(t)], loc.at[i]
        )
        copy.start()
        own_columns.append(copy)
    g_wout.share_own()
    for i in range(3):
        own_columns[i].wait()
        g_wout.spread(i)
    g_hn.finish()
    for copy in own_moe:
        copy.wait()
    seven_blocks(r.aa.wm[0]).wait_recv()

    expert = lax.broadcasted_iota(jnp.int32, (16, 128), 0)
    first_row = (lax.broadcasted_iota(jnp.int32, (8, 128), 0) == 0).astype(F32)

    def core_copy(own, i):
        part = own.part.at[rows(2 * i + (1 - c)), :]
        return remote(part, own.core.at[i], own.sems[0].at[0], own.sems[1].at[i], me.partner())

    def plane_copy(own, i, k):
        return remote(
            own.part.at[rows(2 * i + c), cols(me.peer_t(k))],
            own.plane.at[i, k - 1],
            own.sems[2].at[0],
            own.sems[3].at[i, 0],
            me.plane(k),
        )

    def half_rows(i, k):
        return pl.ds(pl.multiple_of((2 * i + c) * TB + HALF * (k - 1), HALF), HALF)

    def diagonal_copy(own, i, k):
        return remote(
            own.part.at[half_rows(i, k), cols(me.peer_t(3))],
            own.diagonal.at[i, k - 1],
            own.sems[2].at[0],
            own.sems[3].at[i, 1],
            me.plane(k),
        )

    def plane_relay(own, i):
        both = own.diagonal.at[i]
        remote(both, both, own.sems[2].at[0], own.sems[3].at[i, 1], me.plane(1)).wait_recv()
        for k in (1, 2):
            where, lanes = half_rows(i, k), cols(me.peer_t(3 - k))
            own.part[where, lanes] = (
                own.part[where, lanes].astype(F32) + own.diagonal[i, k - 1].astype(F32)
            ).astype(BF16)
        for k in (1, 2):
            plane_copy(own, i, k).start()

    def core_sum(own, i):
        core_copy(own, i).wait_recv()

        def add(chunk):
            where = pl.ds(pl.multiple_of((2 * i + c) * TB + chunk.start, 64), 64)
            own.part[where, :] = (
                own.part[where, :].astype(F32) + own.core[i, chunk, :].astype(F32)
            ).astype(BF16)

        row_chunks(add)
        for k in (1, 2):
            diagonal_copy(own, i, k).start()

    def expert_block(e, where, block):
        base = 384 * e
        gate_up = jnp.dot(
            r.hn[where, :], r.w_moe[:, base : base + 256], preferred_element_type=F32
        )
        v = jnp.dot(
            r.d_moe[where, :], r.w_moe[:, base + 256 : base + 384], preferred_element_type=F32
        )
        g, u = gate_up[:, 0:128], gate_up[:, 128:256]
        chosen_one = (expert == 2 * b + e).astype(F32)
        scale = contract(r.comb[block, :, 0:TB], chosen_one, 0, 0, lax.Precision.HIGHEST)
        sig = 1.0 / (1.0 + jnp.exp(-g))
        silu = g * sig
        active = (silu * u).astype(BF16).astype(F32)
        r.cz[where, 128 * e : 128 * (e + 1)] = (scale * active).astype(BF16)
        dc = contract(first_row, active * v, 1, 1, lax.Precision.HIGHEST)
        r.dc_own[block, e : e + 1, 0:TB] = dc[0:1, :]
        dz = scale * v
        r.dgu[where, 256 * e : 256 * e + 128] = (dz * u * sig * (1.0 + g * (1.0 - sig))).astype(
            BF16
        )
        r.dgu[where, 256 * e + 128 : 256 * e + 256] = (dz * silu).astype(BF16)

    def expert_one(block, carry):
        expert_block(0, rows(block), block)
        return carry

    lax.fori_loop(0, NBLK, expert_one, 0)

    def weight_grads(e):
        def step(n, carry):
            lanes = pl.ds(pl.multiple_of(n * 256, 256), 256)
            base = 384 * e
            r.g_moe[lanes, base : base + 256] = contract(
                r.hn[:, lanes], r.dgu[:, 256 * e : 256 * (e + 1)], 0, 0
            ).astype(BF16)
            r.g_moe[lanes, base + 256 : base + 384] = contract(
                r.d_moe[:, lanes], r.cz[:, 128 * e : 128 * (e + 1)], 0, 0
            ).astype(BF16)
            return carry

        lax.fori_loop(0, DM // 256, step, 0)

    moe_targets = [list(zip((r.gate_out, r.up_out, r.down_out), lanes)) for lanes in moe_lanes]

    def send_grads(e, ks):
        send, recv = r.aa.gm[e]
        for k in ks:
            peer = me.other(k)
            for target, lanes in moe_targets[e]:
                remote(
                    r.g_moe.at[rows(peer), lanes],
                    target.at[2 * b + e],
                    send.at[0],
                    recv.at[0],
                    me.at_block(peer),
                ).start()

    weight_grads(0)
    send_grads(0, (4, 3, 5, 2, 6, 1, 7))

    def hidden_one(block, carry):
        where = rows(block)
        for n in range(3):
            lanes = slice(512 * n, 512 * (n + 1))
            r.h.part[where, lanes] = contract(
                r.dgu[where, 0:256], r.w_moe[lanes, 0:256], 1, 1
            ).astype(BF16)
        return carry

    lax.fori_loop(0, NBLK, hidden_one, 0)
    for i in range(3):
        g_wout.relay(i)
    seven_blocks(r.aa.wm[1]).wait_recv()
    early.drain()

    class Chain:
        def __init__(self, piece, line, send, recv, arrived):
            self.piece, self.line, self.send, self.recv = piece, line, send, recv
            self.arrived = arrived

        def copy(self, j):
            i = me.dest(j)
            upper = z // 2
            inner = (z * (3 - z)) // 2
            if j == 0:
                to, slot = z + 1 - 2 * upper, i
            elif j == 1:
                to, slot = z + 1 - 2 * upper, i + inner * (4 + upper - i)
            else:
                to, slot = i, 4 + z % 2
            return remote(
                self.piece(i), self.line.at[slot], self.send.at[0], self.recv.at[slot], me.at_z(to)
            )

        def wait_slot(self, slot):
            there = self.line.at[slot]
            remote(
                there, there, self.send.at[0], self.recv.at[slot], me.partner()
            ).wait_recv()

        def step(self, j):
            i = me.dest(j)
            self.arrived(i)

            @pl.when(me.middle())
            def _():
                self.wait_slot(i)
                piece = self.piece(i)
                piece[...] = (piece[...].astype(F32) + self.line[i].astype(F32)).astype(BF16)

            self.copy(j).start()

        def steps(self, when=None):
            if when is None:
                for j in range(3):
                    self.step(j)
            else:
                pl.when(when)(self.steps)

        def total(self, acc):
            self.arrived(z)
            acc[...] = self.piece(z)[...].astype(F32)
            for slot, there in ((4, z > 0), (5, z < 3)):

                @pl.when(there)
                def _(slot=slot):
                    self.wait_slot(slot)
                    acc[...] += self.line[slot].astype(F32)

        def drain(self):
            three = self.line.at[0:3]
            remote(three, three, self.send.at[0], self.recv.at[0], me.partner()).wait_send()

    def plane_add(own, i):
        both = own.plane.at[i]
        remote(both, both, own.sems[2].at[0], own.sems[3].at[i, 0], me.plane(1)).wait_recv()
        where = rows(2 * i + c)
        total = own.part[where, cols(t)].astype(F32)
        for k in range(2):
            total = total + own.plane[i, k].astype(F32)
        own.part[where, cols(t)] = total.astype(BF16)

    def scatter_chain(own):
        return Chain(
            lambda i: own.part.at[rows(2 * i + c), cols(t)],
            own.line,
            own.sems[4],
            own.sems[5],
            lambda i: plane_add(own, i),
        )

    def scatter_drain(own):
        remote(own.core, own.core, own.sems[0].at[0], own.sems[1].at[0], me.partner()).wait_send()
        twelve = own.part.at[0:576, :]
        remote(twelve, twelve, own.sems[2].at[0], own.sems[3].at[0, 0], me.plane(1)).wait_send()

    chain_h, chain_y = scatter_chain(r.h), scatter_chain(r.y)

    def expert_two(step, carry):
        i = me.dest(step // 2)
        late = step % 2
        block = 2 * i + (1 - c) + late * (2 * c - 1)
        where = rows(block)
        expert_block(1, where, block)
        for n in range(3):
            lanes = slice(512 * n, 512 * (n + 1))
            r.h.part[where, lanes] = (
                r.h.part[where, lanes].astype(F32)
                + contract(r.dgu[where, 256:512], r.w_moe[lanes, 384:640], 1, 1)
            ).astype(BF16)

        @pl.when(late == 0)
        def _():
            core_copy(r.h, i).start()

        for n in range(3):
            lanes = slice(512 * n, 512 * (n + 1))
            r.y.part[where, lanes] = (
                contract(r.cz[where, 0:128], r.w_moe[lanes, 256:384], 1, 1)
                + contract(r.cz[where, 128:256], r.w_moe[lanes, 640:768], 1, 1)
            ).astype(BF16)

        @pl.when(late == 0)
        def _():
            core_copy(r.y, i).start()

        @pl.when(late == 1)
        def _():
            core_sum(r.h, i)

        @pl.when((late == 1) & (step > 1))
        def _():
            plane_relay(r.h, me.dest(step // 2 - 1))

        for j in range(2):

            @pl.when(end_chip & (step == 2 * j + 5))
            def _(j=j):
                chain_h.step(j)

        return carry

    lax.fori_loop(0, NBLK, expert_two, 0)

    plane_relay(r.h, z)
    dc_send, dc_recv = r.aa.dc
    for k in range(1, NBLK):
        peer = me.other(k)
        pend.begin(
            remote(
                r.dc_own.at[peer], r.dc_in.at[b], dc_send.at[0], dc_recv.at[0],
                me.at_block(peer),
            )
        )
    dc_seven = r.dc_own.at[0:7]
    dc_all = remote(dc_seven, dc_seven, dc_send.at[0], dc_recv.at[0], me.partner())
    pend.later(dc_all)
    r.dc_in[b] = r.dc_own[b]

    for i in range(3):
        g_wout.cross(i)

    @pl.when(me.middle())
    def _():
        chain_h.step(0)
        chain_h.step(1)

    chain_h.step(2)
    weight_grads(1)
    own_grads = [
        pltpu.make_async_copy(
            r.g_moe.at[rows(b), lanes], target.at[2 * b + e], loc.at[4 + 3 * e + i]
        )
        for e in range(2)
        for i, (target, lanes) in enumerate(moe_targets[e])
    ]
    for copy in own_grads:
        copy.start()

    dc_all.wait_recv()
    wait_dc = to_plane(r.pl.dc, lambda k: (r.dc_in, r.dc_plane.at[k - 1]), r.dc_plane)

    @pl.when(me.middle())
    def _():
        send_grads(1, (1, 7, 2))

    @pl.when(end_chip)
    def _():
        send_grads(1, (4, 3, 5, 2, 6, 1, 7))

    chain_h.total(r.acc.at[:, 0:TC])
    r.dhn[:, cols(t)] = r.acc[:, 0:TC].astype(BF16)

    @pl.when(me.middle())
    def _():
        send_grads(1, (6, 3))

    wait_dh = plane_gather(r.pl.dh, r.dhn)
    for j in range(4):
        core_sum(r.y, me.dest(j))
    wait_dc()
    for k in range(NBLK):
        total = r.dc_in[k] + r.dc_plane[0, k] + r.dc_plane[1, k] + r.dc_plane[2, k]
        r.dc_t[2 * k : 2 * k + 2, :] = total[0:2, :]
    dc = r.dc_t[:, 0:TB]
    combine = r.comb[b, :, 0:TB]
    d_logits = combine * (dc - jnp.sum(combine * dc, axis=0, keepdims=True))
    d_logits = d_logits.astype(BF16)
    r.flat[0:16, :] = jnp.dot(d_logits, r.hn[rows(b), :], preferred_element_type=F32)

    wait_dh()

    r.dh[...] = r.dhn[...].astype(F32) + contract(d_logits, r.router_t[...], 0, 0)
    r.flat[16:24, :] = jnp.zeros((8, DM), F32)

    def norm_two_back(chunk):
        dhn = r.dh[chunk, :]
        unit = r.hidden[chunk, :] * r.r_two[chunk, :]
        r.flat[16:17, :] += jnp.sum(dhn * unit, axis=0, keepdims=True)
        du = dhn * r.gains[1:2, :]
        mean = jnp.mean(du * unit, axis=1, keepdims=True)
        dh = r.gout[chunk, :] + r.r_two[chunk, :] * (du - unit * mean)
        r.dh[chunk, :] = dh
        r.dproj[chunk, :] = (residual_scale * dh).astype(BF16)

    row_chunks(norm_two_back)

    def to_owners(store, sems, width):
        send, recv = sems
        for k in range(NBLK):
            store.own[k, :, 0:TB] = r.flat[0:width, TB * k : TB * (k + 1)]
        store.inn[b] = store.own[b]
        for k in range(1, NBLK):
            peer = me.other(k)
            pend.begin(
                remote(
                    store.own.at[peer], store.inn.at[b], send.at[0], recv.at[0],
                    me.at_block(peer),
                )
            )
        seven = store.own.at[0:7]
        all_seven = remote(seven, seven, send.at[0], recv.at[0], me.partner())
        pend.later(all_seven)

        def wait():
            all_seven.wait_recv()
            total = store.inn[0]
            for k in range(1, NBLK):
                total = total + store.inn[k]
            return total

        return wait

    wait_sm = to_owners(r.sm, r.aa.sm, 24)

    g_wout.finish()
    d_o = contract(r.dproj[...], r.w_out[cols(t), :], 1, 1).astype(BF16).astype(F32)
    for h in range(NQ):
        pair = h // 2
        dh_z = head_from_chunk(d_o[:, 128 * pair : 128 * (pair + 1)], h)
        den = r.den[h]
        r.dnz[h] = (dh_z / den).astype(BF16)
        r.den[h] = (
            jnp.broadcast_to(jnp.sum(dh_z * r.oz[h], axis=1, keepdims=True), (TB, 128)) / den
        )
        r.oz[h] = jnp.zeros((TB, 128), F32)

    def out_grads(n, carry):
        lanes = pl.ds(pl.multiple_of(n * 256, 256), 256)
        g_out_part[lanes, :] = contract(
            r.o_full[:, lanes], r.dproj[:, cols(t)], 0, 0
        ).astype(BF16)
        return carry

    lax.fori_loop(0, DM // 256, out_grads, 0)

    class Reduce(Chain):
        def __init__(self, part, own):
            self.part, self.core, self.sems = part, own.core, own.sems
            super().__init__(
                lambda i: part.at[rows(2 * i + c), :], own.line, own.sems[2], own.sems[3], self.chip
            )

        def core_copy(self, i):
            return remote(
                self.part.at[rows(2 * i + (1 - c)), :],
                self.core.at[i],
                self.sems[0].at[0],
                self.sems[1].at[i],
                me.partner(),
            )

        def start(self):
            for j in range(4):
                self.core_copy(me.dest(j)).start()

        def chip(self, i):
            self.core_copy(i).wait_recv()
            piece = self.piece(i)
            piece[...] = (piece[...].astype(F32) + self.core[i].astype(F32)).astype(BF16)

        def drain(self):
            super().drain()
            self.drain_core()

        def drain_core(self):
            remote(
                self.core, self.core, self.sems[0].at[0], self.sems[1].at[0], me.partner()
            ).wait_send()

        def down(self):
            for i in range(4):
                self.chip(i)

            @pl.when(z == 1)
            def _():
                self.wait_slot(0)
                piece = self.piece(0)
                piece[...] = (piece[...].astype(F32) + self.line[0].astype(F32)).astype(BF16)

            for i, slot, when in (
                (0, 0, z == 2),
                (1, 5, z == 2),
                (0, 5, z == 1),
                (2, 5, z + c == 4),
            ):
                pend.start(
                    remote(
                        self.piece(i),
                        self.line.at[slot],
                        self.send.at[1 if i == 1 else 0],
                        self.recv.at[slot],
                        me.at_z(z - 1),
                    ),
                    when,
                )

        def down_total(self, acc):
            acc[...] = self.piece(z)[...].astype(F32)

            @pl.when(z < 2 + c)
            def _():
                self.wait_slot(5)
                acc[...] += self.line[5].astype(F32)

    red_out = Reduce(g_out_part, r.rd.go)
    red_out.start()
    red_out.steps(z * (3 - z) == 0)

    for j in range(4):
        plane_relay(r.y, me.dest(j))
    def clear(i, carry):
        r.dkv[rows(i), :] = jnp.zeros((TB, 256), BF16)
        return carry

    lax.fori_loop(0, NBLK, clear, 0)

    def attend_back(kb, carry):
        keys = r.kv[rows(kb), 0:128]
        values = r.kv[rows(kb), 128:256]
        mask = allowed(kb)
        dk = jnp.zeros((TB, 128), F32)
        dv = jnp.zeros((TB, 128), F32)
        for g in range(2):
            heads = pl.ds(3 * g, 3)
            q = r.qz[heads].reshape(3 * TB, 128)
            dn = r.dnz[heads].reshape(3 * TB, 128)
            e = jnp.exp(contract(q, keys, 1, 1) * score_scale).reshape(3, TB, TB)
            e = jnp.where(mask[None], e, 0.0)
            dp = contract(dn, values, 1, 1).reshape(3, TB, TB)
            ds = (e * (dp - r.den[heads][:, :, 0:1])).reshape(3 * TB, TB).astype(BF16)
            e = e.reshape(3 * TB, TB).astype(BF16)
            r.oz[heads] += jnp.dot(ds, keys, preferred_element_type=F32).reshape(3, TB, 128)
            dk = dk + contract(ds, q, 0, 0)
            dv = dv + contract(e, dn, 0, 0)
        r.dkv[rows(kb), 0:128] = (dk * score_scale).astype(BF16)
        r.dkv[rows(kb), 128:256] = dv.astype(BF16)
        return carry

    lax.fori_loop(first_block, b + 1, attend_back, 0)
    red_kv = Reduce(r.dkv, r.rd.dkv)
    red_kv.start()
    for pair in range(3):
        heads = [
            jnp.where(half_mask(h // 3), r.oz[h] * score_scale, 0.0)
            for h in (2 * pair, 2 * pair + 1)
        ]
        u = chunk_from_heads(heads[0], heads[1], pair).astype(BF16).astype(F32)
        r.dqkv[:, 128 * pair : 128 * (pair + 1)] = (
            u * cosine - swap_halves(u) * sine
        ).astype(BF16)
    red_kv.down()

    @pl.when(me.middle())
    def _():
        send_grads(1, (5, 4))


    def q_grads(n, carry):
        lanes = pl.ds(pl.multiple_of(n * 256, 256), 256)
        g_q_part[lanes, :] = contract(r.xn[:, lanes], r.dqkv[:, 0:TC], 0, 0).astype(BF16)
        return carry

    lax.fori_loop(0, DM // 256, q_grads, 0)
    red_gq = Reduce(g_q_part, r.rd.gq)
    red_gq.start()
    red_gq.steps(end_chip)
    d_kv_acc = r.acc.at[:, 0:256]
    red_kv.down_total(d_kv_acc)
    d_kv = d_kv_acc[...].astype(BF16)
    u = d_kv[:, 0:128].astype(F32)
    r.dqkv[:, 384:512] = (u * cosine - swap_halves(u) * sine).astype(BF16)
    r.dqkv[:, 512:640] = d_kv[:, 128:256]

    for n in range(3):
        lanes = slice(512 * n, 512 * (n + 1))
        r.dx[:, lanes] = contract(r.dqkv[...], r.w_qkv[lanes, :], 1, 1).astype(BF16)
    wait_xs = to_plane(
        r.pl.xs, lambda k: (r.dx.at[:, cols(me.peer_t(k))], r.dx_in.at[k - 1]), r.dx_in
    )

    def kv_grads(n, carry):
        lanes = pl.ds(pl.multiple_of(n * 256, 256), 256)
        g_kv_part[lanes, :] = contract(r.xn[:, lanes], r.dqkv[:, TC:640], 0, 0).astype(BF16)
        return carry

    lax.fori_loop(0, DM // 256, kv_grads, 0)
    red_gkv = Reduce(g_kv_part, r.rd.gkv)
    red_gkv.start()
    red_gq.steps(me.middle())
    red_gkv.steps(end_chip)
    chain_y.steps(end_chip)
    wait_xs()
    total = r.dx[:, cols(t)].astype(F32)
    for k in range(3):
        total = total + r.dx_in[k].astype(F32)
    r.dxn[:, cols(t)] = total.astype(BF16)
    wait_dx = plane_gather(r.pl.xg, r.dxn)
    own_qkv, from_qkv = [], []

    def give(n, start, width, target, sems, three):
        def lanes(index):
            return pl.ds(pl.multiple_of(width * index, 128), width)

        piece = r.g_qkv_sum.at[:, start : start + width]
        there = target.at[:, lanes(t)]
        own = pltpu.make_async_copy(piece, there, loc.at[1 + n])
        own.start()
        own_qkv.append(own)
        from_qkv.append(to_plane(sems, lambda k: (piece, there), three))

    red_gkv.steps(me.middle())
    red_gq.total(r.acc.at[:, 0:TC])
    r.g_qkv_sum[:, 0:TC] = r.acc[:, 0:TC].astype(BF16)
    give(0, 0, TC, r.gq_out, r.pl.gq, r.dx_in)
    red_out.steps(me.middle())
    wait_dx()
    r.flat[0:8, :] = jnp.zeros((8, DM), F32)

    def norm_one_back(chunk):
        dxn = r.dxn[chunk, :].astype(F32)
        factor = r.r_one[chunk, :]
        unit = r.x[chunk, :].astype(F32) * factor
        r.flat[0:1, :] += jnp.sum(dxn * unit, axis=0, keepdims=True)
        du = dxn * r.gains[0:1, :]
        mean = jnp.mean(du * unit, axis=1, keepdims=True)
        r.grad_in[chunk, :] = r.dh[chunk, :] + factor * (du - unit * mean)

    row_chunks(norm_one_back)
    wait_sn = to_owners(r.sn, r.aa.sn, 8)
    red_gkv.total(r.acc.at[:, 0:256])
    r.g_qkv_sum[:, TC:640] = r.acc[:, 0:256].astype(BF16)
    give(1, 384, 128, r.gk_out, r.pl.gk, r.g_qkv_sum.at[:, 0:TC])
    give(2, 512, 128, r.gv_out, r.pl.gv, r.g_qkv_sum.at[:, 0:TC])
    red_out.total(r.acc.at[:, 0:TC])
    r.g_out_sum[...] = r.acc[:, 0:TC].astype(BF16)
    own_go = pltpu.make_async_copy(r.g_out_sum, r.g_out_out.at[:, cols(t)], loc.at[0])
    own_go.start()
    go_there = r.g_out_out.at[:, cols(t)]
    wait_go = to_plane(r.pl.go, lambda k: (r.g_out_sum, go_there), r.dx_in)
    chain_y.steps(me.middle())
    chain_y.total(r.acc.at[:, 0:TC])
    r.block_out[...] = r.hidden[:, cols(t)] + residual_scale * r.acc[:, 0:TC]
    r.sm_out[...] = wait_sm()
    r.sn_out[...] = wait_sn()

    wait_go()
    for wait in from_qkv:
        wait()
    own_go.wait()
    for copy in own_qkv:
        copy.wait()
    for copy in own_grads:
        copy.wait()
    for e in range(2):
        seven_blocks(r.aa.gm[e]).wait()
        seven_blocks(r.aa.wm[e]).wait_send()
    scatter_drain(r.h)
    scatter_drain(r.y)
    chain_h.drain()
    chain_y.drain()
    red_out.drain()
    red_kv.drain_core()
    red_gq.drain()
    red_gkv.drain()
    pend.drain()


def fast_body(
    block_input,
    segments,
    routes,
    attn_gain,
    ffn_gain,
    query_weight,
    key_matrix,
    value_matrix,
    out_weight,
    router_weight,
    gate_weight,
    up_weight,
    down_weight,
    grad_output,
):
    half = HEAD_DIM // 2
    inverse = rope_base ** (-(np.arange(half, dtype=np.float64) * 2.0 / HEAD_DIM))
    inverse = np.tile(inverse.astype(np.float32).astype(np.float64), 4)

    def table(positions):
        angles = positions[:, None] * inverse[None, :]
        return np.stack([np.cos(angles), np.sin(angles)]).astype(np.float32)

    vectors = (
        jnp.pad(segments, (0, 512)).astype(F32)
        + jnp.pad(attn_gain.astype(F32), (DM, 320))
        + jnp.pad(ffn_gain.astype(F32), (DM + 256, 64))
    ).reshape(16, 128)
    vmem, hbm = pl.BlockSpec(memory_space=pltpu.VMEM), pl.BlockSpec(memory_space=pl.ANY)
    ins = dict(
        x=(block_input, vmem),
        gout=(grad_output, vmem),
        rope_block=(jnp.asarray(table(np.arange(NBLK) * TB)), vmem),
        rope_row=(jnp.asarray(table(np.arange(TB))), vmem),
        vectors=(vectors, vmem),
        routes_t=(routes.T, vmem),
        router_own=(router_weight.T, vmem),
        wq=(query_weight, hbm),
        wk=(key_matrix, hbm),
        wv=(value_matrix, hbm),
        wo=(out_weight, hbm),
        gate=(gate_weight, hbm),
        up=(up_weight, hbm),
        down_t=(down_weight.transpose(0, 2, 1), hbm),
    )
    outs = dict(
        block_out=((TB, TC), F32, vmem),
        grad_in=((TB, DM), F32, vmem),
        sm_out=((24, 256), F32, vmem),
        sn_out=((8, 256), F32, vmem),
        gq_out=((TB, DM), BF16, hbm),
        gk_out=((TB, 512), BF16, hbm),
        gv_out=((TB, 512), BF16, hbm),
        g_out_out=((TB, DM), BF16, hbm),
        gate_out=((E, TB, 128), BF16, hbm),
        up_out=((E, TB, 128), BF16, hbm),
        down_out=((E, TB, 128), BF16, hbm),
    )
    leaves, tree = jax.tree.flatten(scratch_tree())

    def entry(*refs):
        table = bags(jax.tree.unflatten(tree, refs[len(ins) + len(outs) :]))
        table.update(zip((*ins, *outs), refs))
        kernel(table)

    results = pl.pallas_call(
        entry,
        name="layer",
        out_shape=[jax.ShapeDtypeStruct(shape, kind) for shape, kind, _ in outs.values()],
        in_specs=[spec for _, spec in ins.values()],
        out_specs=[spec for _, _, spec in outs.values()],
        scratch_shapes=leaves,
        compiler_params=pltpu.CompilerParams(
            collective_id=0, has_side_effects=True, vmem_limit_bytes=VMEM_BYTES
        ),
    )(*[value for value, _ in ins.values()])
    res = Bag(zip(outs, results))
    wide = widen(
        res.block_out, res.grad_in, res.gq_out, res.gk_out, res.gv_out, res.g_out_out,
        res.gate_out, res.up_out, res.down_out, res.sm_out, res.sn_out,
    )
    block_output, grad_input, g_query, g_key, g_value, g_out, gate, up, down = wide[:9]
    router, gain_two, gain_one = wide[9:]
    return (
        block_output,
        grad_input,
        gain_one.reshape(TB),
        gain_two.reshape(TB),
        g_query,
        g_key,
        g_value,
        g_out,
        router.T,
        gate,
        up,
        down.transpose(0, 2, 1),
    )


def widen(*arrays):
    steps = 2

    def spec(array):
        rest = (0,) * (array.ndim - 1)
        return pl.BlockSpec((array.shape[0] // steps, *array.shape[1:]), lambda i: (i, *rest))

    def entry(*refs):
        count = len(arrays)
        for source, target in zip(refs[: count - 2], refs[count:]):
            target[...] = source[...].astype(F32)
        sm, sn = refs[count - 2 : count]
        router, gain_two, gain_one = refs[-3:]
        router[...] = sm[0:16, 0:TB]
        gain_two[...] = sm[16:17, 0:TB]
        gain_one[...] = sn[0:1, 0:TB]

    def whole(*shape):
        return pl.BlockSpec(shape, lambda i: (0, 0))

    specs = [spec(a) for a in arrays[:-2]]
    return pl.pallas_call(
        entry,
        name="widen",
        grid=(steps,),
        in_specs=[*specs, whole(24, 256), whole(8, 256)],
        out_specs=[*specs, whole(16, TB), whole(1, TB), whole(1, TB)],
        out_shape=[
            *(jax.ShapeDtypeStruct(a.shape, F32) for a in arrays[:-2]),
            jax.ShapeDtypeStruct((16, TB), F32),
            jax.ShapeDtypeStruct((1, TB), F32),
            jax.ShapeDtypeStruct((1, TB), F32),
        ],
        cost_estimate=pl.CostEstimate(flops=4_000_000, bytes_accessed=16_000_000, transcendentals=0),
    )(*arrays)


VMEM_BYTES = 67043328


def fits(mesh):
    return (mesh.shape["fsdp"], mesh.shape["heads"], mesh.shape["tensor"]) == (4, 2, 4)


def solution(mesh):
    in_specs = (
        P(("fsdp", "heads"), None),
        P(),
        P(("fsdp", "heads"), None),
        P(("fsdp", "heads")),
        P(("fsdp", "heads")),
        P(("fsdp", "heads"), None),
        P(("fsdp", "heads"), None),
        P(("fsdp", "heads"), None),
        P(("fsdp", "heads"), None),
        P(("fsdp", "heads"), None),
        P(None, ("fsdp", "heads"), "tensor"),
        P(None, ("fsdp", "heads"), "tensor"),
        P(None, "tensor", ("fsdp", "heads")),
        P(("fsdp", "heads"), None),
    )
    out_specs = (
        P(("fsdp", "heads"), "tensor"),
        P(("fsdp", "heads"), None),
        P(("fsdp", "heads")),
        P(("fsdp", "heads")),
        P(("fsdp", "heads"), None),
        P(("fsdp", "heads"), None),
        P(("fsdp", "heads"), None),
        P(("fsdp", "heads"), None),
        P(("fsdp", "heads"), None),
        P(None, ("fsdp", "heads"), "tensor"),
        P(None, ("fsdp", "heads"), "tensor"),
        P(None, "tensor", ("fsdp", "heads")),
    )
    chosen = fast_body if fits(mesh) else body
    return jax.shard_map(chosen, mesh=mesh, in_specs=in_specs, out_specs=out_specs, check_vma=False)
```
